32 devices in a mesh: up: 8 (over z, core), down: 4 (over y, x).
Axes of the slice: x: 2, y: 2, z: 4, core: 2. Of those that a mesh axis runs over, the one named last changes fastest.
Arguments:
- deltas: bfloat16 [256, 4096], P('down', 'up'), may hold values from -6 to 6
- gradients: bfloat16 [256, 4096], P('up', 'down'), may hold values from -0.375 to 0.375
- up_blocks: int32 [8, 16], P(None, 'up'), may hold values from 0 to 3, as said below
- down_blocks: int32 [16], P('down'), may hold values from 0 to 7, as said below
- decoder: bfloat16 [4096, 4608], P('up', 'down'), may hold values from -0.09375 to 0.09375
- encoder: bfloat16 [4608, 4096], P('up', 'down'), may hold values from -6 to 6
Outputs:
- edge_scores: float32 [4096, 4096], P('up', 'down')
The draws below stay inside these ranges and needn't reach their ends.
Inputs may be any that keep to these rules, and one draw needn't show every extreme that they name: `up_blocks`: for each window and each index i of up, the 2 entries in columns i * 2 to (i + 1) * 2 - 1 are distinct. `down_blocks`: for each index j of down, the 4 entries j * 4 to (j + 1) * 4 - 1 are distinct.
All inputs are finite; a program needn't handle non-finite values.
Results may differ from the reference program's by a relative error of at most 0.0003.
Values may be sent and summed in bfloat16 or wider, within the bound.
A program may use at most 64 MiB of HBM per device.

```python
import jax
import jax.numpy as jnp
from jax import lax

D = 4608
VF_DEV = 1024
BLOCK = 128
UACT = 2
DACT = 4
WIN = 32
TOKENS = 256
WINDOWS = 8
UB_DEV = 4
VB_DEV = 8
UF = 4096
VF = 4096
N_UP = 8
N_DOWN = 4


def draw_up_blocks(key, part):
    ranked = jax.random.randint(key, (WINDOWS, N_UP, UB_DEV), 0, 1 << 20, dtype=jnp.int32)
    ranked = ranked * UB_DEV + jnp.arange(UB_DEV, dtype=jnp.int32)
    ordering = jnp.argsort(ranked, axis=-1, stable=True)
    return ordering[:, :, :UACT].reshape(WINDOWS, N_UP * UACT).astype(jnp.int32)


def draw_down_blocks(key, part):
    ranked = jax.random.randint(jax.random.fold_in(key, 7), (N_DOWN, VB_DEV), 0, 1 << 20, dtype=jnp.int32)
    ranked = ranked * VB_DEV + jnp.arange(VB_DEV, dtype=jnp.int32)
    ordering = jnp.argsort(ranked, axis=-1, stable=True)
    return ordering[:, :DACT].reshape(N_DOWN * DACT).astype(jnp.int32)


def level_of(key, shape, cuts, low, high):
    gain, own = 1.0, jax.random.fold_in(key, 6)
    for position, blocks in cuts:
        heights = jnp.exp(jax.random.uniform(jax.random.fold_in(own, position), (blocks,), jnp.float32, low / len(cuts), high / len(cuts)))
        gain = gain * jnp.repeat(heights, shape[position] // blocks).reshape([-1 if axis == position else 1 for axis in range(len(shape))])
    return gain


def normal_values(key, dims, scale, bound, split=(), kind=jnp.bfloat16):
    gain = level_of(key, dims, split, -0.22, 0.18) if split else 1.0
    drawn = jax.random.normal(key, dims, jnp.float32) * scale * gain
    return jnp.minimum(jnp.maximum(drawn, -bound), bound).astype(kind)


def setup_inputs(seed: int = 0) -> dict:
    key_of = jax.random.split(jax.random.key(seed), 7)
    return {
        "deltas": normal_values(key_of[0], (TOKENS, UF), 1.0, 6.0, ((0, 4), (1, 8))),
        "gradients": normal_values(key_of[1], (TOKENS, VF), TOKENS ** -0.5, 0.375, ((0, 8), (1, 4))),
        "up_blocks": draw_up_blocks(jax.random.fold_in(key_of[6], 71), 0),
        "down_blocks": draw_down_blocks(jax.random.fold_in(key_of[6], 71), 0),
        "decoder": normal_values(key_of[4], (UF, D), D ** -0.5, 0.09375, ((0, 8), (1, 4))),
        "encoder": normal_values(key_of[5], (D, VF), 1.0, 6.0, ((0, 8), (1, 4))),
    }


def reference(deltas, gradients, up_blocks, down_blocks, decoder, encoder):
    owners = (jnp.arange(N_UP * UACT, dtype=jnp.int32) // UACT) * UB_DEV
    global_ids = up_blocks + owners[None, :]
    every_block = jnp.arange(N_UP * UB_DEV, dtype=jnp.int32)
    block_on = jnp.any(global_ids[:, :, None] == every_block[None, None, :], axis=1)
    masked = deltas.reshape(WINDOWS, WIN, N_UP * UB_DEV, BLOCK) * block_on[:, None, :, None].astype(deltas.dtype)
    masked = masked.reshape(TOKENS, UF)

    def shard_scores(shard_index):
        enc_cols = lax.dynamic_slice_in_dim(encoder, shard_index * VF_DEV, VF_DEV, 1).reshape(D, VB_DEV, BLOCK)
        grad_cols = lax.dynamic_slice_in_dim(gradients, shard_index * VF_DEV, VF_DEV, 1).reshape(TOKENS, VB_DEV, BLOCK)
        chosen = lax.dynamic_slice_in_dim(down_blocks, shard_index * DACT, DACT, 0)
        enc_used = jnp.take(enc_cols, chosen, axis=1).reshape(D, DACT * BLOCK)
        grad_used = jnp.take(grad_cols, chosen, axis=1).reshape(TOKENS, DACT * BLOCK)
        virtual = jnp.dot(decoder, enc_used, preferred_element_type=jnp.float32)
        product = lax.dot_general(masked, grad_used, (((0,), (0,)), ((), ())), preferred_element_type=jnp.float32)
        scored = (product * virtual).reshape(UF, DACT, BLOCK)
        filled = jnp.zeros((UF, VB_DEV, BLOCK), jnp.float32).at[:, chosen, :].set(scored)
        return filled.reshape(UF, VF_DEV)

    stacked = lax.map(shard_scores, jnp.arange(N_DOWN, dtype=jnp.int32))
    return jnp.transpose(stacked, (1, 0, 2)).reshape(UF, VF)
```

```python
import functools

import jax
import jax.numpy as jnp
from jax import lax
from jax.experimental import pallas as pl
from jax.experimental.pallas import tpu as pltpu
from jax.sharding import PartitionSpec as P

BLOCK = 128
TAIL = 256
LARGE = 24 << 20
MESH = pl.DeviceIdType.MESH
F32 = jnp.float32


def flag(number, block, kind):
    return jnp.where(jnp.full((1, BLOCK), number, jnp.int32) == block, 1.0, 0.0).astype(kind)


def pick(ref, rows, number, blocks):
    total = None
    for b in range(blocks):
        term = ref[rows, b * BLOCK:(b + 1) * BLOCK] * flag(number, b, ref.dtype)
        total = term if total is None else total + term
    return total


def gather_scores(
    n_up, n_down, upb_in, downb_in, deltas, grads, dec, enc, out,
    upb, downb, dec_all, enc_raw, enc_all, del_raw, del_all, grad_raw, grad_all, masked, acc, prod,
    load_sem, send_sem, dec_recv, del_recv, enc_recv, pair_recv, grad_recv,
):
    levels = n_up // 2
    rows, depth = dec.shape
    height = enc.shape[0]
    half = enc_all.shape[2]
    part = rows // 2
    piece = part // 2
    toks = grads.shape[0]
    wins = del_all.shape[1]
    win = del_all.shape[2]
    uact = upb.shape[0]
    dact = downb.shape[0]
    blocks = enc.shape[1] // BLOCK
    up, down = lax.axis_index("up"), lax.axis_index("down")
    z, core = up // 2, up % 2
    place = lambda d: 2 * (d // 2) + (d + d // 2) % 2
    pos = place(down)
    right, left = place((pos + 1) % 4), place((pos + 3) % 4)
    diag = place((pos + 2) % 4)
    ring_to = ((up, right), (up, left))
    ring_from = (left, right)
    step_of = (1, -1)
    pair = (2 * z + 1 - core, down)
    others = [(up, right), (up, left), (up, diag)]
    can_go = (z < levels - 1, z > 0)
    last = levels - 1
    at_end = jnp.logical_or(z == 0, z == last)
    inside = lambda level: jnp.logical_and(level >= 0, level < levels)
    levels_of = [(2 * ((z + i) % levels) + core, down) for i in range(1, levels)]

    barrier = pltpu.get_barrier_semaphore()
    for dev in (*others, pair, *levels_of):
        pl.semaphore_signal(barrier, inc=1, device_id=dev, device_id_type=MESH)

    loads = [
        pltpu.make_async_copy(downb_in, downb, load_sem.at[0]),
        pltpu.make_async_copy(enc, enc_raw, load_sem.at[1]),
        pltpu.make_async_copy(grads, grad_raw, load_sem.at[2]),
        pltpu.make_async_copy(dec, dec_all.at[down], load_sem.at[3]),
        pltpu.make_async_copy(upb_in, upb, load_sem.at[4]),
        pltpu.make_async_copy(deltas, del_raw, load_sem.at[5]),
    ]
    for copy in loads:
        copy.start()

    def remote(src, dst, kind, recv, dev):
        return pltpu.make_async_remote_copy(
            src, dst, send_sem.at[kind], recv, device_id=dev, device_id_type=MESH)

    def dec_half(r, i, owner):
        m = (i + r) % 2
        ref = dec_all.at[owner, m * part:(m + 1) * part]
        return remote(ref, ref, 0, dec_recv.at[r, i], ring_to[r])

    def dec_relay(r, i, owner):
        ref = dec_all.at[owner, r * part + i * piece:r * part + (i + 1) * piece]
        return remote(ref, ref, 0, dec_recv.at[r, 2 + i], ring_to[r])

    def enc_rows(level, c):
        return pl.ds(pl.multiple_of((level * 2 + c) * height, 16), height)

    def enc_a(level, c):
        return pl.ds(pl.multiple_of((level * 2 + c) * height + (1 - c) * TAIL, 16), height - TAIL)

    def enc_b(level, c):
        return pl.ds(pl.multiple_of((level * 2 + c) * height + c * (height - TAIL), 16), TAIL)

    def enc_copy(r, level, h, where, sem):
        ref = enc_all.at[h, where(level, core)]
        return remote(ref, ref, 1, enc_recv.at[sem], (up + 2 * step_of[r], down))

    def pair_copy(ref, sem):
        return remote(ref, ref, 2, pair_recv.at[sem], pair)

    def del_copy(dev):
        ref = del_all.at[down]
        return remote(ref, ref, 3, del_recv.at[0], dev)

    def grad_rows(level, c):
        return grad_all.at[pl.ds(pl.multiple_of((level * 2 + c) * toks, toks), toks)]

    def grad_copy(dev):
        ref = grad_rows(z, core)
        return remote(ref, ref, 4, grad_recv.at[0], dev)

    def pair_grad(level):
        ref = grad_rows(level, core)
        return remote(ref, ref, 5, grad_recv.at[1], pair)

    def pick_enc(h):
        for s in range(h * dact // 2, (h + 1) * dact // 2):
            at = s * BLOCK - h * half
            enc_all[h, pl.ds(pl.multiple_of(up * height, 16), height), at:at + BLOCK] = pick(
                enc_raw, slice(0, height), downb[s], blocks)

    loads[0].wait()
    loads[2].wait()
    for s in range(dact):
        grad_all[pl.ds(pl.multiple_of(up * toks, toks), toks), s * BLOCK:(s + 1) * BLOCK] = pick(
            grad_raw, slice(0, toks), downb[s], blocks)
    loads[1].wait()
    pick_enc(0)
    pl.semaphore_wait(barrier, len(others) + 1 + len(levels_of))

    def send_enc(h):
        for r in range(2):
            @pl.when(can_go[r])
            def _():
                enc_copy(r, z, h, enc_rows, 2 * z + h).start()

    for dev in levels_of:
        grad_copy(dev).start()
    send_enc(0)
    loads[3].wait()
    for i in range(2):
        for r in range(2):
            dec_half(r, i, down).start()
    pick_enc(1)
    send_enc(1)
    pair_copy(enc_all.at[:, enc_rows(z, core)], z).start()
    loads[4].wait()
    loads[5].wait()
    for w in range(wins):
        for s in range(uact):
            del_all[down, w, :, s * BLOCK:(s + 1) * BLOCK] = pick(
                del_raw, slice(w * win, (w + 1) * win), upb[s, down * wins + w], rows // BLOCK)
    for dev in others:
        del_copy(dev).start()

    acc[...] = jnp.zeros_like(acc)

    def mult(q, rs, n):
        acc[n, rs] += jnp.dot(
            dec_all[q, rs, :], enc_all[n, pl.ds(pl.multiple_of(q * depth, 128), depth), :],
            preferred_element_type=F32)

    def enc_stage(q, n):
        gap = jnp.maximum(q - z, z - q)
        return jnp.where(gap == last, 5 + n, 2 * gap)

    def products(low, high):
        @pl.loop(0, 4 * levels)
        def _(u):
            q, m, n = u // 4, u // 2 % 2, u % 2
            first = jnp.where(jnp.where(q == left, 1, 0) + m == 1, 2, 4)
            stage = jnp.maximum(enc_stage(q, n), jnp.where(q == down, 0, first))
            ready = jnp.logical_and(stage >= low, stage <= high)

            @pl.when(jnp.logical_and(ready, q != diag))
            def _():
                mult(q, pl.ds(pl.multiple_of(m * part, part), part), n)

    def diag_products(i):
        @pl.loop(0, 4)
        def _(u):
            m, n = u // 2, u % 2

            @pl.when(enc_stage(diag, n) <= 5)
            def _():
                mult(diag, pl.ds(pl.multiple_of(m * part + i * piece, piece), piece), n)

    def pair_whole(level):
        return pair_copy(enc_all.at[:, enc_rows(level, 1 - core)], level)

    def each(j, act):
        for r in range(2):
            level = z - step_of[r] * j

            @pl.when(inside(level))
            def _():
                act(r, level)

    def relay(j, h):
        def act(r, level):
            enc_copy(r, level, h, enc_rows, 2 * level + h).wait_recv()

            @pl.when(can_go[r])
            def _():
                if j == last - 1 and h == 1:
                    enc_copy(r, level, h, enc_a, 2 * level + h).start()
                    enc_copy(r, level, h, enc_b, 2 * levels).start()
                else:
                    enc_copy(r, level, h, enc_rows, 2 * level + h).start()
            if h == 1:
                pair_copy(enc_all.at[:, enc_rows(level, core)], level).start()
        each(j, act)

    relay(1, 0)
    pltpu.make_async_copy(
        grad_all.at[pl.ds(0, (levels - 1) * toks)], grad_all.at[pl.ds(0, (levels - 1) * toks)], grad_recv.at[0]).wait()
    for level in range(levels):
        pair_grad(level).start()
    relay(1, 1)
    for r in range(2):
        dec_half(r, 0, ring_from[r]).wait_recv()
        for i in range(2):
            dec_relay(r, i, ring_from[r]).start()
    pair_whole(z).wait_recv()
    each(1, lambda r, level: pair_whole(level).wait_recv())
    products(0, 2)
    relay(2, 0)

    pltpu.make_async_copy(
        del_all.at[pl.ds(0, n_down - 1)], del_all.at[pl.ds(0, n_down - 1)], del_recv.at[0]).wait()
    pltpu.make_async_copy(
        grad_all.at[pl.ds(0, levels * toks)], grad_all.at[pl.ds(0, levels * toks)], grad_recv.at[1]).wait()
    for d in range(n_down):
        for w in range(wins):
            for b in range(rows // BLOCK):
                value = jnp.zeros((win, BLOCK), masked.dtype)
                for s in range(uact):
                    on = flag(upb[s, d * wins + w], b, masked.dtype)
                    value = value + del_all[d, w, :, s * BLOCK:(s + 1) * BLOCK] * on
                t = (d * wins + w) * win
                masked[t:t + win, b * BLOCK:(b + 1) * BLOCK] = value
    prod[...] = lax.dot_general(
        masked[...], grad_all[...], (((0,), (0,)), ((), ())), preferred_element_type=F32)

    relay(2, 1)
    for r in range(2):
        dec_half(r, 1, ring_from[r]).wait_recv()
    each(2, lambda r, level: pair_whole(level).wait_recv())
    products(3, 4)

    far = last - z

    def end_wait(h, where, sem):
        for r in range(2):
            @pl.when(z == (0 if r else last))
            def _():
                enc_copy(r, far, h, where, sem).wait_recv()

    @pl.when(at_end)
    def _():
        end_wait(0, enc_rows, 2 * far)
        pair_copy(enc_all.at[0, enc_rows(far, core)], far).start()
    for r in range(2):
        dec_relay(r, 0, diag).wait_recv()

    @pl.when(at_end)
    def _():
        pair_copy(enc_all.at[0, enc_rows(far, 1 - core)], far).wait_recv()
    products(5, 5)
    diag_products(0)

    def mult_end(start, size):
        ks = pl.ds(pl.multiple_of(start, BLOCK), size)
        acc[1] += jnp.dot(
            dec_all[far, :, ks], enc_all[1, pl.ds(pl.multiple_of(far * depth + start, BLOCK), size), :],
            preferred_element_type=F32)

    @pl.when(at_end)
    def _():
        end_wait(1, enc_a, 2 * far + 1)
        pair_copy(enc_all.at[1, enc_a(far, core)], levels).start()
        end_wait(1, enc_b, 2 * levels)
        pair_copy(enc_all.at[1, enc_b(far, core)], levels + 1).start()
    for r in range(2):
        dec_relay(r, 1, diag).wait_recv()
    diag_products(1)

    @pl.when(at_end)
    def _():
        pair_copy(enc_all.at[1, enc_a(far, 1 - core)], levels).wait_recv()
        mult_end(TAIL, depth - 2 * TAIL)
        mult_end(core * (depth - TAIL), TAIL)
        pair_copy(enc_all.at[1, enc_b(far, 1 - core)], levels + 1).wait_recv()
        mult_end((1 - core) * (depth - TAIL), TAIL)

    tile = 64

    @pl.loop(0, rows // tile)
    def _(t):
        rs = pl.ds(pl.multiple_of(t * tile, tile), tile)
        values = []
        for s in range(dact):
            side, at = divmod(s * BLOCK, half)
            values.append(acc[side, rs, at:at + BLOCK] * prod[rs, s * BLOCK:(s + 1) * BLOCK])
        for c in range(blocks):
            total = None
            for s in range(dact):
                term = values[s] * flag(downb[s], c, F32)
                total = term if total is None else total + term
            out[rs, c * BLOCK:(c + 1) * BLOCK] = total

    def sent(ref, kind):
        pltpu.make_async_copy(ref, ref, send_sem.at[kind]).wait()

    sent(dec_all.at[pl.ds(0, 3)], 0)

    @pl.when(at_end)
    def _():
        sent(enc_all.at[:, pl.ds(0, height)], 1)

    @pl.when(jnp.logical_not(at_end))
    def _():
        sent(enc_all.at[:, pl.ds(0, (levels + 1) * height)], 1)
    sent(enc_all.at[:, pl.ds(0, levels * height)], 2)
    sent(del_all.at[pl.ds(0, n_down - 1)], 3)
    sent(grad_all.at[pl.ds(0, (levels - 1) * toks)], 4)
    sent(grad_all.at[pl.ds(0, levels * toks)], 5)


def ring_local(n_up, n_down, win, deltas, gradients, up_blocks, down_blocks, decoder, encoder):
    rows, depth = decoder.shape
    height, cols = encoder.shape
    toks = gradients.shape[0]
    uact, dact = up_blocks.shape[1], down_blocks.shape[0]
    tokens = deltas.shape[0] * n_down
    wins = deltas.shape[0] // win
    used = dact * BLOCK
    levels = n_up // 2
    kind = decoder.dtype
    dma = pltpu.SemaphoreType.DMA
    hbm = pl.BlockSpec(memory_space=pltpu.HBM)
    return pl.pallas_call(
        functools.partial(gather_scores, n_up, n_down),
        out_shape=jax.ShapeDtypeStruct((rows, cols), F32),
        in_specs=[hbm] * 6,
        out_specs=pl.BlockSpec(memory_space=pltpu.VMEM),
        scratch_shapes=[
            pltpu.SMEM((uact, up_blocks.shape[0]), jnp.int32),
            pltpu.SMEM((dact,), jnp.int32),
            pltpu.VMEM((n_down, rows, depth), kind),
            pltpu.VMEM((height, cols), kind),
            pltpu.VMEM((2, n_up * height, used // 2), kind),
            pltpu.VMEM(deltas.shape, kind),
            pltpu.VMEM((n_down, wins, win, uact * BLOCK), kind),
            pltpu.VMEM((toks, cols), kind),
            pltpu.VMEM((n_up * toks, used), kind),
            pltpu.VMEM((tokens, rows), kind),
            pltpu.VMEM((2, rows, used // 2), F32),
            pltpu.VMEM((rows, used), F32),
            dma((6,)),
            dma((6,)),
            dma((2, 4)),
            dma((1,)),
            dma((2 * levels + 1,)),
            dma((levels + 2,)),
            dma((2,)),
        ],
        compiler_params=pltpu.CompilerParams(collective_id=0, has_side_effects=True, vmem_limit_bytes=LARGE),
        name="gather_scores",
    )(*[pltpu.with_memory_space_constraint(x, pltpu.HBM) for x in (up_blocks.T, down_blocks, deltas, gradients, decoder, encoder)])


def plain_local(deltas, gradients, up_blocks, down_blocks, decoder, encoder):
    token_deltas = lax.all_gather(deltas, "down", axis=0, tiled=True)
    token_grads = lax.all_gather(gradients, "up", axis=0, tiled=True)
    tokens, rows = token_deltas.shape
    windows, dact = up_blocks.shape[0], down_blocks.shape[0]
    row_blocks, col_blocks = rows // BLOCK, encoder.shape[1] // BLOCK
    local_ids = jnp.arange(row_blocks, dtype=jnp.int32)
    block_on = jnp.any(up_blocks[:, :, None] == local_ids[None, None, :], axis=1)
    masked = token_deltas.reshape(windows, tokens // windows, row_blocks, BLOCK) * block_on[
        :, None, :, None].astype(token_deltas.dtype)
    masked = masked.reshape(tokens, rows)
    dec_whole = lax.all_gather(decoder, "down", axis=1, tiled=True)
    height = encoder.shape[0]
    enc_used = jnp.take(encoder.reshape(height, col_blocks, BLOCK), down_blocks, axis=1).reshape(height, dact * BLOCK)
    virtual = jnp.dot(dec_whole, lax.all_gather(enc_used, "up", axis=0, tiled=True), preferred_element_type=F32)
    grad_used = jnp.take(token_grads.reshape(tokens, col_blocks, BLOCK), down_blocks, axis=1).reshape(tokens, dact * BLOCK)
    product = lax.dot_general(masked, grad_used, (((0,), (0,)), ((), ())), preferred_element_type=F32)
    scored = (product * virtual).reshape(rows, dact, BLOCK)
    filled = jnp.zeros((rows, col_blocks, BLOCK), F32).at[:, down_blocks, :].set(scored)
    return filled.reshape(rows, encoder.shape[1])


def solution(mesh):
    n_up, n_down = mesh.shape["up"], mesh.shape["down"]
    ringed = n_down == 4 and n_up == 2 * n_down

    def local(deltas, gradients, up_blocks, down_blocks, decoder, encoder):
        args = (deltas, gradients, up_blocks, down_blocks, decoder, encoder)
        tokens = deltas.shape[0] * n_down
        win = tokens // up_blocks.shape[0]
        if ringed and deltas.shape[0] == 2 * win:
            return ring_local(n_up, n_down, win, *args)
        return plain_local(*args)

    placed = (P("down", "up"), P("up", "down"), P(None, "up"), P("down"), P("up", "down"), P("up", "down"))
    return jax.shard_map(local, mesh=mesh, in_specs=placed, out_specs=P("up", "down"), check_vma=False)
```

```python
import functools

import jax
import jax.numpy as jnp
from jax import lax
from jax.experimental import pallas as pl
from jax.experimental.pallas import tpu as pltpu
from jax.sharding import PartitionSpec as P

BLOCK = 128
TAIL = 256
LARGE = 24 << 20
MESH = pl.DeviceIdType.MESH
F32 = jnp.float32


def flag(number, block, kind):
    return jnp.where(jnp.full((1, BLOCK), number, jnp.int32) == block, 1.0, 0.0).astype(kind)


def pick(ref, rows, number, blocks):
    total = None
    for b in range(blocks):
        term = ref[rows, b * BLOCK:(b + 1) * BLOCK] * flag(number, b, ref.dtype)
        total = term if total is None else total + term
    return total


def block(number):
    return pl.ds(pl.multiple_of(number * BLOCK, BLOCK), BLOCK)


def hits_of(number, slots):
    return [1 - jnp.minimum(jnp.abs(slot - number), 1) for slot in slots]


def gather_scores(
    n_up, n_down, upb_in, downb_in, deltas, grads, dec, enc, out,
    upb, downb, dec_all, enc_raw, enc_all, del_raw, del_all, grad_raw, grad_all, masked, acc, prod,
    load_sem, send_sem, dec_recv, del_recv, enc_recv, pair_recv, grad_recv, pg_recv, ready,
):
    levels = n_up // 2
    rows, depth = dec.shape
    height = enc.shape[0]
    half = enc_all.shape[2]
    part = rows // 2
    body = depth - TAIL
    toks = grads.shape[0]
    wins = del_all.shape[1]
    win = del_all.shape[2]
    uact = upb.shape[0]
    dact = downb.shape[0]
    blocks = enc.shape[1] // BLOCK
    up, down = lax.axis_index("up"), lax.axis_index("down")
    z, core = up // 2, up % 2
    place = lambda d: 2 * (d // 2) + (d + d // 2) % 2
    pos = place(down)
    right, left = place((pos + 1) % 4), place((pos + 3) % 4)
    diag = place((pos + 2) % 4)
    ring_to = ((up, right), (up, left))
    ring_from = (left, right)
    step_of = (1, -1)
    pair = (2 * z + 1 - core, down)
    others = [(up, right), (up, left), (up, diag)]
    can_go = (z < levels - 1, z > 0)
    last = levels - 1
    at_end = jnp.logical_or(z == 0, z == last)
    inside = lambda level: jnp.logical_and(level >= 0, level < levels)
    low, high = levels // 2 - 1, levels // 2
    above = jnp.logical_and(z < last, z != low)
    below = jnp.logical_and(z > 0, z != high)

    barrier = pltpu.get_barrier_semaphore()
    for dev in (*others, pair):
        pl.semaphore_signal(barrier, inc=1, device_id=dev, device_id_type=MESH)

    @pl.when(z < last)
    def _():
        pl.semaphore_signal(barrier, inc=1, device_id=(up + 2, down), device_id_type=MESH)

    @pl.when(below)
    def _():
        pl.semaphore_signal(barrier, inc=1, device_id=(up - 2, down), device_id_type=MESH)

    loads = [
        pltpu.make_async_copy(downb_in, downb, load_sem.at[0]),
        pltpu.make_async_copy(grads, grad_raw, load_sem.at[1]),
        pltpu.make_async_copy(enc, enc_raw, load_sem.at[2]),
        pltpu.make_async_copy(dec, dec_all.at[down], load_sem.at[3]),
        pltpu.make_async_copy(upb_in, upb, load_sem.at[4]),
        pltpu.make_async_copy(deltas, del_raw, load_sem.at[5]),
    ]
    for copy in loads:
        copy.start()

    def remote(src, dst, kind, recv, dev):
        return pltpu.make_async_remote_copy(
            src, dst, send_sem.at[kind], recv, device_id=dev, device_id_type=MESH)

    def dec_half(r, i, owner):
        m = (i + r) % 2
        ref = dec_all.at[owner, m * part:(m + 1) * part]
        return remote(ref, ref, 0, dec_recv.at[r, i], ring_to[r])

    def dec_relay(r, i, owner):
        ref = dec_all.at[owner, r * part:(r + 1) * part, (body if i else 0):(depth if i else body)]
        return remote(ref, ref, 0, dec_recv.at[r, 2 + i], ring_to[r])

    def enc_rows(level, c):
        return pl.ds(pl.multiple_of((level * 2 + c) * height, 16), height)

    def enc_a(level, c):
        return pl.ds(pl.multiple_of((level * 2 + c) * height + (1 - c) * TAIL, 16), height - TAIL)

    def enc_b(level, c):
        return pl.ds(pl.multiple_of((level * 2 + c) * height + c * (height - TAIL), 16), TAIL)

    def enc_copy(r, level, h, where, sem):
        ref = enc_all.at[h, where(level, core)]
        return remote(ref, ref, 1, enc_recv.at[sem], (up + 2 * step_of[r], down))

    def pair_copy(ref, sem):
        return remote(ref, ref, 2, pair_recv.at[sem], pair)

    def del_copy(dev):
        ref = del_all.at[down]
        return remote(ref, ref, 3, del_recv.at[0], dev)

    def grad_rows(level, c):
        return grad_all.at[pl.ds(pl.multiple_of((level * 2 + c) * toks, toks), toks)]

    def grad_copy(r, level):
        ref = grad_rows(level, core)
        return remote(ref, ref, 4, grad_recv.at[level], (up + 2 * step_of[r], down))

    def pair_grad(level):
        ref = grad_rows(level, core)
        return remote(ref, ref, 5, pg_recv.at[0], pair)

    def pick_enc(h):
        for s in range(h * dact // 2, (h + 1) * dact // 2):
            at = s * BLOCK - h * half
            enc_all[h, pl.ds(pl.multiple_of(up * height, 16), height), at:at + BLOCK] = pick(enc_raw, slice(0, height), downb[s], blocks)

    loads[0].wait()
    loads[1].wait()
    for s in range(dact):
        grad_all[pl.ds(pl.multiple_of(up * toks, toks), toks), s * BLOCK:(s + 1) * BLOCK] = pick(grad_raw, slice(0, toks), downb[s], blocks)
    pl.semaphore_wait(barrier, len(others) + 1 + jnp.where(z > 0, 1, 0) + jnp.where(above, 1, 0))

    @pl.when(z == high)
    def _():
        pl.semaphore_signal(ready, inc=1, device_id=(up - 2, down), device_id_type=MESH)

    early = (above, z > 0)

    def send_own(which, act):
        for r in (1, 0):
            @pl.when(which[r])
            def _():
                act(r)

    send_own(early, lambda r: grad_copy(r, z).start())
    loads[2].wait()
    pick_enc(0)
    send_own(early, lambda r: enc_copy(r, z, 0, enc_rows, 2 * z).start())
    loads[3].wait()
    for r in range(2):
        dec_half(r, 0, down).start()
    pick_enc(1)
    pair_copy(enc_all.at[:, enc_rows(z, core)], z).start()
    loads[4].wait()
    loads[5].wait()
    for w in range(wins):
        for s in range(uact):
            del_all[down, w, :, s * BLOCK:(s + 1) * BLOCK] = pick(
                del_raw, slice(w * win, (w + 1) * win), upb[s, down * wins + w], rows // BLOCK)
    for dev in others:
        del_copy(dev).start()
    for r in range(2):
        dec_half(r, 1, down).start()

    def each(j, act):
        for r in range(2):
            level = z - step_of[r] * j

            @pl.when(inside(level))
            def _():
                act(r, level)

    def relay_grad(r, level):
        grad_copy(r, level).wait_recv()

        @pl.when(can_go[r])
        def _():
            grad_copy(r, level).start()
        pair_grad(level).start()

    @pl.when(z == low)
    def _():
        pl.semaphore_wait(ready, 1)
        grad_copy(0, z).start()
        enc_copy(0, z, 0, enc_rows, 2 * z).start()
    pair_grad(z).start()
    each(1, relay_grad)
    send_own(can_go, lambda r: enc_copy(r, z, 1, enc_rows, 2 * z + 1).start())

    acc[...] = jnp.zeros_like(acc)

    def mult(q, rs, n, start=0, size=depth):
        ks = pl.ds(pl.multiple_of(start, BLOCK), size)
        acc[n, rs] += jnp.dot(
            dec_all[q, rs, ks], enc_all[n, pl.ds(pl.multiple_of(q * depth + start, BLOCK), size), :],
            preferred_element_type=F32)

    def enc_stage(q, n):
        gap = jnp.maximum(q - z, z - q)
        return jnp.where(gap == last, 5 + n, 2 * gap)

    def products(low, high):
        @pl.loop(0, 4 * levels)
        def _(u):
            q, m, n = u // 4, u // 2 % 2, u % 2
            first = jnp.where(jnp.where(q == left, 1, 0) + m == 1, 2, 4)
            stage = jnp.maximum(enc_stage(q, n), jnp.where(q == down, 0, first))
            ready = jnp.logical_and(stage >= low, stage <= high)

            @pl.when(jnp.logical_and(ready, q != diag))
            def _():
                mult(q, pl.ds(pl.multiple_of(m * part, part), part), n)

    everything = slice(0, rows)

    def diag_products(i):
        for n in range(2):
            @pl.when(enc_stage(diag, n) <= 5)
            def _():
                mult(diag, everything, n, body if i else 0, TAIL if i else body)

    def pair_whole(level):
        return pair_copy(enc_all.at[:, enc_rows(level, 1 - core)], level)

    def relay(j, h):
        def act(r, level):
            enc_copy(r, level, h, enc_rows, 2 * level + h).wait_recv()

            @pl.when(can_go[r])
            def _():
                if j == last - 1 and h == 1:
                    enc_copy(r, level, h, enc_a, 2 * level + h).start()
                    enc_copy(r, level, h, enc_b, 2 * levels).start()
                else:
                    enc_copy(r, level, h, enc_rows, 2 * level + h).start()
            if h == 1:
                pair_copy(enc_all.at[:, enc_rows(level, core)], level).start()
        each(j, act)

    relay(1, 0)
    each(2, relay_grad)
    relay(1, 1)
    for r in range(2):
        dec_half(r, 0, ring_from[r]).wait_recv()
        for i in range(2):
            dec_relay(r, i, ring_from[r]).start()
    pair_whole(z).wait_recv()
    each(1, lambda r, level: pair_whole(level).wait_recv())
    products(0, 2)
    each(3, relay_grad)
    relay(2, 0)

    pltpu.make_async_copy(
        del_all.at[pl.ds(0, n_down - 1)], del_all.at[pl.ds(0, n_down - 1)], del_recv.at[0]).wait()
    pltpu.make_async_copy(
        grad_all.at[pl.ds(0, levels * toks)], grad_all.at[pl.ds(0, levels * toks)], pg_recv.at[0]).wait()
    for d in range(n_down):
        for w in range(wins):
            for b in range(rows // BLOCK):
                value = jnp.zeros((win, BLOCK), masked.dtype)
                for s in range(uact):
                    on = flag(upb[s, d * wins + w], b, masked.dtype)
                    value = value + del_all[d, w, :, s * BLOCK:(s + 1) * BLOCK] * on
                t = (d * wins + w) * win
                masked[t:t + win, b * BLOCK:(b + 1) * BLOCK] = value
    prod[:, dact * BLOCK:] = jnp.zeros((rows, BLOCK), F32)
    prod[:, :dact * BLOCK] = lax.dot_general(
        masked[...], grad_all[...], (((0,), (0,)), ((), ())), preferred_element_type=F32)

    relay(2, 1)
    for r in range(2):
        dec_half(r, 1, ring_from[r]).wait_recv()
    each(2, lambda r, level: pair_whole(level).wait_recv())
    products(3, 4)

    far = last - z

    def end_wait(h, where, sem):
        for r in range(2):
            @pl.when(z == (0 if r else last))
            def _():
                enc_copy(r, far, h, where, sem).wait_recv()

    @pl.when(at_end)
    def _():
        end_wait(0, enc_rows, 2 * far)
        pair_copy(enc_all.at[0, enc_rows(far, core)], far).start()
        pair_copy(enc_all.at[0, enc_rows(far, 1 - core)], far).wait_recv()

        @pl.when(far != diag)
        def _():
            mult(far, everything, 0)
        end_wait(1, enc_a, 2 * far + 1)
        pair_copy(enc_all.at[1, enc_a(far, core)], levels).start()
    for r in range(2):
        dec_relay(r, 0, diag).wait_recv()
    diag_products(0)

    @pl.when(at_end)
    def _():
        pair_copy(enc_all.at[1, enc_a(far, 1 - core)], levels).wait_recv()
        mult(far, everything, 1, TAIL, depth - 2 * TAIL)
    for r in range(2):
        dec_relay(r, 1, diag).wait_recv()
    diag_products(1)

    @pl.when(at_end)
    def _():
        end_wait(1, enc_b, 2 * levels)
        pair_copy(enc_all.at[1, enc_b(far, core)], levels + 1).start()
        mult(far, everything, 1, core * body, TAIL)
        pair_copy(enc_all.at[1, enc_b(far, 1 - core)], levels + 1).wait_recv()
        mult(far, everything, 1, (1 - core) * body, TAIL)

    tile = 64
    @pl.loop(0, rows // tile)
    def _(t):
        rs = pl.ds(pl.multiple_of(t * tile, tile), tile)
        values = []
        for s in range(dact):
            side, at = divmod(s * BLOCK, half)
            values.append(acc[side, rs, at:at + BLOCK] * prod[rs, s * BLOCK:(s + 1) * BLOCK])
        for c in range(blocks):
            total = None
            for s in range(dact):
                term = values[s] * flag(downb[s], c, F32)
                total = term if total is None else total + term
            out[rs, c * BLOCK:(c + 1) * BLOCK] = total

    def sent(ref, kind):
        pltpu.make_async_copy(ref, ref, send_sem.at[kind]).wait()

    sent(dec_all.at[pl.ds(0, 3)], 0)

    @pl.when(at_end)
    def _():
        sent(enc_all.at[:, pl.ds(0, height)], 1)
        sent(grad_all.at[pl.ds(0, toks)], 4)

    @pl.when(jnp.logical_not(at_end))
    def _():
        sent(enc_all.at[:, pl.ds(0, (levels + 1) * height)], 1)
        sent(grad_all.at[pl.ds(0, (levels + 1) * toks)], 4)
    sent(enc_all.at[:, pl.ds(0, levels * height)], 2)
    sent(del_all.at[pl.ds(0, n_down - 1)], 3)
    sent(grad_all.at[pl.ds(0, levels * toks)], 5)


def ring_local(n_up, n_down, win, deltas, gradients, up_blocks, down_blocks, decoder, encoder):
    rows, depth = decoder.shape
    height, cols = encoder.shape
    toks = gradients.shape[0]
    uact, dact = up_blocks.shape[1], down_blocks.shape[0]
    tokens = deltas.shape[0] * n_down
    wins = deltas.shape[0] // win
    used = dact * BLOCK
    levels = n_up // 2
    kind = decoder.dtype
    dma = pltpu.SemaphoreType.DMA
    hbm = pl.BlockSpec(memory_space=pltpu.HBM)
    return pl.pallas_call(
        functools.partial(gather_scores, n_up, n_down),
        out_shape=jax.ShapeDtypeStruct((rows, cols), F32),
        in_specs=[hbm] * 6,
        out_specs=pl.BlockSpec(memory_space=pltpu.VMEM),
        scratch_shapes=[
            pltpu.SMEM((uact, up_blocks.shape[0]), jnp.int32),
            pltpu.SMEM((dact,), jnp.int32),
            pltpu.VMEM((n_down, rows, depth), kind),
            pltpu.VMEM((height, cols), kind),
            pltpu.VMEM((2, n_up * height, used // 2), kind),
            pltpu.VMEM(deltas.shape, kind),
            pltpu.VMEM((n_down, wins, win, uact * BLOCK), kind),
            pltpu.VMEM((toks, cols), kind),
            pltpu.VMEM((n_up * toks, used), kind),
            pltpu.VMEM((tokens, rows), kind),
            pltpu.VMEM((2, rows, used // 2), F32),
            pltpu.VMEM((rows, used + BLOCK), F32),
            dma((6,)),
            dma((6,)),
            dma((2, 4)),
            dma((1,)),
            dma((2 * levels + 1,)),
            dma((levels + 2,)),
            dma((levels,)),
            dma((1,)),
            pltpu.SemaphoreType.REGULAR,
        ],
        compiler_params=pltpu.CompilerParams(collective_id=0, has_side_effects=True, vmem_limit_bytes=LARGE),
        name="gather_scores",
    )(*[pltpu.with_memory_space_constraint(x, pltpu.HBM) for x in (up_blocks.T, down_blocks, deltas, gradients, decoder, encoder)])


def plain_local(deltas, gradients, up_blocks, down_blocks, decoder, encoder):
    token_deltas = lax.all_gather(deltas, "down", axis=0, tiled=True)
    token_grads = lax.all_gather(gradients, "up", axis=0, tiled=True)
    tokens, rows = token_deltas.shape
    windows, dact = up_blocks.shape[0], down_blocks.shape[0]
    row_blocks, col_blocks = rows // BLOCK, encoder.shape[1] // BLOCK
    local_ids = jnp.arange(row_blocks, dtype=jnp.int32)
    block_on = jnp.any(up_blocks[:, :, None] == local_ids[None, None, :], axis=1)
    masked = token_deltas.reshape(windows, tokens // windows, row_blocks, BLOCK) * block_on[
        :, None, :, None].astype(token_deltas.dtype)
    masked = masked.reshape(tokens, rows)
    dec_whole = lax.all_gather(decoder, "down", axis=1, tiled=True)
    height = encoder.shape[0]
    enc_used = jnp.take(encoder.reshape(height, col_blocks, BLOCK), down_blocks, axis=1).reshape(height, dact * BLOCK)
    virtual = jnp.dot(dec_whole, lax.all_gather(enc_used, "up", axis=0, tiled=True), preferred_element_type=F32)
    grad_used = jnp.take(token_grads.reshape(tokens, col_blocks, BLOCK), down_blocks, axis=1).reshape(tokens, dact * BLOCK)
    product = lax.dot_general(masked, grad_used, (((0,), (0,)), ((), ())), preferred_element_type=F32)
    scored = (product * virtual).reshape(rows, dact, BLOCK)
    filled = jnp.zeros((rows, col_blocks, BLOCK), F32).at[:, down_blocks, :].set(scored)
    return filled.reshape(rows, encoder.shape[1])


def solution(mesh):
    n_up, n_down = mesh.shape["up"], mesh.shape["down"]
    ringed = n_down == 4 and n_up == 2 * n_down

    def local(deltas, gradients, up_blocks, down_blocks, decoder, encoder):
        args = (deltas, gradients, up_blocks, down_blocks, decoder, encoder)
        tokens = deltas.shape[0] * n_down
        win = tokens // up_blocks.shape[0]
        if ringed and deltas.shape[0] == 2 * win:
            return ring_local(n_up, n_down, win, *args)
        return plain_local(*args)

    placed = (P("down", "up"), P("up", "down"), P(None, "up"), P("down"), P("up", "down"), P("up", "down"))
    return jax.shard_map(local, mesh=mesh, in_specs=placed, out_specs=P("up", "down"), check_vma=False)
```

```python
import functools

import jax
import jax.numpy as jnp
from jax import lax
from jax.experimental import pallas as pl
from jax.experimental.pallas import tpu as pltpu
from jax.sharding import PartitionSpec as P

BLOCK = 128
TAIL = 256
LARGE = 24 << 20
MESH = pl.DeviceIdType.MESH
F32 = jnp.float32


def flag(number, block, kind):
    return jnp.where(jnp.full((1, BLOCK), number, jnp.int32) == block, 1.0, 0.0).astype(kind)


def pick(ref, rows, number, blocks):
    total = None
    for b in range(blocks):
        term = ref[rows, b * BLOCK:(b + 1) * BLOCK] * flag(number, b, ref.dtype)
        total = term if total is None else total + term
    return total


def block(number):
    return pl.ds(pl.multiple_of(number * BLOCK, BLOCK), BLOCK)


def hits_of(number, slots):
    return [1 - jnp.minimum(jnp.abs(slot - number), 1) for slot in slots]


def gather_scores(
    n_up, n_down, upb_in, downb_in, deltas, grads, dec, enc, out,
    upb, downb, dec_all, enc_raw, enc_all, del_raw, del_all, grad_raw, grad_all, masked, acc, prod,
    load_sem, send_sem, dec_recv, del_recv, enc_recv, pair_recv, grad_recv, pg_recv, ready_z, ready_xy,
):
    levels = n_up // 2
    rows, depth = dec.shape
    height = enc.shape[0]
    half = enc_all.shape[2]
    part = rows // 2
    body = depth - TAIL
    toks = grads.shape[0]
    wins = del_all.shape[1]
    win = del_all.shape[2]
    uact = upb.shape[0]
    dact = downb.shape[0]
    blocks = enc.shape[1] // BLOCK
    up, down = lax.axis_index("up"), lax.axis_index("down")
    z, core = up // 2, up % 2
    place = lambda d: 2 * (d // 2) + (d + d // 2) % 2
    pos = place(down)
    right, left = place((pos + 1) % 4), place((pos + 3) % 4)
    diag = place((pos + 2) % 4)
    ring_to = ((up, right), (up, left))
    ring_from = (left, right)
    step_of = (1, -1)
    pair = (2 * z + 1 - core, down)
    others = [(up, right), (up, left), (up, diag)]
    can_go = (z < levels - 1, z > 0)
    last = levels - 1
    at_end = jnp.logical_or(z == 0, z == last)
    inside = lambda level: jnp.logical_and(level >= 0, level < levels)

    barrier = pltpu.get_barrier_semaphore()
    pl.semaphore_signal(barrier, inc=1, device_id=pair, device_id_type=MESH)

    def greet(sem, toward):
        for d in range(n_down):
            @pl.when(d > down if toward > 0 else d < down)
            def _():
                pl.semaphore_signal(ready_xy if sem is None else sem, inc=1, device_id=(up, d), device_id_type=MESH)

        @pl.when(z < last if toward > 0 else z > 0)
        def _():
            pl.semaphore_signal(ready_z if sem is None else sem, inc=1, device_id=(up + 2 * toward, down), device_id_type=MESH)

    greet(barrier, 1)
    loads = [
        pltpu.make_async_copy(downb_in, downb, load_sem.at[0]),
        pltpu.make_async_copy(grads, grad_raw, load_sem.at[1]),
        pltpu.make_async_copy(enc, enc_raw, load_sem.at[2]),
        pltpu.make_async_copy(dec, dec_all.at[down], load_sem.at[3]),
        pltpu.make_async_copy(upb_in, upb, load_sem.at[4]),
        pltpu.make_async_copy(deltas, del_raw, load_sem.at[5]),
    ]
    for copy in loads:
        copy.start()

    def remote(src, dst, kind, recv, dev):
        return pltpu.make_async_remote_copy(
            src, dst, send_sem.at[kind], recv, device_id=dev, device_id_type=MESH)

    def dec_half(r, i, owner):
        m = (i + r) % 2
        ref = dec_all.at[owner, m * part:(m + 1) * part]
        return remote(ref, ref, 0, dec_recv.at[r, i], ring_to[r])

    def dec_relay(r, i, owner):
        ref = dec_all.at[owner, r * part:(r + 1) * part, (body if i else 0):(depth if i else body)]
        return remote(ref, ref, 0, dec_recv.at[r, 2 + i], ring_to[r])

    def enc_rows(level, c):
        return pl.ds(pl.multiple_of((level * 2 + c) * height, 16), height)

    def enc_a(level, c):
        return pl.ds(pl.multiple_of((level * 2 + c) * height + (1 - c) * TAIL, 16), height - TAIL)

    def enc_b(level, c):
        return pl.ds(pl.multiple_of((level * 2 + c) * height + c * (height - TAIL), 16), TAIL)

    def enc_copy(r, level, h, where, sem):
        ref = enc_all.at[h, where(level, core)]
        return remote(ref, ref, 1, enc_recv.at[sem], (up + 2 * step_of[r], down))

    def pair_copy(ref, sem):
        return remote(ref, ref, 2, pair_recv.at[sem], pair)

    def del_copy(dev):
        ref = del_all.at[down]
        return remote(ref, ref, 3, del_recv.at[0], dev)

    def grad_rows(level, c):
        return grad_all.at[pl.ds(pl.multiple_of((level * 2 + c) * toks, toks), toks)]

    def grad_copy(r, level):
        ref = grad_rows(level, core)
        return remote(ref, ref, 4, grad_recv.at[level], (up + 2 * step_of[r], down))

    def pair_grad(level):
        ref = grad_rows(level, core)
        return remote(ref, ref, 5, pg_recv.at[0], pair)

    def pick_enc(h):
        for s in range(h * dact // 2, (h + 1) * dact // 2):
            at = s * BLOCK - h * half
            enc_all[h, pl.ds(pl.multiple_of(up * height, 16), height), at:at + BLOCK] = pick(enc_raw, slice(0, height), downb[s], blocks)

    loads[0].wait()
    loads[1].wait()
    for s in range(dact):
        grad_all[pl.ds(pl.multiple_of(up * toks, toks), toks), s * BLOCK:(s + 1) * BLOCK] = pick(grad_raw, slice(0, toks), downb[s], blocks)
    pl.semaphore_wait(barrier, 1 + down + jnp.where(z > 0, 1, 0))
    greet(None, -1)

    def send_own(act):
        for r in (1, 0):
            @pl.when(can_go[r])
            def _():
                act(r)

    @pl.when(z > 0)
    def _():
        grad_copy(1, z).start()
    loads[2].wait()
    pick_enc(0)

    @pl.when(z > 0)
    def _():
        enc_copy(1, z, 0, enc_rows, 2 * z).start()
    loads[3].wait()

    @pl.when(down < n_down - 1)
    def _():
        pl.semaphore_wait(ready_xy, n_down - 1 - down)
    for r in range(2):
        dec_half(r, 0, down).start()
    pick_enc(1)
    pair_copy(enc_all.at[:, enc_rows(z, core)], z).start()
    loads[4].wait()
    loads[5].wait()
    for w in range(wins):
        for s in range(uact):
            del_all[down, w, :, s * BLOCK:(s + 1) * BLOCK] = pick(
                del_raw, slice(w * win, (w + 1) * win), upb[s, down * wins + w], rows // BLOCK)
    for dev in others:
        del_copy(dev).start()
    for r in range(2):
        dec_half(r, 1, down).start()

    def each(j, act):
        for r in range(2):
            level = z - step_of[r] * j

            @pl.when(inside(level))
            def _():
                act(r, level)

    def relay_grad(r, level):
        grad_copy(r, level).wait_recv()

        @pl.when(can_go[r])
        def _():
            grad_copy(r, level).start()
        pair_grad(level).start()

    @pl.when(z < last)
    def _():
        pl.semaphore_wait(ready_z, 1)
        grad_copy(0, z).start()
        enc_copy(0, z, 0, enc_rows, 2 * z).start()
    pair_grad(z).start()
    each(1, relay_grad)
    send_own(lambda r: enc_copy(r, z, 1, enc_rows, 2 * z + 1).start())

    acc[...] = jnp.zeros_like(acc)

    def mult(q, rs, n, start=0, size=depth):
        ks = pl.ds(pl.multiple_of(start, BLOCK), size)
        result = jnp.dot(
            dec_all[q, rs, ks], enc_all[n, pl.ds(pl.multiple_of(q * depth + start, BLOCK), size), :],
            preferred_element_type=F32)
        for i in range(half // BLOCK):
            acc[n * (half // BLOCK) + i, rs] += result[:, i * BLOCK:(i + 1) * BLOCK]

    def enc_stage(q, n):
        gap = jnp.maximum(q - z, z - q)
        return jnp.where(gap == last, 5 + n, 2 * gap)

    def products(low, high):
        @pl.loop(0, 4 * levels)
        def _(u):
            q, m, n = u // 4, u // 2 % 2, u % 2
            first = jnp.where(jnp.where(q == left, 1, 0) + m == 1, 2, 4)
            stage = jnp.maximum(enc_stage(q, n), jnp.where(q == down, 0, first))
            ready = jnp.logical_and(stage >= low, stage <= high)

            @pl.when(jnp.logical_and(ready, q != diag))
            def _():
                mult(q, pl.ds(pl.multiple_of(m * part, part), part), n)

    everything = slice(0, rows)

    def diag_products(i):
        for n in range(2):
            @pl.when(enc_stage(diag, n) <= 5)
            def _():
                mult(diag, everything, n, body if i else 0, TAIL if i else body)

    def pair_whole(level):
        return pair_copy(enc_all.at[:, enc_rows(level, 1 - core)], level)

    def relay(j, h):
        def act(r, level):
            enc_copy(r, level, h, enc_rows, 2 * level + h).wait_recv()

            @pl.when(can_go[r])
            def _():
                if j == last - 1 and h == 1:
                    enc_copy(r, level, h, enc_a, 2 * level + h).start()
                    enc_copy(r, level, h, enc_b, 2 * levels).start()
                else:
                    enc_copy(r, level, h, enc_rows, 2 * level + h).start()
            if h == 1:
                pair_copy(enc_all.at[:, enc_rows(level, core)], level).start()
        each(j, act)

    relay(1, 0)
    each(2, relay_grad)
    relay(1, 1)
    for r in range(2):
        dec_half(r, 0, ring_from[r]).wait_recv()
        for i in range(2):
            dec_relay(r, i, ring_from[r]).start()
    pair_whole(z).wait_recv()
    each(1, lambda r, level: pair_whole(level).wait_recv())
    products(0, 2)
    each(3, relay_grad)
    relay(2, 0)

    pltpu.make_async_copy(
        del_all.at[pl.ds(0, n_down - 1)], del_all.at[pl.ds(0, n_down - 1)], del_recv.at[0]).wait()
    pltpu.make_async_copy(
        grad_all.at[pl.ds(0, levels * toks)], grad_all.at[pl.ds(0, levels * toks)], pg_recv.at[0]).wait()
    for d in range(n_down):
        for w in range(wins):
            for b in range(rows // BLOCK):
                value = jnp.zeros((win, BLOCK), masked.dtype)
                for s in range(uact):
                    on = flag(upb[s, d * wins + w], b, masked.dtype)
                    value = value + del_all[d, w, :, s * BLOCK:(s + 1) * BLOCK] * on
                t = (d * wins + w) * win
                masked[t:t + win, b * BLOCK:(b + 1) * BLOCK] = value
    whole = lax.dot_general(
        masked[...], grad_all[...], (((0,), (0,)), ((), ())), preferred_element_type=F32)
    for s in range(dact):
        prod[s] = whole[:, s * BLOCK:(s + 1) * BLOCK]
    prod[dact] = jnp.zeros((rows, BLOCK), F32)

    relay(2, 1)
    for r in range(2):
        dec_half(r, 1, ring_from[r]).wait_recv()
    each(2, lambda r, level: pair_whole(level).wait_recv())
    products(3, 4)

    far = last - z

    def end_wait(h, where, sem):
        for r in range(2):
            @pl.when(z == (0 if r else last))
            def _():
                enc_copy(r, far, h, where, sem).wait_recv()

    @pl.when(at_end)
    def _():
        end_wait(0, enc_rows, 2 * far)
        pair_copy(enc_all.at[0, enc_rows(far, core)], far).start()
        pair_copy(enc_all.at[0, enc_rows(far, 1 - core)], far).wait_recv()

        @pl.when(far != diag)
        def _():
            mult(far, everything, 0)
        end_wait(1, enc_a, 2 * far + 1)
        pair_copy(enc_all.at[1, enc_a(far, core)], levels).start()
    for r in range(2):
        dec_relay(r, 0, diag).wait_recv()
    diag_products(0)

    @pl.when(at_end)
    def _():
        pair_copy(enc_all.at[1, enc_a(far, 1 - core)], levels).wait_recv()
        mult(far, everything, 1, TAIL, depth - 2 * TAIL)
    for r in range(2):
        dec_relay(r, 1, diag).wait_recv()
    diag_products(1)

    @pl.when(at_end)
    def _():
        end_wait(1, enc_b, 2 * levels)
        pair_copy(enc_all.at[1, enc_b(far, core)], levels + 1).start()
        mult(far, everything, 1, core * body, TAIL)
        pair_copy(enc_all.at[1, enc_b(far, 1 - core)], levels + 1).wait_recv()
        mult(far, everything, 1, (1 - core) * body, TAIL)

    tile = 64
    places = []
    for c in range(blocks):
        hits = [1 - jnp.minimum(jnp.abs(downb[s] - c), 1) for s in range(dact)]
        slot = sum(s * hit for s, hit in enumerate(hits))
        factor = slot + dact * (1 - sum(hits))
        places.append((jnp.maximum(jnp.minimum(slot, dact - 1), 0), jnp.maximum(jnp.minimum(factor, dact), 0)))

    @pl.loop(0, rows // tile)
    def _(t):
        rs = pl.ds(pl.multiple_of(t * tile, tile), tile)
        for c, (slot, factor) in enumerate(places):
            out[rs, c * BLOCK:(c + 1) * BLOCK] = acc[slot, rs] * prod[factor, rs]

    def sent(ref, kind):
        pltpu.make_async_copy(ref, ref, send_sem.at[kind]).wait()

    sent(dec_all.at[pl.ds(0, 3)], 0)

    @pl.when(at_end)
    def _():
        sent(enc_all.at[:, pl.ds(0, height)], 1)
        sent(grad_all.at[pl.ds(0, toks)], 4)

    @pl.when(jnp.logical_not(at_end))
    def _():
        sent(enc_all.at[:, pl.ds(0, (levels + 1) * height)], 1)
        sent(grad_all.at[pl.ds(0, (levels + 1) * toks)], 4)
    sent(enc_all.at[:, pl.ds(0, levels * height)], 2)
    sent(del_all.at[pl.ds(0, n_down - 1)], 3)
    sent(grad_all.at[pl.ds(0, levels * toks)], 5)


def ring_local(n_up, n_down, win, deltas, gradients, up_blocks, down_blocks, decoder, encoder):
    rows, depth = decoder.shape
    height, cols = encoder.shape
    toks = gradients.shape[0]
    uact, dact = up_blocks.shape[1], down_blocks.shape[0]
    tokens = deltas.shape[0] * n_down
    wins = deltas.shape[0] // win
    used = dact * BLOCK
    levels = n_up // 2
    kind = decoder.dtype
    dma = pltpu.SemaphoreType.DMA
    hbm = pl.BlockSpec(memory_space=pltpu.HBM)
    return pl.pallas_call(
        functools.partial(gather_scores, n_up, n_down),
        out_shape=jax.ShapeDtypeStruct((rows, cols), F32),
        in_specs=[hbm] * 6,
        out_specs=pl.BlockSpec(memory_space=pltpu.VMEM),
        scratch_shapes=[
            pltpu.SMEM((uact, up_blocks.shape[0]), jnp.int32),
            pltpu.SMEM((dact,), jnp.int32),
            pltpu.VMEM((n_down, rows, depth), kind),
            pltpu.VMEM((height, cols), kind),
            pltpu.VMEM((2, n_up * height, used // 2), kind),
            pltpu.VMEM(deltas.shape, kind),
            pltpu.VMEM((n_down, wins, win, uact * BLOCK), kind),
            pltpu.VMEM((toks, cols), kind),
            pltpu.VMEM((n_up * toks, used), kind),
            pltpu.VMEM((tokens, rows), kind),
            pltpu.VMEM((dact, rows, BLOCK), F32),
            pltpu.VMEM((dact + 1, rows, BLOCK), F32),
            dma((6,)),
            dma((6,)),
            dma((2, 4)),
            dma((1,)),
            dma((2 * levels + 1,)),
            dma((levels + 2,)),
            dma((levels,)),
            dma((1,)),
            pltpu.SemaphoreType.REGULAR,
            pltpu.SemaphoreType.REGULAR,
        ],
        compiler_params=pltpu.CompilerParams(collective_id=0, has_side_effects=True, vmem_limit_bytes=LARGE),
        name="gather_scores",
    )(*[pltpu.with_memory_space_constraint(x, pltpu.HBM) for x in (up_blocks.T, down_blocks, deltas, gradients, decoder, encoder)])


def plain_local(deltas, gradients, up_blocks, down_blocks, decoder, encoder):
    token_deltas = lax.all_gather(deltas, "down", axis=0, tiled=True)
    token_grads = lax.all_gather(gradients, "up", axis=0, tiled=True)
    tokens, rows = token_deltas.shape
    windows, dact = up_blocks.shape[0], down_blocks.shape[0]
    row_blocks, col_blocks = rows // BLOCK, encoder.shape[1] // BLOCK
    local_ids = jnp.arange(row_blocks, dtype=jnp.int32)
    block_on = jnp.any(up_blocks[:, :, None] == local_ids[None, None, :], axis=1)
    masked = token_deltas.reshape(windows, tokens // windows, row_blocks, BLOCK) * block_on[
        :, None, :, None].astype(token_deltas.dtype)
    masked = masked.reshape(tokens, rows)
    dec_whole = lax.all_gather(decoder, "down", axis=1, tiled=True)
    height = encoder.shape[0]
    enc_used = jnp.take(encoder.reshape(height, col_blocks, BLOCK), down_blocks, axis=1).reshape(height, dact * BLOCK)
    virtual = jnp.dot(dec_whole, lax.all_gather(enc_used, "up", axis=0, tiled=True), preferred_element_type=F32)
    grad_used = jnp.take(token_grads.reshape(tokens, col_blocks, BLOCK), down_blocks, axis=1).reshape(tokens, dact * BLOCK)
    product = lax.dot_general(masked, grad_used, (((0,), (0,)), ((), ())), preferred_element_type=F32)
    scored = (product * virtual).reshape(rows, dact, BLOCK)
    filled = jnp.zeros((rows, col_blocks, BLOCK), F32).at[:, down_blocks, :].set(scored)
    return filled.reshape(rows, encoder.shape[1])


def solution(mesh):
    n_up, n_down = mesh.shape["up"], mesh.shape["down"]
    ringed = n_down == 4 and n_up == 2 * n_down

    def local(deltas, gradients, up_blocks, down_blocks, decoder, encoder):
        args = (deltas, gradients, up_blocks, down_blocks, decoder, encoder)
        tokens = deltas.shape[0] * n_down
        win = tokens // up_blocks.shape[0]
        if ringed and deltas.shape[0] == 2 * win:
            return ring_local(n_up, n_down, win, *args)
        return plain_local(*args)

    placed = (P("down", "up"), P("up", "down"), P(None, "up"), P("down"), P("up", "down"), P("up", "down"))
    return jax.shard_map(local, mesh=mesh, in_specs=placed, out_specs=P("up", "down"), check_vma=False)
```

```python
import functools

import jax
import jax.numpy as jnp
from jax import lax
from jax.experimental import pallas as pl
from jax.experimental.pallas import tpu as pltpu
from jax.sharding import PartitionSpec as P

BLOCK = 128
TAIL = 128
LARGE = 24 << 20
MESH = pl.DeviceIdType.MESH
F32 = jnp.float32


def flag(number, block, kind):
    return jnp.where(jnp.full((1, BLOCK), number, jnp.int32) == block, 1.0, 0.0).astype(kind)


def within(number, count):
    return jnp.maximum(jnp.minimum(number, count - 1), 0)


def hits_of(number, slots):
    return [1 - jnp.minimum(jnp.abs(slot - number), 1) for slot in slots]


def gather_scores(
    n_up, n_down, upb_in, downb_in, deltas, grads, dec, enc, out,
    upb, downb, dec_all, enc_raw, enc_all, del_raw, del_all, grad_raw, grad_all, masked, acc, prod,
    load_sem, send_sem, dec_recv, del_recv, enc_recv, pair_recv, grad_recv, pg_recv, ready_z, ready_xy,
):
    levels = n_up // 2
    rows, depth = dec.shape
    height = enc.shape[0]
    half = enc_all.shape[2]
    part = rows // 2
    body = depth - TAIL
    toks = grads.shape[0]
    wins, uact, win = del_all.shape[1:4]
    dact = downb.shape[0]
    blocks = enc.shape[1] // BLOCK
    up, down = lax.axis_index("up"), lax.axis_index("down")
    z, core = up // 2, up % 2
    place = lambda d: 2 * (d // 2) + (d + d // 2) % 2
    pos = place(down)
    right, left = place((pos + 1) % 4), place((pos + 3) % 4)
    diag = place((pos + 2) % 4)
    ring_to = ((up, right), (up, left))
    ring_from = (left, right)
    step_of = (1, -1)
    pair = (2 * z + 1 - core, down)
    can_go = (z < levels - 1, z > 0)
    last = levels - 1
    at_end = jnp.logical_or(z == 0, z == last)
    inside = lambda level: jnp.logical_and(level >= 0, level < levels)

    high = levels // 2
    later = jnp.where(right > down, 1, 0) + jnp.where(left > down, 1, 0)
    barrier = pltpu.get_barrier_semaphore()

    def signal(sem, dev, when=None):
        if when is None:
            pl.semaphore_signal(sem, inc=1, device_id=dev, device_id_type=MESH)
        else:
            pl.when(when)(lambda: pl.semaphore_signal(sem, inc=1, device_id=dev, device_id_type=MESH))

    signal(barrier, pair)
    signal(barrier, (up + 2, down), z < last)
    signal(barrier, (up - 2, down), z > high)
    for d in (right, left):
        signal(barrier, (up, d), d > down)

    def by_block(src, dst, sem):
        return [pltpu.make_async_copy(src.at[:, b * BLOCK:(b + 1) * BLOCK], dst.at[b], sem) for b in range(dst.shape[0])]

    def loaded(ref, sem):
        pltpu.make_async_copy(ref, ref, sem).wait()

    load_downb = pltpu.make_async_copy(downb_in, downb, load_sem.at[0])
    load_upb = pltpu.make_async_copy(upb_in, upb, load_sem.at[4])
    load_dec = pltpu.make_async_copy(dec, dec_all.at[down], load_sem.at[3])
    for copy in (
        load_downb, *by_block(grads, grad_raw, load_sem.at[1]), load_dec, *by_block(enc, enc_raw, load_sem.at[2]),
        load_upb, *by_block(deltas, del_raw, load_sem.at[5]),
    ):
        copy.start()

    def remote(src, dst, kind, recv, dev):
        return pltpu.make_async_remote_copy(
            src, dst, send_sem.at[kind], recv, device_id=dev, device_id_type=MESH)

    def dec_half(r, i, owner):
        m = (i + r) % 2
        ref = dec_all.at[owner, m * part:(m + 1) * part]
        return remote(ref, ref, 0, dec_recv.at[r, i], ring_to[r])

    def dec_relay(r, i, owner):
        ref = dec_all.at[owner, r * part:(r + 1) * part, (body if i else 0):(depth if i else body)]
        return remote(ref, ref, 0, dec_recv.at[r, 2 + i], ring_to[r])

    def enc_rows(level, c):
        return pl.ds(pl.multiple_of((level * 2 + c) * height, 16), height)

    def enc_a(level, c):
        return pl.ds(pl.multiple_of((level * 2 + c) * height + (1 - c) * TAIL, 16), height - TAIL)

    def enc_b(level, c):
        return pl.ds(pl.multiple_of((level * 2 + c) * height + c * (height - TAIL), 16), TAIL)

    def enc_copy(r, level, h, where, sem):
        ref = enc_all.at[h, where(level, core)]
        return remote(ref, ref, 1, enc_recv.at[sem], (up + 2 * step_of[r], down))

    def pair_copy(ref, sem):
        return remote(ref, ref, 2, pair_recv.at[sem], pair)

    def del_copy(r, owner):
        ref = del_all.at[owner]
        return remote(ref, ref, 3, del_recv.at[r], ring_to[r])

    def del_relay(r, owner):
        ref = del_all.at[owner, r]
        return remote(ref, ref, 3, del_recv.at[2], ring_to[r])

    def grad_rows(level, c):
        return grad_all.at[pl.ds(pl.multiple_of((level * 2 + c) * toks, toks), toks)]

    def grad_copy(r, level):
        ref = grad_rows(level, core)
        return remote(ref, ref, 4, grad_recv.at[level], (up + 2 * step_of[r], down))

    def pair_grad(level):
        ref = grad_rows(level, core)
        return remote(ref, ref, 5, pg_recv.at[0], pair)

    def pick_enc(h):
        for s in range(h * dact // 2, (h + 1) * dact // 2):
            at = s * BLOCK - h * half
            enc_all[h, pl.ds(pl.multiple_of(up * height, 16), height), at:at + BLOCK] = enc_raw[chosen[s]]

    load_downb.wait()
    chosen = [within(downb[s], blocks) for s in range(dact)]
    loaded(grad_raw, load_sem.at[1])
    for s in range(dact):
        grad_all[pl.ds(pl.multiple_of(up * toks, toks), toks), s * BLOCK:(s + 1) * BLOCK] = grad_raw[chosen[s]]
    pl.semaphore_wait(barrier, 3 - later + jnp.where(z > 0, 1, 0) + jnp.where(z >= high, 1, 0) - jnp.where(z == last, 1, 0))
    signal(ready_z, (up - 2, down), jnp.logical_and(z > 0, z <= high))
    for d in (right, left):
        signal(ready_xy, (up, d), d < down)

    early = (jnp.logical_and(z >= high, z < last), z > 0)

    def send_own(which, act):
        for r in (1, 0):
            @pl.when(which[r])
            def _():
                act(r)

    send_own(early, lambda r: grad_copy(r, z).start())
    load_dec.wait()

    @pl.when(later == 0)
    def _():
        for r in range(2):
            dec_half(r, 0, down).start()
    loaded(enc_raw, load_sem.at[2])
    pick_enc(0)
    send_own(early, lambda r: enc_copy(r, z, 0, enc_rows, 2 * z).start())
    pick_enc(1)

    @pl.when(later > 0)
    def _():
        pl.semaphore_wait(ready_xy, later)
        for r in range(2):
            dec_half(r, 0, down).start()
    pair_copy(enc_all.at[:, enc_rows(z, core)], z).start()
    load_upb.wait()
    loaded(del_raw, load_sem.at[5])
    for w in range(wins):
        for s in range(uact):
            del_all[down, w, s] = del_raw[within(upb[s, down * wins + w], rows // BLOCK), w * win:(w + 1) * win]
    for r in range(2):
        del_copy(r, down).start()
    for r in range(2):
        dec_half(r, 1, down).start()

    def each(j, act):
        for r in range(2):
            level = z - step_of[r] * j

            @pl.when(inside(level))
            def _():
                act(r, level)

    def relay_grad(r, level):
        grad_copy(r, level).wait_recv()

        @pl.when(can_go[r])
        def _():
            grad_copy(r, level).start()
        pair_grad(level).start()

    @pl.when(z < high)
    def _():
        pl.semaphore_wait(ready_z, 1)
        grad_copy(0, z).start()
        enc_copy(0, z, 0, enc_rows, 2 * z).start()
    pair_grad(z).start()
    each(1, relay_grad)
    send_own(can_go, lambda r: enc_copy(r, z, 1, enc_rows, 2 * z + 1).start())

    acc[...] = jnp.zeros_like(acc)

    def mult(q, rs, n, start=0, size=depth):
        ks = pl.ds(pl.multiple_of(start, BLOCK), size)
        result = jnp.dot(
            dec_all[q, rs, ks], enc_all[n, pl.ds(pl.multiple_of(q * depth + start, BLOCK), size), :],
            preferred_element_type=F32)
        for i in range(half // BLOCK):
            acc[n * (half // BLOCK) + i, rs] += result[:, i * BLOCK:(i + 1) * BLOCK]

    def enc_stage(q, n):
        gap = jnp.maximum(q - z, z - q)
        return jnp.where(gap == last, 5 + n, 2 * gap)

    def products(low, high):
        @pl.loop(0, 4 * levels)
        def _(u):
            q, m, n = u // 4, u // 2 % 2, u % 2
            first = jnp.where(jnp.where(q == left, 1, 0) + m == 1, 2, 4)
            stage = jnp.maximum(enc_stage(q, n), jnp.where(q == down, 0, first))
            ready = jnp.logical_and(stage >= low, stage <= high)

            @pl.when(jnp.logical_and(ready, q != diag))
            def _():
                mult(q, pl.ds(pl.multiple_of(m * part, part), part), n)

    everything = slice(0, rows)

    def diag_products(i):
        for n in range(2):
            @pl.when(enc_stage(diag, n) <= 5)
            def _():
                mult(diag, everything, n, body if i else 0, TAIL if i else body)

    def pair_whole(level):
        return pair_copy(enc_all.at[:, enc_rows(level, 1 - core)], level)

    def relay(j, h):
        def act(r, level):
            enc_copy(r, level, h, enc_rows, 2 * level + h).wait_recv()

            @pl.when(can_go[r])
            def _():
                if j == last - 1 and h == 1:
                    enc_copy(r, level, h, enc_a, 2 * level + h).start()
                    enc_copy(r, level, h, enc_b, 2 * levels).start()
                else:
                    enc_copy(r, level, h, enc_rows, 2 * level + h).start()
            if h == 1:
                pair_copy(enc_all.at[:, enc_rows(level, core)], level).start()
        each(j, act)

    relay(1, 0)
    each(2, relay_grad)
    relay(1, 1)
    for r in range(2):
        dec_half(r, 0, ring_from[r]).wait_recv()
        for i in range(2):
            dec_relay(r, i, ring_from[r]).start()
    for r in range(2):
        del_copy(r, ring_from[r]).wait_recv()
        del_relay(r, ring_from[r]).start()
    pair_whole(z).wait_recv()
    each(1, lambda r, level: pair_whole(level).wait_recv())
    products(0, 2)
    each(3, relay_grad)
    relay(2, 0)

    relay(2, 1)
    for r in range(2):
        dec_half(r, 1, ring_from[r]).wait_recv()
    each(2, lambda r, level: pair_whole(level).wait_recv())
    products(3, 4)

    loaded(del_all.at[diag], del_recv.at[2])
    loaded(grad_all.at[pl.ds(0, levels * toks)], pg_recv.at[0])
    for d in range(n_down):
        for w in range(wins):
            for b in range(rows // BLOCK):
                hits = hits_of(b, [upb[s, d * wins + w] for s in range(uact)])
                slot = within(sum(s * hit for s, hit in enumerate(hits)), uact)
                t = (d * wins + w) * win
                masked[t:t + win, b * BLOCK:(b + 1) * BLOCK] = del_all[d, w, slot] * flag(sum(hits), 1, masked.dtype)
    whole = lax.dot_general(
        masked[...], grad_all[...], (((0,), (0,)), ((), ())), preferred_element_type=F32)
    for s in range(dact):
        prod[s] = whole[:, s * BLOCK:(s + 1) * BLOCK]
    prod[dact] = jnp.zeros((rows, BLOCK), F32)

    far = last - z

    def end_wait(h, where, sem):
        for r in range(2):
            @pl.when(z == (0 if r else last))
            def _():
                enc_copy(r, far, h, where, sem).wait_recv()

    @pl.when(at_end)
    def _():
        end_wait(0, enc_rows, 2 * far)
        pair_copy(enc_all.at[0, enc_rows(far, core)], far).start()
        pair_copy(enc_all.at[0, enc_rows(far, 1 - core)], far).wait_recv()

        @pl.when(far != diag)
        def _():
            mult(far, everything, 0)
        end_wait(1, enc_a, 2 * far + 1)
        pair_copy(enc_all.at[1, enc_a(far, core)], levels).start()
    for r in range(2):
        dec_relay(r, 0, diag).wait_recv()
    diag_products(0)

    @pl.when(at_end)
    def _():
        end_wait(1, enc_b, 2 * levels)
        pair_copy(enc_all.at[1, enc_b(far, core)], levels + 1).start()
        pair_copy(enc_all.at[1, enc_a(far, 1 - core)], levels).wait_recv()
        mult(far, everything, 1, TAIL, depth - 2 * TAIL)
    for r in range(2):
        dec_relay(r, 1, diag).wait_recv()
    diag_products(1)

    @pl.when(at_end)
    def _():
        mult(far, everything, 1, core * body, TAIL)
        pair_copy(enc_all.at[1, enc_b(far, 1 - core)], levels + 1).wait_recv()
        mult(far, everything, 1, (1 - core) * body, TAIL)

    tile = 64
    places = []
    for c in range(blocks):
        hits = hits_of(c, [downb[s] for s in range(dact)])
        slot = sum(s * hit for s, hit in enumerate(hits))
        places.append((within(slot, dact), within(slot + dact * (1 - sum(hits)), dact + 1)))

    @pl.loop(0, rows // tile)
    def _(t):
        rs = pl.ds(pl.multiple_of(t * tile, tile), tile)
        for c, (slot, factor) in enumerate(places):
            out[rs, c * BLOCK:(c + 1) * BLOCK] = acc[slot, rs] * prod[factor, rs]

    def sent(ref, kind):
        pltpu.make_async_copy(ref, ref, send_sem.at[kind]).wait()

    sent(dec_all.at[pl.ds(0, 3)], 0)

    @pl.when(at_end)
    def _():
        sent(enc_all.at[:, pl.ds(0, height)], 1)
        sent(grad_all.at[pl.ds(0, toks)], 4)

    @pl.when(jnp.logical_not(at_end))
    def _():
        sent(enc_all.at[:, pl.ds(0, (levels + 1) * height)], 1)
        sent(grad_all.at[pl.ds(0, (levels + 1) * toks)], 4)
    sent(enc_all.at[:, pl.ds(0, levels * height)], 2)
    sent(del_all.at[pl.ds(0, n_down - 1)], 3)
    sent(grad_all.at[pl.ds(0, levels * toks)], 5)


def ring_local(n_up, n_down, win, deltas, gradients, up_blocks, down_blocks, decoder, encoder):
    rows, depth = decoder.shape
    height, cols = encoder.shape
    toks = gradients.shape[0]
    uact, dact = up_blocks.shape[1], down_blocks.shape[0]
    tokens = deltas.shape[0] * n_down
    wins = deltas.shape[0] // win
    used = dact * BLOCK
    levels = n_up // 2
    kind = decoder.dtype
    dma = pltpu.SemaphoreType.DMA
    hbm = pl.BlockSpec(memory_space=pltpu.HBM)
    return pl.pallas_call(
        functools.partial(gather_scores, n_up, n_down),
        out_shape=jax.ShapeDtypeStruct((rows, cols), F32),
        in_specs=[hbm] * 6,
        out_specs=pl.BlockSpec(memory_space=pltpu.VMEM),
        scratch_shapes=[
            pltpu.SMEM((uact, up_blocks.shape[0]), jnp.int32),
            pltpu.SMEM((dact,), jnp.int32),
            pltpu.VMEM((n_down, rows, depth), kind),
            pltpu.VMEM((cols // BLOCK, height, BLOCK), kind),
            pltpu.VMEM((2, n_up * height, used // 2), kind),
            pltpu.VMEM((rows // BLOCK, deltas.shape[0], BLOCK), kind),
            pltpu.VMEM((n_down, wins, uact, win, BLOCK), kind),
            pltpu.VMEM((cols // BLOCK, toks, BLOCK), kind),
            pltpu.VMEM((n_up * toks, used), kind),
            pltpu.VMEM((tokens, rows), kind),
            pltpu.VMEM((dact, rows, BLOCK), F32),
            pltpu.VMEM((dact + 1, rows, BLOCK), F32),
            dma((6,)),
            dma((6,)),
            dma((2, 4)),
            dma((3,)),
            dma((2 * levels + 1,)),
            dma((levels + 2,)),
            dma((levels,)),
            dma((1,)),
            pltpu.SemaphoreType.REGULAR,
            pltpu.SemaphoreType.REGULAR,
        ],
        compiler_params=pltpu.CompilerParams(collective_id=0, has_side_effects=True, vmem_limit_bytes=LARGE),
        name="gather_scores",
    )(*[pltpu.with_memory_space_constraint(x, pltpu.HBM) for x in (up_blocks.T, down_blocks, deltas, gradients, decoder, encoder)])


def plain_local(deltas, gradients, up_blocks, down_blocks, decoder, encoder):
    token_deltas = lax.all_gather(deltas, "down", axis=0, tiled=True)
    token_grads = lax.all_gather(gradients, "up", axis=0, tiled=True)
    tokens, rows = token_deltas.shape
    windows, dact = up_blocks.shape[0], down_blocks.shape[0]
    row_blocks, col_blocks = rows // BLOCK, encoder.shape[1] // BLOCK
    local_ids = jnp.arange(row_blocks, dtype=jnp.int32)
    block_on = jnp.any(up_blocks[:, :, None] == local_ids[None, None, :], axis=1)
    masked = token_deltas.reshape(windows, tokens // windows, row_blocks, BLOCK) * block_on[
        :, None, :, None].astype(token_deltas.dtype)
    masked = masked.reshape(tokens, rows)
    dec_whole = lax.all_gather(decoder, "down", axis=1, tiled=True)
    height = encoder.shape[0]
    enc_used = jnp.take(encoder.reshape(height, col_blocks, BLOCK), down_blocks, axis=1).reshape(height, dact * BLOCK)
    virtual = jnp.dot(dec_whole, lax.all_gather(enc_used, "up", axis=0, tiled=True), preferred_element_type=F32)
    grad_used = jnp.take(token_grads.reshape(tokens, col_blocks, BLOCK), down_blocks, axis=1).reshape(tokens, dact * BLOCK)
    product = lax.dot_general(masked, grad_used, (((0,), (0,)), ((), ())), preferred_element_type=F32)
    scored = (product * virtual).reshape(rows, dact, BLOCK)
    filled = jnp.zeros((rows, col_blocks, BLOCK), F32).at[:, down_blocks, :].set(scored)
    return filled.reshape(rows, encoder.shape[1])


def solution(mesh):
    n_up, n_down = mesh.shape["up"], mesh.shape["down"]
    ringed = n_down == 4 and n_up == 2 * n_down

    def local(deltas, gradients, up_blocks, down_blocks, decoder, encoder):
        args = (deltas, gradients, up_blocks, down_blocks, decoder, encoder)
        tokens = deltas.shape[0] * n_down
        win = tokens // up_blocks.shape[0]
        if ringed and deltas.shape[0] == 2 * win:
            return ring_local(n_up, n_down, win, *args)
        return plain_local(*args)

    placed = (P("down", "up"), P("up", "down"), P(None, "up"), P("down"), P("up", "down"), P("up", "down"))
    return jax.shard_map(local, mesh=mesh, in_specs=placed, out_specs=P("up", "down"), check_vma=False)
```

```python
import functools

import jax
import jax.numpy as jnp
from jax import lax
from jax.experimental import pallas as pl
from jax.experimental.pallas import tpu as pltpu
from jax.sharding import PartitionSpec as P

BLOCK = 128
TAIL = 128
LARGE = 24 << 20
MESH = pl.DeviceIdType.MESH
F32 = jnp.float32


def flag(number, block, kind):
    return jnp.where(jnp.full((1, BLOCK), number, jnp.int32) == block, 1.0, 0.0).astype(kind)


def within(number, count):
    return jnp.maximum(jnp.minimum(number, count - 1), 0)


def hits_of(number, slots):
    return [1 - jnp.minimum(jnp.abs(slot - number), 1) for slot in slots]


def gather_scores(
    n_up, n_down, upb_in, downb_in, deltas, grads, dec, enc, out,
    upb, downb, dec_all, enc_raw, enc_all, del_raw, del_all, grad_raw, grad_all, masked, acc, prod,
    load_sem, send_sem, dec_recv, del_recv, enc_recv, pair_recv, grad_recv, pg_recv, ready_z, ready_xy,
):
    levels = n_up // 2
    rows, depth = dec.shape
    height = enc.shape[0]
    half = enc_all.shape[2]
    part = rows // 2
    body = depth - TAIL
    toks = grads.shape[0]
    wins, uact, win = del_all.shape[1:4]
    dact = downb.shape[0]
    blocks = enc.shape[1] // BLOCK
    up, down = lax.axis_index("up"), lax.axis_index("down")
    z, core = up // 2, up % 2
    place = lambda d: 2 * (d // 2) + (d + d // 2) % 2
    pos = place(down)
    right, left = place((pos + 1) % 4), place((pos + 3) % 4)
    diag = place((pos + 2) % 4)
    ring_to = ((up, right), (up, left))
    ring_from = (left, right)
    step_of = (1, -1)
    pair = (2 * z + 1 - core, down)
    can_go = (z < levels - 1, z > 0)
    last = levels - 1
    at_end = jnp.logical_or(z == 0, z == last)
    inside = lambda level: jnp.logical_and(level >= 0, level < levels)

    high = levels // 2
    later = jnp.where(right > down, 1, 0) + jnp.where(left > down, 1, 0)
    barrier = pltpu.get_barrier_semaphore()

    def signal(sem, dev, when=None):
        if when is None:
            pl.semaphore_signal(sem, inc=1, device_id=dev, device_id_type=MESH)
        else:
            pl.when(when)(lambda: pl.semaphore_signal(sem, inc=1, device_id=dev, device_id_type=MESH))

    signal(barrier, pair)
    signal(barrier, (up + 2, down), z < last)
    signal(barrier, (up - 2, down), z > high)
    for d in (right, left):
        signal(barrier, (up, d), d > down)

    def by_block(src, dst, sem):
        return [pltpu.make_async_copy(src.at[:, b * BLOCK:(b + 1) * BLOCK], dst.at[b], sem) for b in range(dst.shape[0])]

    def loaded(ref, sem):
        pltpu.make_async_copy(ref, ref, sem).wait()

    load_downb = pltpu.make_async_copy(downb_in, downb, load_sem.at[0])
    load_upb = pltpu.make_async_copy(upb_in, upb, load_sem.at[4])
    load_dec = pltpu.make_async_copy(dec, dec_all.at[down], load_sem.at[3])
    for copy in (
        load_downb, *by_block(grads, grad_raw, load_sem.at[1]), load_dec, *by_block(enc, enc_raw, load_sem.at[2]),
        load_upb, *by_block(deltas, del_raw, load_sem.at[5]),
    ):
        copy.start()

    def remote(src, dst, kind, recv, dev):
        return pltpu.make_async_remote_copy(
            src, dst, send_sem.at[kind], recv, device_id=dev, device_id_type=MESH)

    def dec_half(r, i, owner):
        m = (i + r) % 2
        ref = dec_all.at[owner, m * part:(m + 1) * part]
        return remote(ref, ref, 0, dec_recv.at[r, i], ring_to[r])

    def dec_relay(r, i, owner):
        ref = dec_all.at[owner, r * part:(r + 1) * part, (body if i else 0):(depth if i else body)]
        return remote(ref, ref, 0, dec_recv.at[r, 2 + i], ring_to[r])

    def enc_rows(level, c):
        return pl.ds(pl.multiple_of((level * 2 + c) * height, 16), height)

    def enc_a(level, c):
        return pl.ds(pl.multiple_of((level * 2 + c) * height + (1 - c) * TAIL, 16), height - TAIL)

    def enc_b(level, c):
        return pl.ds(pl.multiple_of((level * 2 + c) * height + c * (height - TAIL), 16), TAIL)

    def enc_copy(r, level, h, where, sem):
        ref = enc_all.at[h, where(level, core)]
        return remote(ref, ref, 1, enc_recv.at[sem], (up + 2 * step_of[r], down))

    def pair_copy(ref, sem):
        return remote(ref, ref, 2, pair_recv.at[sem], pair)

    def del_copy(r, owner):
        ref = del_all.at[owner]
        return remote(ref, ref, 3, del_recv.at[r], ring_to[r])

    def del_relay(r, owner):
        ref = del_all.at[owner, r]
        return remote(ref, ref, 3, del_recv.at[2], ring_to[r])

    def grad_rows(level, c):
        return grad_all.at[pl.ds(pl.multiple_of((level * 2 + c) * toks, toks), toks)]

    def grad_copy(r, level):
        ref = grad_rows(level, core)
        return remote(ref, ref, 4, grad_recv.at[level], (up + 2 * step_of[r], down))

    def pair_grad(level):
        ref = grad_rows(level, core)
        return remote(ref, ref, 5, pg_recv.at[0], pair)

    def pick_enc(h):
        for s in range(h * dact // 2, (h + 1) * dact // 2):
            at = s * BLOCK - h * half
            enc_all[h, pl.ds(pl.multiple_of(up * height, 16), height), at:at + BLOCK] = enc_raw[chosen[s]]

    load_downb.wait()
    chosen = [within(downb[s], blocks) for s in range(dact)]
    loaded(grad_raw, load_sem.at[1])
    for s in range(dact):
        grad_all[pl.ds(pl.multiple_of(up * toks, toks), toks), s * BLOCK:(s + 1) * BLOCK] = grad_raw[chosen[s]]
    pl.semaphore_wait(barrier, 3 - later + jnp.where(z > 0, 1, 0) + jnp.where(z >= high, 1, 0) - jnp.where(z == last, 1, 0))
    signal(ready_z, (up - 2, down), jnp.logical_and(z > 0, z <= high))
    for d in (right, left):
        signal(ready_xy, (up, d), d < down)

    early = (jnp.logical_and(z >= high, z < last), z > 0)

    def send_own(which, act):
        for r in (1, 0):
            @pl.when(which[r])
            def _():
                act(r)

    send_own(early, lambda r: grad_copy(r, z).start())
    load_dec.wait()

    @pl.when(later == 0)
    def _():
        for r in range(2):
            dec_half(r, 0, down).start()
    loaded(enc_raw, load_sem.at[2])
    pick_enc(0)
    send_own(early, lambda r: enc_copy(r, z, 0, enc_rows, 2 * z).start())
    pick_enc(1)

    @pl.when(later > 0)
    def _():
        pl.semaphore_wait(ready_xy, later)
        for r in range(2):
            dec_half(r, 0, down).start()
    pair_copy(enc_all.at[:, enc_rows(z, core)], z).start()
    load_upb.wait()
    loaded(del_raw, load_sem.at[5])
    for w in range(wins):
        for s in range(uact):
            del_all[down, w, s] = del_raw[within(upb[s, down * wins + w], rows // BLOCK), w * win:(w + 1) * win]
    for r in range(2):
        del_copy(r, down).start()
    for r in range(2):
        dec_half(r, 1, down).start()

    def each(j, act):
        for r in range(2):
            level = z - step_of[r] * j

            @pl.when(inside(level))
            def _():
                act(r, level)

    def relay_grad(r, level):
        grad_copy(r, level).wait_recv()

        @pl.when(can_go[r])
        def _():
            grad_copy(r, level).start()
        pair_grad(level).start()

    @pl.when(z < high)
    def _():
        pl.semaphore_wait(ready_z, 1)
        grad_copy(0, z).start()
        enc_copy(0, z, 0, enc_rows, 2 * z).start()
    pair_grad(z).start()
    each(1, relay_grad)
    send_own(can_go, lambda r: enc_copy(r, z, 1, enc_rows, 2 * z + 1).start())

    acc[...] = jnp.zeros_like(acc)

    def mult(q, rs, n, start=0, size=depth):
        ks = pl.ds(pl.multiple_of(start, BLOCK), size)
        result = jnp.dot(
            dec_all[q, rs, ks], enc_all[n, pl.ds(pl.multiple_of(q * depth + start, BLOCK), size), :],
            preferred_element_type=F32)
        for i in range(half // BLOCK):
            acc[n * (half // BLOCK) + i, rs] += result[:, i * BLOCK:(i + 1) * BLOCK]

    def enc_stage(q, n):
        gap = jnp.maximum(q - z, z - q)
        return jnp.where(gap == last, 5 + n, 2 * gap)

    def products(low, high):
        @pl.loop(0, 4 * levels)
        def _(u):
            q, m, n = u // 4, u // 2 % 2, u % 2
            first = jnp.where(jnp.where(q == left, 1, 0) + m == 1, 2, 4)
            stage = jnp.maximum(enc_stage(q, n), jnp.where(q == down, 0, first))
            ready = jnp.logical_and(stage >= low, stage <= high)

            @pl.when(jnp.logical_and(ready, q != diag))
            def _():
                mult(q, pl.ds(pl.multiple_of(m * part, part), part), n)

    everything = slice(0, rows)

    def diag_products(i):
        for n in range(2):
            @pl.when(enc_stage(diag, n) <= 5)
            def _():
                mult(diag, everything, n, body if i else 0, TAIL if i else body)

    def pair_whole(level):
        return pair_copy(enc_all.at[:, enc_rows(level, 1 - core)], level)

    def relay(j, h):
        def act(r, level):
            enc_copy(r, level, h, enc_rows, 2 * level + h).wait_recv()

            @pl.when(can_go[r])
            def _():
                if j == last - 1 and h == 1:
                    enc_copy(r, level, h, enc_a, 2 * level + h).start()
                    enc_copy(r, level, h, enc_b, 2 * levels).start()
                else:
                    enc_copy(r, level, h, enc_rows, 2 * level + h).start()
            if h == 1:
                pair_copy(enc_all.at[:, enc_rows(level, core)], level).start()
        each(j, act)

    relay(1, 0)
    each(2, relay_grad)
    relay(1, 1)
    for r in range(2):
        dec_half(r, 0, ring_from[r]).wait_recv()
        del_copy(r, ring_from[r]).wait_recv()
        del_relay(r, ring_from[r]).start()
        for i in range(2):
            dec_relay(r, i, ring_from[r]).start()
    pair_whole(z).wait_recv()
    each(1, lambda r, level: pair_whole(level).wait_recv())
    products(0, 2)
    each(3, relay_grad)
    relay(2, 0)

    relay(2, 1)
    for r in range(2):
        dec_half(r, 1, ring_from[r]).wait_recv()
    each(2, lambda r, level: pair_whole(level).wait_recv())
    products(3, 4)

    loaded(del_all.at[diag], del_recv.at[2])
    loaded(grad_all.at[pl.ds(0, levels * toks)], pg_recv.at[0])
    for d in range(n_down):
        for w in range(wins):
            for b in range(rows // BLOCK):
                hits = hits_of(b, [upb[s, d * wins + w] for s in range(uact)])
                slot = within(sum(s * hit for s, hit in enumerate(hits)), uact)
                t = (d * wins + w) * win
                masked[t:t + win, b * BLOCK:(b + 1) * BLOCK] = del_all[d, w, slot] * flag(sum(hits), 1, masked.dtype)
    whole = lax.dot_general(
        masked[...], grad_all[...], (((0,), (0,)), ((), ())), preferred_element_type=F32)
    for s in range(dact):
        prod[s] = whole[:, s * BLOCK:(s + 1) * BLOCK]
    prod[dact] = jnp.zeros((rows, BLOCK), F32)

    far = last - z

    def end_wait(h, where, sem):
        for r in range(2):
            @pl.when(z == (0 if r else last))
            def _():
                enc_copy(r, far, h, where, sem).wait_recv()

    @pl.when(at_end)
    def _():
        end_wait(0, enc_rows, 2 * far)
        pair_copy(enc_all.at[0, enc_rows(far, core)], far).start()
        pair_copy(enc_all.at[0, enc_rows(far, 1 - core)], far).wait_recv()

        @pl.when(far != diag)
        def _():
            mult(far, everything, 0)
        end_wait(1, enc_a, 2 * far + 1)
        pair_copy(enc_all.at[1, enc_a(far, core)], levels).start()
    for r in range(2):
        dec_relay(r, 0, diag).wait_recv()
    diag_products(0)

    @pl.when(at_end)
    def _():
        end_wait(1, enc_b, 2 * levels)
        pair_copy(enc_all.at[1, enc_b(far, core)], levels + 1).start()
        pair_copy(enc_all.at[1, enc_a(far, 1 - core)], levels).wait_recv()
        mult(far, everything, 1, TAIL, depth - 2 * TAIL)
    for r in range(2):
        dec_relay(r, 1, diag).wait_recv()
    diag_products(1)

    @pl.when(at_end)
    def _():
        mult(far, everything, 1, core * body, TAIL)
        pair_copy(enc_all.at[1, enc_b(far, 1 - core)], levels + 1).wait_recv()
        mult(far, everything, 1, (1 - core) * body, TAIL)

    tile = 64
    places = []
    for c in range(blocks):
        hits = hits_of(c, [downb[s] for s in range(dact)])
        slot = sum(s * hit for s, hit in enumerate(hits))
        places.append((within(slot, dact), within(slot + dact * (1 - sum(hits)), dact + 1)))

    @pl.loop(0, rows // tile)
    def _(t):
        rs = pl.ds(pl.multiple_of(t * tile, tile), tile)
        for c, (slot, factor) in enumerate(places):
            out[rs, c * BLOCK:(c + 1) * BLOCK] = acc[slot, rs] * prod[factor, rs]

    def sent(ref, kind):
        pltpu.make_async_copy(ref, ref, send_sem.at[kind]).wait()

    sent(dec_all.at[pl.ds(0, 3)], 0)

    @pl.when(at_end)
    def _():
        sent(enc_all.at[:, pl.ds(0, height)], 1)
        sent(grad_all.at[pl.ds(0, toks)], 4)

    @pl.when(jnp.logical_not(at_end))
    def _():
        sent(enc_all.at[:, pl.ds(0, (levels + 1) * height)], 1)
        sent(grad_all.at[pl.ds(0, (levels + 1) * toks)], 4)
    sent(enc_all.at[:, pl.ds(0, levels * height)], 2)
    sent(del_all.at[pl.ds(0, n_down - 1)], 3)
    sent(grad_all.at[pl.ds(0, levels * toks)], 5)


def ring_local(n_up, n_down, win, deltas, gradients, up_blocks, down_blocks, decoder, encoder):
    rows, depth = decoder.shape
    height, cols = encoder.shape
    toks = gradients.shape[0]
    uact, dact = up_blocks.shape[1], down_blocks.shape[0]
    tokens = deltas.shape[0] * n_down
    wins = deltas.shape[0] // win
    used = dact * BLOCK
    levels = n_up // 2
    kind = decoder.dtype
    dma = pltpu.SemaphoreType.DMA
    hbm = pl.BlockSpec(memory_space=pltpu.HBM)
    return pl.pallas_call(
        functools.partial(gather_scores, n_up, n_down),
        out_shape=jax.ShapeDtypeStruct((rows, cols), F32),
        in_specs=[hbm] * 6,
        out_specs=pl.BlockSpec(memory_space=pltpu.VMEM),
        scratch_shapes=[
            pltpu.SMEM((uact, up_blocks.shape[0]), jnp.int32),
            pltpu.SMEM((dact,), jnp.int32),
            pltpu.VMEM((n_down, rows, depth), kind),
            pltpu.VMEM((cols // BLOCK, height, BLOCK), kind),
            pltpu.VMEM((2, n_up * height, used // 2), kind),
            pltpu.VMEM((rows // BLOCK, deltas.shape[0], BLOCK), kind),
            pltpu.VMEM((n_down, wins, uact, win, BLOCK), kind),
            pltpu.VMEM((cols // BLOCK, toks, BLOCK), kind),
            pltpu.VMEM((n_up * toks, used), kind),
            pltpu.VMEM((tokens, rows), kind),
            pltpu.VMEM((dact, rows, BLOCK), F32),
            pltpu.VMEM((dact + 1, rows, BLOCK), F32),
            dma((6,)),
            dma((6,)),
            dma((2, 4)),
            dma((3,)),
            dma((2 * levels + 1,)),
            dma((levels + 2,)),
            dma((levels,)),
            dma((1,)),
            pltpu.SemaphoreType.REGULAR,
            pltpu.SemaphoreType.REGULAR,
        ],
        compiler_params=pltpu.CompilerParams(collective_id=0, has_side_effects=True, vmem_limit_bytes=LARGE),
        name="gather_scores",
    )(*[pltpu.with_memory_space_constraint(x, pltpu.HBM) for x in (up_blocks.T, down_blocks, deltas, gradients, decoder, encoder)])


def plain_local(deltas, gradients, up_blocks, down_blocks, decoder, encoder):
    token_deltas = lax.all_gather(deltas, "down", axis=0, tiled=True)
    token_grads = lax.all_gather(gradients, "up", axis=0, tiled=True)
    tokens, rows = token_deltas.shape
    windows, dact = up_blocks.shape[0], down_blocks.shape[0]
    row_blocks, col_blocks = rows // BLOCK, encoder.shape[1] // BLOCK
    local_ids = jnp.arange(row_blocks, dtype=jnp.int32)
    block_on = jnp.any(up_blocks[:, :, None] == local_ids[None, None, :], axis=1)
    masked = token_deltas.reshape(windows, tokens // windows, row_blocks, BLOCK) * block_on[
        :, None, :, None].astype(token_deltas.dtype)
    masked = masked.reshape(tokens, rows)
    dec_whole = lax.all_gather(decoder, "down", axis=1, tiled=True)
    height = encoder.shape[0]
    enc_used = jnp.take(encoder.reshape(height, col_blocks, BLOCK), down_blocks, axis=1).reshape(height, dact * BLOCK)
    virtual = jnp.dot(dec_whole, lax.all_gather(enc_used, "up", axis=0, tiled=True), preferred_element_type=F32)
    grad_used = jnp.take(token_grads.reshape(tokens, col_blocks, BLOCK), down_blocks, axis=1).reshape(tokens, dact * BLOCK)
    product = lax.dot_general(masked, grad_used, (((0,), (0,)), ((), ())), preferred_element_type=F32)
    scored = (product * virtual).reshape(rows, dact, BLOCK)
    filled = jnp.zeros((rows, col_blocks, BLOCK), F32).at[:, down_blocks, :].set(scored)
    return filled.reshape(rows, encoder.shape[1])


def solution(mesh):
    n_up, n_down = mesh.shape["up"], mesh.shape["down"]
    ringed = n_down == 4 and n_up == 2 * n_down

    def local(deltas, gradients, up_blocks, down_blocks, decoder, encoder):
        args = (deltas, gradients, up_blocks, down_blocks, decoder, encoder)
        tokens = deltas.shape[0] * n_down
        win = tokens // up_blocks.shape[0]
        if ringed and deltas.shape[0] == 2 * win:
            return ring_local(n_up, n_down, win, *args)
        return plain_local(*args)

    placed = (P("down", "up"), P("up", "down"), P(None, "up"), P("down"), P("up", "down"), P("up", "down"))
    return jax.shard_map(local, mesh=mesh, in_specs=placed, out_specs=P("up", "down"), check_vma=False)
```

```python
import functools

import jax
import jax.numpy as jnp
from jax import lax
from jax.experimental import pallas as pl
from jax.experimental.pallas import tpu as pltpu
from jax.sharding import PartitionSpec as P

BLOCK = 128
TAIL = 64
LAST = 128
LARGE = 24 << 20
MESH = pl.DeviceIdType.MESH
F32 = jnp.float32


def flag(number, block, kind):
    return jnp.where(jnp.full((1, BLOCK), number, jnp.int32) == block, 1.0, 0.0).astype(kind)


def within(number, count):
    return jnp.maximum(jnp.minimum(number, count - 1), 0)


def hits_of(number, slots):
    return [1 - jnp.minimum(jnp.abs(slot - number), 1) for slot in slots]


def gather_scores(
    n_up, n_down, upb_in, downb_in, deltas, grads, dec, enc, out,
    upb, downb, dec_all, enc_raw, enc_all, del_raw, del_all, grad_raw, grad_all, masked, acc, prod,
    load_sem, send_sem, dec_recv, del_recv, enc_recv, pair_recv, grad_recv, pg_recv, ready_z, ready_xy,
):
    levels = n_up // 2
    rows, depth = dec.shape
    height = enc.shape[0]
    half = enc_all.shape[2]
    part = rows // 2
    body = depth - LAST
    toks = grads.shape[0]
    wins, uact, win = del_all.shape[1:4]
    dact = downb.shape[0]
    blocks = enc.shape[1] // BLOCK
    up, down = lax.axis_index("up"), lax.axis_index("down")
    z, core = up // 2, up % 2
    place = lambda d: 2 * (d // 2) + (d + d // 2) % 2
    pos = place(down)
    right, left = place((pos + 1) % 4), place((pos + 3) % 4)
    diag = place((pos + 2) % 4)
    ring_to = ((up, right), (up, left))
    ring_from = (left, right)
    step_of = (1, -1)
    pair = (2 * z + 1 - core, down)
    can_go = (z < levels - 1, z > 0)
    last = levels - 1
    at_end = jnp.logical_or(z == 0, z == last)
    inside = lambda level: jnp.logical_and(level >= 0, level < levels)

    high = levels // 2
    later = jnp.where(right > down, 1, 0) + jnp.where(left > down, 1, 0)
    barrier = pltpu.get_barrier_semaphore()

    def signal(sem, dev, when=None):
        if when is None:
            pl.semaphore_signal(sem, inc=1, device_id=dev, device_id_type=MESH)
        else:
            pl.when(when)(lambda: pl.semaphore_signal(sem, inc=1, device_id=dev, device_id_type=MESH))

    signal(barrier, pair)
    signal(barrier, (up + 2, down), z < last)
    signal(barrier, (up - 2, down), z > high)
    signal(barrier, (up + 3 - 2 * core, down), z == 0)
    signal(barrier, (up - 1 - 2 * core, down), z == last)
    for d in (right, left):
        signal(barrier, (up, d), d > down)

    def by_block(src, dst, sem):
        return [pltpu.make_async_copy(src.at[:, b * BLOCK:(b + 1) * BLOCK], dst.at[b], sem) for b in range(dst.shape[0])]

    def loaded(ref, sem):
        pltpu.make_async_copy(ref, ref, sem).wait()

    load_downb = pltpu.make_async_copy(downb_in, downb, load_sem.at[0])
    load_upb = pltpu.make_async_copy(upb_in, upb, load_sem.at[4])
    load_dec = pltpu.make_async_copy(dec, dec_all.at[down], load_sem.at[3])
    for copy in (
        load_downb, *by_block(grads, grad_raw, load_sem.at[1]), load_dec, *by_block(enc, enc_raw, load_sem.at[2]),
        load_upb, *by_block(deltas, del_raw, load_sem.at[5]),
    ):
        copy.start()

    def remote(src, dst, kind, recv, dev):
        return pltpu.make_async_remote_copy(
            src, dst, send_sem.at[kind], recv, device_id=dev, device_id_type=MESH)

    def dec_half(r, i, owner):
        m = (i + r) % 2
        ref = dec_all.at[owner, m * part:(m + 1) * part]
        return remote(ref, ref, 0, dec_recv.at[i], ring_to[r])

    def dec_relay(r, i, owner):
        ref = dec_all.at[owner, r * part:(r + 1) * part, (body if i else 0):(depth if i else body)]
        return remote(ref, ref, 0, dec_recv.at[2 + i], ring_to[r])

    def enc_rows(level, c):
        return pl.ds(pl.multiple_of((level * 2 + c) * height, 16), height)

    def enc_a(level, c):
        return pl.ds(pl.multiple_of((level * 2 + c) * height + c * TAIL, 16), height - TAIL)

    def enc_b(level, c):
        return pl.ds(pl.multiple_of((level * 2 + c) * height + (1 - c) * (height - TAIL), 16), TAIL)

    def enc_copy(r, level, h, where, sem, cross=False):
        ref = enc_all.at[h, where(level, core)]
        target = up + 2 * step_of[r]
        return remote(ref, ref, 1, enc_recv.at[sem], (target + 1 - 2 * core if cross else target, down))

    def pair_copy(ref, sem):
        return remote(ref, ref, 2, pair_recv.at[sem], pair)

    def del_copy(r, owner):
        ref = del_all.at[owner]
        return remote(ref, ref, 3, del_recv.at[0], ring_to[r])

    def del_relay(r, owner):
        ref = del_all.at[owner, r]
        return remote(ref, ref, 3, del_recv.at[1], ring_to[r])

    def grad_rows(level, c):
        return grad_all.at[pl.ds(pl.multiple_of((level * 2 + c) * toks, toks), toks)]

    def grad_copy(r, level):
        ref = grad_rows(level, core)
        return remote(ref, ref, 4, grad_recv.at[level], (up + 2 * step_of[r], down))

    def pair_grad(level):
        ref = grad_rows(level, core)
        return remote(ref, ref, 5, pg_recv.at[0], pair)

    def pick_enc(h):
        for s in range(h * dact // 2, (h + 1) * dact // 2):
            at = s * BLOCK - h * half
            enc_all[h, pl.ds(pl.multiple_of(up * height, 16), height), at:at + BLOCK] = enc_raw[chosen[s]]

    load_downb.wait()
    chosen = [within(downb[s], blocks) for s in range(dact)]
    loaded(grad_raw, load_sem.at[1])
    for s in range(dact):
        grad_all[pl.ds(pl.multiple_of(up * toks, toks), toks), s * BLOCK:(s + 1) * BLOCK] = grad_raw[chosen[s]]
    pl.semaphore_wait(barrier, (
        3 - later + jnp.where(z > 0, 1, 0) + jnp.where(z >= high, 1, 0) - jnp.where(z == last, 1, 0)
        + jnp.where(z == 1, 1, 0) + jnp.where(z == last - 1, 1, 0)))
    signal(ready_z, (up - 2, down), jnp.logical_and(z > 0, z <= high))
    for d in (right, left):
        signal(ready_xy, (up, d), d < down)

    early = (jnp.logical_and(z >= high, z < last), z > 0)

    def send_own(which, act):
        for r in (1, 0):
            @pl.when(which[r])
            def _():
                act(r)

    send_own(early, lambda r: grad_copy(r, z).start())
    load_dec.wait()

    @pl.when(later == 0)
    def _():
        for r in range(2):
            dec_half(r, 0, down).start()
    loaded(enc_raw, load_sem.at[2])
    pick_enc(0)
    send_own(early, lambda r: enc_copy(r, z, 0, enc_rows, 2 * z).start())
    pick_enc(1)

    @pl.when(later > 0)
    def _():
        pl.semaphore_wait(ready_xy, later)
        for r in range(2):
            dec_half(r, 0, down).start()
    pair_copy(enc_all.at[:, enc_rows(z, core)], z).start()
    load_upb.wait()
    loaded(del_raw, load_sem.at[5])
    for w in range(wins):
        for s in range(uact):
            del_all[down, w, s] = del_raw[within(upb[s, down * wins + w], rows // BLOCK), w * win:(w + 1) * win]
    for r in range(2):
        del_copy(r, down).start()
    for r in range(2):
        dec_half(r, 1, down).start()

    def each(j, act):
        for r in range(2):
            level = z - step_of[r] * j

            @pl.when(inside(level))
            def _():
                act(r, level)

    def relay_grad(r, level):
        grad_copy(r, level).wait_recv()

        @pl.when(can_go[r])
        def _():
            grad_copy(r, level).start()
        pair_grad(level).start()

    @pl.when(z < high)
    def _():
        pl.semaphore_wait(ready_z, 1)
        grad_copy(0, z).start()
        enc_copy(0, z, 0, enc_rows, 2 * z).start()
    pair_grad(z).start()
    each(1, relay_grad)
    send_own(can_go, lambda r: enc_copy(r, z, 1, enc_rows, 2 * z + 1).start())

    acc[...] = jnp.zeros_like(acc)

    def mult(q, rs, n, start=0, size=depth):
        ks = pl.ds(pl.multiple_of(start, BLOCK), size)
        result = jnp.dot(
            dec_all[q, rs, ks], enc_all[n, pl.ds(pl.multiple_of(q * depth + start, BLOCK), size), :],
            preferred_element_type=F32)
        for i in range(half // BLOCK):
            acc[n * (half // BLOCK) + i, rs] += result[:, i * BLOCK:(i + 1) * BLOCK]

    def enc_stage(q, n):
        gap = jnp.maximum(q - z, z - q)
        return jnp.where(gap == last, 5 + n, 2 * gap)

    def products(low, high):
        @pl.loop(0, 4 * levels)
        def _(u):
            q, m, n = u // 4, u // 2 % 2, u % 2
            first = jnp.where(jnp.where(q == left, 1, 0) + m == 1, 2, 4)
            stage = jnp.maximum(enc_stage(q, n), jnp.where(q == down, 0, first))
            ready = jnp.logical_and(stage >= low, stage <= high)

            @pl.when(jnp.logical_and(ready, q != diag))
            def _():
                mult(q, pl.ds(pl.multiple_of(m * part, part), part), n)

    everything = slice(0, rows)

    def diag_products(i):
        for n in range(2):
            @pl.when(enc_stage(diag, n) <= 5)
            def _():
                mult(diag, everything, n, body if i else 0, LAST if i else body)

    def pair_whole(level):
        return pair_copy(enc_all.at[:, enc_rows(level, 1 - core)], level)

    def relay(j, h):
        def act(r, level):
            enc_copy(r, level, h, enc_rows, 2 * level + h).wait_recv()

            @pl.when(can_go[r])
            def _():
                if j == last - 1 and h == 1:
                    enc_copy(r, level, h, enc_a, 2 * level + h).start()
                    for cross in (False, True):
                        enc_copy(r, level, h, enc_b, 2 * levels, cross).start()
                else:
                    enc_copy(r, level, h, enc_rows, 2 * level + h).start()
            if h == 1:
                pair_copy(enc_all.at[:, enc_rows(level, core)], level).start()
        each(j, act)

    relay(1, 0)
    each(2, relay_grad)
    relay(1, 1)
    loaded(dec_all.at[left], dec_recv.at[0])
    loaded(del_all.at[pl.ds(0, 2)], del_recv.at[0])
    for r in range(2):
        del_relay(r, ring_from[r]).start()
        for i in range(2):
            dec_relay(r, i, ring_from[r]).start()
    pair_whole(z).wait_recv()
    each(1, lambda r, level: pair_whole(level).wait_recv())
    products(0, 2)
    each(3, relay_grad)
    relay(2, 0)

    relay(2, 1)
    loaded(dec_all.at[left], dec_recv.at[1])
    each(2, lambda r, level: pair_whole(level).wait_recv())
    products(3, 4)

    loaded(del_all.at[diag], del_recv.at[1])
    loaded(grad_all.at[pl.ds(0, levels * toks)], pg_recv.at[0])
    for d in range(n_down):
        for w in range(wins):
            for b in range(rows // BLOCK):
                hits = hits_of(b, [upb[s, d * wins + w] for s in range(uact)])
                slot = within(sum(s * hit for s, hit in enumerate(hits)), uact)
                t = (d * wins + w) * win
                masked[t:t + win, b * BLOCK:(b + 1) * BLOCK] = del_all[d, w, slot] * flag(sum(hits), 1, masked.dtype)
    whole = lax.dot_general(
        masked[...], grad_all[...], (((0,), (0,)), ((), ())), preferred_element_type=F32)
    for s in range(dact):
        prod[s] = whole[:, s * BLOCK:(s + 1) * BLOCK]
    prod[dact] = jnp.zeros((rows, BLOCK), F32)

    far = last - z

    def end_wait(h, where, sem):
        for r in range(2):
            @pl.when(z == (0 if r else last))
            def _():
                enc_copy(r, far, h, where, sem).wait_recv()

    @pl.when(at_end)
    def _():
        end_wait(0, enc_rows, 2 * far)
        pair_copy(enc_all.at[0, enc_rows(far, core)], far).start()
        pair_copy(enc_all.at[0, enc_rows(far, 1 - core)], far).wait_recv()

        @pl.when(far != diag)
        def _():
            mult(far, everything, 0)
        end_wait(1, enc_a, 2 * far + 1)
        pair_copy(enc_all.at[1, enc_a(far, core)], levels).start()
    loaded(dec_all.at[diag, :, :body], dec_recv.at[2])
    diag_products(0)

    side = height - TAIL

    def other_side():
        pair_copy(enc_all.at[1, enc_a(far, 1 - core)], levels).wait_recv()
        mult(far, everything, 1, (1 - core) * (depth - side), side)

    def own_side():
        mult(far, everything, 1, core * (depth - side), side)

    soon = jnp.logical_or(core == 0, far != diag)
    pl.when(jnp.logical_and(at_end, soon))(own_side)
    loaded(dec_all.at[diag, :, body:], dec_recv.at[3])
    pl.when(jnp.logical_and(at_end, jnp.logical_not(soon)))(own_side)
    pl.when(jnp.logical_and(at_end, core == 0))(other_side)
    diag_products(1)

    @pl.when(at_end)
    def _():
        loaded(enc_all.at[1, pl.ds(pl.multiple_of(far * depth + side, BLOCK), 2 * TAIL)], enc_recv.at[2 * levels])
        mult(far, everything, 1, side, 2 * TAIL)
        pl.when(core == 1)(other_side)

    tile = 64
    places = []
    for c in range(blocks):
        hits = hits_of(c, [downb[s] for s in range(dact)])
        slot = sum(s * hit for s, hit in enumerate(hits))
        places.append((within(slot, dact), within(slot + dact * (1 - sum(hits)), dact + 1)))

    @pl.loop(0, rows // tile)
    def _(t):
        rs = pl.ds(pl.multiple_of(t * tile, tile), tile)
        for c, (slot, factor) in enumerate(places):
            out[rs, c * BLOCK:(c + 1) * BLOCK] = acc[slot, rs] * prod[factor, rs]

    def sent(ref, kind):
        pltpu.make_async_copy(ref, ref, send_sem.at[kind]).wait()

    sent(dec_all.at[pl.ds(0, 3)], 0)

    @pl.when(at_end)
    def _():
        sent(enc_all.at[:, pl.ds(0, height)], 1)
        sent(enc_all.at[:, pl.ds(0, levels * height - TAIL // 2)], 2)
        sent(grad_all.at[pl.ds(0, toks)], 4)

    @pl.when(jnp.logical_not(at_end))
    def _():
        sent(enc_all.at[:, pl.ds(0, (levels + 1) * height + TAIL // 2)], 1)
        sent(enc_all.at[:, pl.ds(0, levels * height)], 2)
        sent(grad_all.at[pl.ds(0, (levels + 1) * toks)], 4)
    sent(del_all.at[pl.ds(0, n_down - 1)], 3)
    sent(grad_all.at[pl.ds(0, levels * toks)], 5)


def ring_local(n_up, n_down, win, deltas, gradients, up_blocks, down_blocks, decoder, encoder):
    rows, depth = decoder.shape
    height, cols = encoder.shape
    toks = gradients.shape[0]
    uact, dact = up_blocks.shape[1], down_blocks.shape[0]
    tokens = deltas.shape[0] * n_down
    wins = deltas.shape[0] // win
    used = dact * BLOCK
    levels = n_up // 2
    kind = decoder.dtype
    dma = pltpu.SemaphoreType.DMA
    hbm = pl.BlockSpec(memory_space=pltpu.HBM)
    return pl.pallas_call(
        functools.partial(gather_scores, n_up, n_down),
        out_shape=jax.ShapeDtypeStruct((rows, cols), F32),
        in_specs=[hbm] * 6,
        out_specs=pl.BlockSpec(memory_space=pltpu.VMEM),
        scratch_shapes=[
            pltpu.SMEM((uact, up_blocks.shape[0]), jnp.int32),
            pltpu.SMEM((dact,), jnp.int32),
            pltpu.VMEM((n_down, rows, depth), kind),
            pltpu.VMEM((cols // BLOCK, height, BLOCK), kind),
            pltpu.VMEM((2, n_up * height, used // 2), kind),
            pltpu.VMEM((rows // BLOCK, deltas.shape[0], BLOCK), kind),
            pltpu.VMEM((n_down, wins, uact, win, BLOCK), kind),
            pltpu.VMEM((cols // BLOCK, toks, BLOCK), kind),
            pltpu.VMEM((n_up * toks, used), kind),
            pltpu.VMEM((tokens, rows), kind),
            pltpu.VMEM((dact, rows, BLOCK), F32),
            pltpu.VMEM((dact + 1, rows, BLOCK), F32),
            dma((6,)),
            dma((6,)),
            dma((4,)),
            dma((2,)),
            dma((2 * levels + 1,)),
            dma((levels + 1,)),
            dma((levels,)),
            dma((1,)),
            pltpu.SemaphoreType.REGULAR,
            pltpu.SemaphoreType.REGULAR,
        ],
        compiler_params=pltpu.CompilerParams(collective_id=0, has_side_effects=True, vmem_limit_bytes=LARGE),
        name="gather_scores",
    )(*[pltpu.with_memory_space_constraint(x, pltpu.HBM) for x in (up_blocks.T, down_blocks, deltas, gradients, decoder, encoder)])


def plain_local(deltas, gradients, up_blocks, down_blocks, decoder, encoder):
    token_deltas = lax.all_gather(deltas, "down", axis=0, tiled=True)
    token_grads = lax.all_gather(gradients, "up", axis=0, tiled=True)
    tokens, rows = token_deltas.shape
    windows, dact = up_blocks.shape[0], down_blocks.shape[0]
    row_blocks, col_blocks = rows // BLOCK, encoder.shape[1] // BLOCK
    local_ids = jnp.arange(row_blocks, dtype=jnp.int32)
    block_on = jnp.any(up_blocks[:, :, None] == local_ids[None, None, :], axis=1)
    masked = token_deltas.reshape(windows, tokens // windows, row_blocks, BLOCK) * block_on[
        :, None, :, None].astype(token_deltas.dtype)
    masked = masked.reshape(tokens, rows)
    dec_whole = lax.all_gather(decoder, "down", axis=1, tiled=True)
    height = encoder.shape[0]
    enc_used = jnp.take(encoder.reshape(height, col_blocks, BLOCK), down_blocks, axis=1).reshape(height, dact * BLOCK)
    virtual = jnp.dot(dec_whole, lax.all_gather(enc_used, "up", axis=0, tiled=True), preferred_element_type=F32)
    grad_used = jnp.take(token_grads.reshape(tokens, col_blocks, BLOCK), down_blocks, axis=1).reshape(tokens, dact * BLOCK)
    product = lax.dot_general(masked, grad_used, (((0,), (0,)), ((), ())), preferred_element_type=F32)
    scored = (product * virtual).reshape(rows, dact, BLOCK)
    filled = jnp.zeros((rows, col_blocks, BLOCK), F32).at[:, down_blocks, :].set(scored)
    return filled.reshape(rows, encoder.shape[1])


def solution(mesh):
    n_up, n_down = mesh.shape["up"], mesh.shape["down"]
    ringed = n_down == 4 and n_up == 2 * n_down

    def local(deltas, gradients, up_blocks, down_blocks, decoder, encoder):
        args = (deltas, gradients, up_blocks, down_blocks, decoder, encoder)
        tokens = deltas.shape[0] * n_down
        win = tokens // up_blocks.shape[0]
        if ringed and deltas.shape[0] == 2 * win:
            return ring_local(n_up, n_down, win, *args)
        return plain_local(*args)

    placed = (P("down", "up"), P("up", "down"), P(None, "up"), P("down"), P("up", "down"), P("up", "down"))
    return jax.shard_map(local, mesh=mesh, in_specs=placed, out_specs=P("up", "down"), check_vma=False)
```

```python
import functools

import jax
import jax.numpy as jnp
from jax import lax
from jax.experimental import pallas as pl
from jax.experimental.pallas import tpu as pltpu
from jax.sharding import PartitionSpec as P

BLOCK = 128
TAIL = 128
LARGE = 24 << 20
MESH = pl.DeviceIdType.MESH
F32 = jnp.float32


def flag(number, block, kind):
    return jnp.where(jnp.full((1, BLOCK), number, jnp.int32) == block, 1.0, 0.0).astype(kind)


def within(number, count):
    return jnp.maximum(jnp.minimum(number, count - 1), 0)


def hits_of(number, slots):
    return [1 - jnp.minimum(jnp.abs(slot - number), 1) for slot in slots]


def gather_scores(
    n_up, n_down, upb_in, downb_in, deltas, grads, dec, enc, out,
    upb, downb, dec_all, enc_raw, enc_all, del_raw, del_all, grad_raw, grad_all, masked, acc, prod,
    load_sem, send_sem, dec_recv, del_recv, enc_recv, pair_recv, grad_recv, pg_recv, ready_z, ready_xy,
):
    levels = n_up // 2
    rows, depth = dec.shape
    height = enc.shape[0]
    half = enc_all.shape[2]
    part = rows // 2
    body = depth - TAIL
    toks = grads.shape[0]
    wins, uact, win = del_all.shape[1:4]
    dact = downb.shape[0]
    blocks = enc.shape[1] // BLOCK
    up, down = lax.axis_index("up"), lax.axis_index("down")
    z, core = up // 2, up % 2
    place = lambda d: 2 * (d // 2) + (d + d // 2) % 2
    pos = place(down)
    right, left = place((pos + 1) % 4), place((pos + 3) % 4)
    diag = place((pos + 2) % 4)
    ring_to = ((up, right), (up, left))
    ring_from = (left, right)
    step_of = (1, -1)
    pair = (2 * z + 1 - core, down)
    can_go = (z < levels - 1, z > 0)
    last = levels - 1
    at_end = jnp.logical_or(z == 0, z == last)
    inside = lambda level: jnp.logical_and(level >= 0, level < levels)

    high = levels // 2
    later = jnp.where(right > down, 1, 0) + jnp.where(left > down, 1, 0)
    barrier = pltpu.get_barrier_semaphore()

    def signal(sem, dev, when=None):
        if when is None:
            pl.semaphore_signal(sem, inc=1, device_id=dev, device_id_type=MESH)
        else:
            pl.when(when)(lambda: pl.semaphore_signal(sem, inc=1, device_id=dev, device_id_type=MESH))

    signal(barrier, pair)
    signal(barrier, (up + 2, down), z < last)
    signal(barrier, (up - 2, down), z > high)
    for d in (right, left):
        signal(barrier, (up, d), d > down)

    def by_block(src, dst, sem):
        return [pltpu.make_async_copy(src.at[:, b * BLOCK:(b + 1) * BLOCK], dst.at[b], sem) for b in range(dst.shape[0])]

    def loaded(ref, sem):
        pltpu.make_async_copy(ref, ref, sem).wait()

    load_downb = pltpu.make_async_copy(downb_in, downb, load_sem.at[0])
    load_upb = pltpu.make_async_copy(upb_in, upb, load_sem.at[4])
    load_dec = pltpu.make_async_copy(dec, dec_all.at[down], load_sem.at[3])
    for copy in (
        load_downb, *by_block(grads, grad_raw, load_sem.at[1]), load_dec, *by_block(enc, enc_raw, load_sem.at[2]),
        load_upb, *by_block(deltas, del_raw, load_sem.at[5]),
    ):
        copy.start()

    def remote(src, dst, kind, recv, dev):
        return pltpu.make_async_remote_copy(
            src, dst, send_sem.at[kind], recv, device_id=dev, device_id_type=MESH)

    def dec_half(r, i, owner):
        m = (i + r) % 2
        ref = dec_all.at[owner, m * part:(m + 1) * part]
        return remote(ref, ref, 0, dec_recv.at[i], ring_to[r])

    def dec_relay(r, i, owner):
        ref = dec_all.at[owner, r * part:(r + 1) * part, (body if i else 0):(depth if i else body)]
        return remote(ref, ref, 0, dec_recv.at[2 + i], ring_to[r])

    def enc_rows(level, c):
        return pl.ds(pl.multiple_of((level * 2 + c) * height, 16), height)

    def enc_a(level, c):
        return pl.ds(pl.multiple_of((level * 2 + c) * height + (1 - c) * TAIL, 16), height - TAIL)

    def enc_b(level, c):
        return pl.ds(pl.multiple_of((level * 2 + c) * height + c * (height - TAIL), 16), TAIL)

    def enc_copy(r, level, h, where, sem):
        ref = enc_all.at[h, where(level, core)]
        return remote(ref, ref, 1, enc_recv.at[sem], (up + 2 * step_of[r], down))

    def pair_copy(ref, sem):
        return remote(ref, ref, 2, pair_recv.at[sem], pair)

    def del_copy(r, owner):
        ref = del_all.at[owner]
        return remote(ref, ref, 3, del_recv.at[0], ring_to[r])

    def del_relay(r, owner):
        ref = del_all.at[owner, r]
        return remote(ref, ref, 3, del_recv.at[1], ring_to[r])

    def grad_rows(level, c):
        return grad_all.at[pl.ds(pl.multiple_of((level * 2 + c) * toks, toks), toks)]

    def grad_copy(r, level):
        ref = grad_rows(level, core)
        return remote(ref, ref, 4, grad_recv.at[level], (up + 2 * step_of[r], down))

    def pair_grad(level):
        ref = grad_rows(level, core)
        return remote(ref, ref, 5, pg_recv.at[0], pair)

    def pick_enc(h):
        for s in range(h * dact // 2, (h + 1) * dact // 2):
            at = s * BLOCK - h * half
            enc_all[h, pl.ds(pl.multiple_of(up * height, 16), height), at:at + BLOCK] = enc_raw[chosen[s]]

    load_downb.wait()
    chosen = [within(downb[s], blocks) for s in range(dact)]
    loaded(grad_raw, load_sem.at[1])
    for s in range(dact):
        grad_all[pl.ds(pl.multiple_of(up * toks, toks), toks), s * BLOCK:(s + 1) * BLOCK] = grad_raw[chosen[s]]
    pl.semaphore_wait(barrier, 3 - later + jnp.where(z > 0, 1, 0) + jnp.where(z >= high, 1, 0) - jnp.where(z == last, 1, 0))
    signal(ready_z, (up - 2, down), jnp.logical_and(z > 0, z <= high))
    for d in (right, left):
        signal(ready_xy, (up, d), d < down)

    early = (jnp.logical_and(z >= high, z < last), z > 0)

    def send_own(which, act):
        for r in (1, 0):
            @pl.when(which[r])
            def _():
                act(r)

    send_own(early, lambda r: grad_copy(r, z).start())
    load_dec.wait()

    @pl.when(later == 0)
    def _():
        for r in range(2):
            dec_half(r, 0, down).start()
    loaded(enc_raw, load_sem.at[2])
    pick_enc(0)
    send_own(early, lambda r: enc_copy(r, z, 0, enc_rows, 2 * z).start())
    pick_enc(1)

    @pl.when(later > 0)
    def _():
        pl.semaphore_wait(ready_xy, later)
        for r in range(2):
            dec_half(r, 0, down).start()
    pair_copy(enc_all.at[:, enc_rows(z, core)], z).start()
    load_upb.wait()
    loaded(del_raw, load_sem.at[5])
    for w in range(wins):
        for s in range(uact):
            del_all[down, w, s] = del_raw[within(upb[s, down * wins + w], rows // BLOCK), w * win:(w + 1) * win]
    for r in range(2):
        del_copy(r, down).start()
    for r in range(2):
        dec_half(r, 1, down).start()

    def each(j, act):
        for r in range(2):
            level = z - step_of[r] * j

            @pl.when(inside(level))
            def _():
                act(r, level)

    def relay_grad(r, level):
        grad_copy(r, level).wait_recv()

        @pl.when(can_go[r])
        def _():
            grad_copy(r, level).start()
        pair_grad(level).start()

    @pl.when(z < high)
    def _():
        pl.semaphore_wait(ready_z, 1)
        grad_copy(0, z).start()
        enc_copy(0, z, 0, enc_rows, 2 * z).start()
    pair_grad(z).start()
    each(1, relay_grad)
    send_own(can_go, lambda r: enc_copy(r, z, 1, enc_rows, 2 * z + 1).start())

    acc[...] = jnp.zeros_like(acc)

    def mult(q, rs, n, start=0, size=depth):
        ks = pl.ds(pl.multiple_of(start, BLOCK), size)
        result = jnp.dot(
            dec_all[q, rs, ks], enc_all[n, pl.ds(pl.multiple_of(q * depth + start, BLOCK), size), :],
            preferred_element_type=F32)
        for i in range(half // BLOCK):
            acc[n * (half // BLOCK) + i, rs] += result[:, i * BLOCK:(i + 1) * BLOCK]

    def enc_stage(q, n):
        gap = jnp.maximum(q - z, z - q)
        return jnp.where(gap == last, 5 + n, 2 * gap)

    def products(low, high):
        @pl.loop(0, 4 * levels)
        def _(u):
            q, m, n = u // 4, u // 2 % 2, u % 2
            first = jnp.where(jnp.where(q == left, 1, 0) + m == 1, 2, 4)
            stage = jnp.maximum(enc_stage(q, n), jnp.where(q == down, 0, first))
            ready = jnp.logical_and(stage >= low, stage <= high)

            @pl.when(jnp.logical_and(ready, q != diag))
            def _():
                mult(q, pl.ds(pl.multiple_of(m * part, part), part), n)

    everything = slice(0, rows)

    def diag_products(i):
        for n in range(2):
            @pl.when(enc_stage(diag, n) <= 5)
            def _():
                mult(diag, everything, n, body if i else 0, TAIL if i else body)

    def pair_whole(level):
        return pair_copy(enc_all.at[:, enc_rows(level, 1 - core)], level)

    def relay(j, h):
        def act(r, level):
            enc_copy(r, level, h, enc_rows, 2 * level + h).wait_recv()

            @pl.when(can_go[r])
            def _():
                if j == last - 1 and h == 1:
                    enc_copy(r, level, h, enc_a, 2 * level + h).start()
                    enc_copy(r, level, h, enc_b, 2 * levels).start()
                else:
                    enc_copy(r, level, h, enc_rows, 2 * level + h).start()
            if h == 1:
                pair_copy(enc_all.at[:, enc_rows(level, core)], level).start()
        each(j, act)

    relay(1, 0)
    each(2, relay_grad)
    relay(1, 1)
    loaded(dec_all.at[left], dec_recv.at[0])
    loaded(del_all.at[pl.ds(0, 2)], del_recv.at[0])
    for r in range(2):
        del_relay(r, ring_from[r]).start()
        for i in range(2):
            dec_relay(r, i, ring_from[r]).start()
    pair_whole(z).wait_recv()
    each(1, lambda r, level: pair_whole(level).wait_recv())
    products(0, 2)
    each(3, relay_grad)
    relay(2, 0)

    relay(2, 1)
    loaded(dec_all.at[left], dec_recv.at[1])
    each(2, lambda r, level: pair_whole(level).wait_recv())
    products(3, 4)

    loaded(del_all.at[diag], del_recv.at[1])
    loaded(grad_all.at[pl.ds(0, levels * toks)], pg_recv.at[0])
    for d in range(n_down):
        for w in range(wins):
            for b in range(rows // BLOCK):
                hits = hits_of(b, [upb[s, d * wins + w] for s in range(uact)])
                slot = within(sum(s * hit for s, hit in enumerate(hits)), uact)
                t = (d * wins + w) * win
                masked[t:t + win, b * BLOCK:(b + 1) * BLOCK] = del_all[d, w, slot] * flag(sum(hits), 1, masked.dtype)
    whole = lax.dot_general(
        masked[...], grad_all[...], (((0,), (0,)), ((), ())), preferred_element_type=F32)
    for s in range(dact):
        prod[s] = whole[:, s * BLOCK:(s + 1) * BLOCK]
    prod[dact] = jnp.zeros((rows, BLOCK), F32)

    far = last - z

    def end_wait(h, where, sem):
        for r in range(2):
            @pl.when(z == (0 if r else last))
            def _():
                enc_copy(r, far, h, where, sem).wait_recv()

    @pl.when(at_end)
    def _():
        end_wait(0, enc_rows, 2 * far)
        pair_copy(enc_all.at[0, enc_rows(far, core)], far).start()
        pair_copy(enc_all.at[0, enc_rows(far, 1 - core)], far).wait_recv()

        @pl.when(far != diag)
        def _():
            mult(far, everything, 0)

    def first_relay():
        loaded(dec_all.at[diag, :, :body], dec_recv.at[2])
        diag_products(0)

    def inner():
        pair_copy(enc_all.at[1, enc_a(far, 1 - core)], levels).wait_recv()
        mult(far, everything, 1, core * TAIL, depth - TAIL)

    @pl.when(at_end)
    def _():
        pl.when(core == 1)(first_relay)
        end_wait(1, enc_a, 2 * far + 1)
        pair_copy(enc_all.at[1, enc_a(far, core)], levels).start()
        pl.when(core == 0)(first_relay)
        end_wait(1, enc_b, 2 * levels)
        pair_copy(enc_all.at[1, enc_b(far, core)], levels + 1).start()
        pl.when(core == 0)(inner)
    pl.when(jnp.logical_not(at_end))(first_relay)
    loaded(dec_all.at[diag, :, body:], dec_recv.at[3])
    diag_products(1)

    @pl.when(at_end)
    def _():
        pl.when(core == 1)(inner)
        pair_copy(enc_all.at[1, enc_b(far, 1 - core)], levels + 1).wait_recv()
        mult(far, everything, 1, (1 - core) * (depth - TAIL), TAIL)

    tile = 64
    places = []
    for c in range(blocks):
        hits = hits_of(c, [downb[s] for s in range(dact)])
        slot = sum(s * hit for s, hit in enumerate(hits))
        places.append((within(slot, dact), within(slot + dact * (1 - sum(hits)), dact + 1)))

    @pl.loop(0, rows // tile)
    def _(t):
        rs = pl.ds(pl.multiple_of(t * tile, tile), tile)
        for c, (slot, factor) in enumerate(places):
            out[rs, c * BLOCK:(c + 1) * BLOCK] = acc[slot, rs] * prod[factor, rs]

    def sent(ref, kind):
        pltpu.make_async_copy(ref, ref, send_sem.at[kind]).wait()

    sent(dec_all.at[pl.ds(0, 3)], 0)

    @pl.when(at_end)
    def _():
        sent(enc_all.at[:, pl.ds(0, height)], 1)
        sent(grad_all.at[pl.ds(0, toks)], 4)

    @pl.when(jnp.logical_not(at_end))
    def _():
        sent(enc_all.at[:, pl.ds(0, (levels + 1) * height)], 1)
        sent(grad_all.at[pl.ds(0, (levels + 1) * toks)], 4)
    sent(enc_all.at[:, pl.ds(0, levels * height)], 2)
    sent(del_all.at[pl.ds(0, n_down - 1)], 3)
    sent(grad_all.at[pl.ds(0, levels * toks)], 5)


def ring_local(n_up, n_down, win, deltas, gradients, up_blocks, down_blocks, decoder, encoder):
    rows, depth = decoder.shape
    height, cols = encoder.shape
    toks = gradients.shape[0]
    uact, dact = up_blocks.shape[1], down_blocks.shape[0]
    tokens = deltas.shape[0] * n_down
    wins = deltas.shape[0] // win
    used = dact * BLOCK
    levels = n_up // 2
    kind = decoder.dtype
    dma = pltpu.SemaphoreType.DMA
    hbm = pl.BlockSpec(memory_space=pltpu.HBM)
    return pl.pallas_call(
        functools.partial(gather_scores, n_up, n_down),
        out_shape=jax.ShapeDtypeStruct((rows, cols), F32),
        in_specs=[hbm] * 6,
        out_specs=pl.BlockSpec(memory_space=pltpu.VMEM),
        scratch_shapes=[
            pltpu.SMEM((uact, up_blocks.shape[0]), jnp.int32),
            pltpu.SMEM((dact,), jnp.int32),
            pltpu.VMEM((n_down, rows, depth), kind),
            pltpu.VMEM((cols // BLOCK, height, BLOCK), kind),
            pltpu.VMEM((2, n_up * height, used // 2), kind),
            pltpu.VMEM((rows // BLOCK, deltas.shape[0], BLOCK), kind),
            pltpu.VMEM((n_down, wins, uact, win, BLOCK), kind),
            pltpu.VMEM((cols // BLOCK, toks, BLOCK), kind),
            pltpu.VMEM((n_up * toks, used), kind),
            pltpu.VMEM((tokens, rows), kind),
            pltpu.VMEM((dact, rows, BLOCK), F32),
            pltpu.VMEM((dact + 1, rows, BLOCK), F32),
            dma((6,)),
            dma((6,)),
            dma((4,)),
            dma((2,)),
            dma((2 * levels + 1,)),
            dma((levels + 2,)),
            dma((levels,)),
            dma((1,)),
            pltpu.SemaphoreType.REGULAR,
            pltpu.SemaphoreType.REGULAR,
        ],
        compiler_params=pltpu.CompilerParams(collective_id=0, has_side_effects=True, vmem_limit_bytes=LARGE),
        name="gather_scores",
    )(*[pltpu.with_memory_space_constraint(x, pltpu.HBM) for x in (up_blocks.T, down_blocks, deltas, gradients, decoder, encoder)])


def plain_local(deltas, gradients, up_blocks, down_blocks, decoder, encoder):
    token_deltas = lax.all_gather(deltas, "down", axis=0, tiled=True)
    token_grads = lax.all_gather(gradients, "up", axis=0, tiled=True)
    tokens, rows = token_deltas.shape
    windows, dact = up_blocks.shape[0], down_blocks.shape[0]
    row_blocks, col_blocks = rows // BLOCK, encoder.shape[1] // BLOCK
    local_ids = jnp.arange(row_blocks, dtype=jnp.int32)
    block_on = jnp.any(up_blocks[:, :, None] == local_ids[None, None, :], axis=1)
    masked = token_deltas.reshape(windows, tokens // windows, row_blocks, BLOCK) * block_on[
        :, None, :, None].astype(token_deltas.dtype)
    masked = masked.reshape(tokens, rows)
    dec_whole = lax.all_gather(decoder, "down", axis=1, tiled=True)
    height = encoder.shape[0]
    enc_used = jnp.take(encoder.reshape(height, col_blocks, BLOCK), down_blocks, axis=1).reshape(height, dact * BLOCK)
    virtual = jnp.dot(dec_whole, lax.all_gather(enc_used, "up", axis=0, tiled=True), preferred_element_type=F32)
    grad_used = jnp.take(token_grads.reshape(tokens, col_blocks, BLOCK), down_blocks, axis=1).reshape(tokens, dact * BLOCK)
    product = lax.dot_general(masked, grad_used, (((0,), (0,)), ((), ())), preferred_element_type=F32)
    scored = (product * virtual).reshape(rows, dact, BLOCK)
    filled = jnp.zeros((rows, col_blocks, BLOCK), F32).at[:, down_blocks, :].set(scored)
    return filled.reshape(rows, encoder.shape[1])


def solution(mesh):
    n_up, n_down = mesh.shape["up"], mesh.shape["down"]
    ringed = n_down == 4 and n_up == 2 * n_down

    def local(deltas, gradients, up_blocks, down_blocks, decoder, encoder):
        args = (deltas, gradients, up_blocks, down_blocks, decoder, encoder)
        tokens = deltas.shape[0] * n_down
        win = tokens // up_blocks.shape[0]
        if ringed and deltas.shape[0] == 2 * win:
            return ring_local(n_up, n_down, win, *args)
        return plain_local(*args)

    placed = (P("down", "up"), P("up", "down"), P(None, "up"), P("down"), P("up", "down"), P("up", "down"))
    return jax.shard_map(local, mesh=mesh, in_specs=placed, out_specs=P("up", "down"), check_vma=False)
```

```python
import functools

import jax
import jax.numpy as jnp
from jax import lax
from jax.experimental import pallas as pl
from jax.experimental.pallas import tpu as pltpu
from jax.sharding import PartitionSpec as P

BLOCK = 128
TAIL = 128
LARGE = 24 << 20
MESH = pl.DeviceIdType.MESH
F32 = jnp.float32


def flag(number, block, kind):
    return jnp.where(jnp.full((1, BLOCK), number, jnp.int32) == block, 1.0, 0.0).astype(kind)


def within(number, count):
    return jnp.maximum(jnp.minimum(number, count - 1), 0)


def hits_of(number, slots):
    return [1 - jnp.minimum(jnp.abs(slot - number), 1) for slot in slots]


def gather_scores(
    n_up, n_down, upb_in, downb_in, deltas, grads, dec, enc, out,
    upb, downb, dec_all, enc_raw, enc_all, del_raw, del_all, grad_raw, grad_all, masked, acc, prod,
    load_sem, send_sem, dec_recv, del_recv, enc_recv, pair_recv, grad_recv, pg_recv, ready_z, ready_xy,
):
    levels = n_up // 2
    rows, depth = dec.shape
    height = enc.shape[0]
    half = enc_all.shape[2]
    part = rows // 2
    body = depth - TAIL
    toks = grads.shape[0]
    wins, uact, win = del_all.shape[1:4]
    dact = downb.shape[0]
    blocks = enc.shape[1] // BLOCK
    up, down = lax.axis_index("up"), lax.axis_index("down")
    z, core = up // 2, up % 2
    place = lambda d: 2 * (d // 2) + (d + d // 2) % 2
    pos = place(down)
    right, left = place((pos + 1) % 4), place((pos + 3) % 4)
    diag = place((pos + 2) % 4)
    ring_to = ((up, right), (up, left))
    ring_from = (left, right)
    step_of = (1, -1)
    pair = (2 * z + 1 - core, down)
    can_go = (z < levels - 1, z > 0)
    last = levels - 1
    at_end = jnp.logical_or(z == 0, z == last)
    inside = lambda level: jnp.logical_and(level >= 0, level < levels)

    high = levels // 2
    later = jnp.where(right > down, 1, 0) + jnp.where(left > down, 1, 0)
    barrier = pltpu.get_barrier_semaphore()

    def signal(sem, dev, when=None):
        if when is None:
            pl.semaphore_signal(sem, inc=1, device_id=dev, device_id_type=MESH)
        else:
            pl.when(when)(lambda: pl.semaphore_signal(sem, inc=1, device_id=dev, device_id_type=MESH))

    signal(barrier, pair)
    signal(barrier, (up + 2, down), z < last)
    signal(barrier, (up - 2, down), z > high)
    for d in (right, left):
        signal(barrier, (up, d), d > down)

    def by_block(src, dst, sem):
        return [pltpu.make_async_copy(src.at[:, b * BLOCK:(b + 1) * BLOCK], dst.at[b], sem) for b in range(dst.shape[0])]

    def loaded(ref, sem):
        pltpu.make_async_copy(ref, ref, sem).wait()

    load_downb = pltpu.make_async_copy(downb_in, downb, load_sem.at[0])
    load_upb = pltpu.make_async_copy(upb_in, upb, load_sem.at[4])
    load_dec = pltpu.make_async_copy(dec, dec_all.at[down], load_sem.at[3])
    for copy in (
        load_downb, *by_block(grads, grad_raw, load_sem.at[1]), *by_block(enc, enc_raw, load_sem.at[2]), load_dec,
        load_upb, *by_block(deltas, del_raw, load_sem.at[5]),
    ):
        copy.start()

    def remote(src, dst, kind, recv, dev):
        return pltpu.make_async_remote_copy(
            src, dst, send_sem.at[kind], recv, device_id=dev, device_id_type=MESH)

    def dec_half(r, i, owner):
        m = (i + r) % 2
        ref = dec_all.at[owner, m * part:(m + 1) * part]
        return remote(ref, ref, 0, dec_recv.at[i], ring_to[r])

    def dec_relay(r, i, owner):
        ref = dec_all.at[owner, r * part:(r + 1) * part, (body if i else 0):(depth if i else body)]
        return remote(ref, ref, 0, dec_recv.at[2 + i], ring_to[r])

    def enc_rows(level, c):
        return pl.ds(pl.multiple_of((level * 2 + c) * height, 16), height)

    def enc_a(level, c):
        return pl.ds(pl.multiple_of((level * 2 + c) * height + (1 - c) * TAIL, 16), height - TAIL)

    def enc_b(level, c):
        return pl.ds(pl.multiple_of((level * 2 + c) * height + c * (height - TAIL), 16), TAIL)

    def enc_copy(r, level, h, where, sem):
        ref = enc_all.at[h, where(level, core)]
        return remote(ref, ref, 1, enc_recv.at[sem], (up + 2 * step_of[r], down))

    def pair_copy(ref, sem):
        return remote(ref, ref, 2, pair_recv.at[sem], pair)

    def del_copy(r, owner):
        ref = del_all.at[owner]
        return remote(ref, ref, 3, del_recv.at[0], ring_to[r])

    def del_relay(r, owner):
        ref = del_all.at[owner, r]
        return remote(ref, ref, 3, del_recv.at[1], ring_to[r])

    def grad_rows(level, c):
        return grad_all.at[pl.ds(pl.multiple_of((level * 2 + c) * toks, toks), toks)]

    def grad_copy(r, level):
        ref = grad_rows(level, core)
        return remote(ref, ref, 4, grad_recv.at[level], (up + 2 * step_of[r], down))

    def pair_grad(level):
        ref = grad_rows(level, core)
        return remote(ref, ref, 5, pg_recv.at[0], pair)

    def pick_enc(h):
        for s in range(h * dact // 2, (h + 1) * dact // 2):
            at = s * BLOCK - h * half
            enc_all[h, pl.ds(pl.multiple_of(up * height, 16), height), at:at + BLOCK] = enc_raw[chosen[s]]

    load_downb.wait()
    chosen = [within(downb[s], blocks) for s in range(dact)]
    loaded(grad_raw, load_sem.at[1])
    for s in range(dact):
        grad_all[pl.ds(pl.multiple_of(up * toks, toks), toks), s * BLOCK:(s + 1) * BLOCK] = grad_raw[chosen[s]]
    pl.semaphore_wait(barrier, 3 - later + jnp.where(z > 0, 1, 0) + jnp.where(z >= high, 1, 0) - jnp.where(z == last, 1, 0))
    signal(ready_z, (up - 2, down), jnp.logical_and(z > 0, z <= high))
    for d in (right, left):
        signal(ready_xy, (up, d), d < down)

    early = (jnp.logical_and(z >= high, z < last), z > 0)

    def send_own(which, act):
        for r in (1, 0):
            @pl.when(which[r])
            def _():
                act(r)

    send_own(early, lambda r: grad_copy(r, z).start())
    loaded(enc_raw, load_sem.at[2])
    pick_enc(0)
    send_own(early, lambda r: enc_copy(r, z, 0, enc_rows, 2 * z).start())
    load_dec.wait()

    for r, d in enumerate((right, left)):
        @pl.when(d < down)
        def _():
            dec_half(r, 0, down).start()
    pick_enc(1)

    @pl.when(later > 0)
    def _():
        pl.semaphore_wait(ready_xy, later)
        for r, d in enumerate((right, left)):
            @pl.when(d > down)
            def _():
                dec_half(r, 0, down).start()
    pair_copy(enc_all.at[:, enc_rows(z, core)], z).start()
    load_upb.wait()
    loaded(del_raw, load_sem.at[5])
    for w in range(wins):
        for s in range(uact):
            del_all[down, w, s] = del_raw[within(upb[s, down * wins + w], rows // BLOCK), w * win:(w + 1) * win]
    for r in range(2):
        del_copy(r, down).start()
    for r in range(2):
        dec_half(r, 1, down).start()

    def each(j, act):
        for r in range(2):
            level = z - step_of[r] * j

            @pl.when(inside(level))
            def _():
                act(r, level)

    def relay_grad(r, level):
        grad_copy(r, level).wait_recv()

        @pl.when(can_go[r])
        def _():
            grad_copy(r, level).start()
        pair_grad(level).start()

    @pl.when(z < high)
    def _():
        pl.semaphore_wait(ready_z, 1)
        grad_copy(0, z).start()
        enc_copy(0, z, 0, enc_rows, 2 * z).start()
    pair_grad(z).start()
    each(1, relay_grad)
    send_own(can_go, lambda r: enc_copy(r, z, 1, enc_rows, 2 * z + 1).start())

    acc[...] = jnp.zeros_like(acc)

    def mult(q, rs, n, start=0, size=depth):
        ks = pl.ds(pl.multiple_of(start, BLOCK), size)
        result = jnp.dot(
            dec_all[q, rs, ks], enc_all[n, pl.ds(pl.multiple_of(q * depth + start, BLOCK), size), :],
            preferred_element_type=F32)
        for i in range(half // BLOCK):
            acc[n * (half // BLOCK) + i, rs] += result[:, i * BLOCK:(i + 1) * BLOCK]

    def enc_stage(q, n):
        gap = jnp.maximum(q - z, z - q)
        return jnp.where(gap == last, 5 + n, 2 * gap)

    def products(low, high):
        @pl.loop(0, 4 * levels)
        def _(u):
            q, m, n = u // 4, u // 2 % 2, u % 2
            first = jnp.where(jnp.where(q == left, 1, 0) + m == 1, 2, 4)
            stage = jnp.maximum(enc_stage(q, n), jnp.where(q == down, 0, first))
            ready = jnp.logical_and(stage >= low, stage <= high)

            @pl.when(jnp.logical_and(ready, q != diag))
            def _():
                mult(q, pl.ds(pl.multiple_of(m * part, part), part), n)

    everything = slice(0, rows)

    def diag_products(i):
        for n in range(2):
            @pl.when(enc_stage(diag, n) <= 5)
            def _():
                mult(diag, everything, n, body if i else 0, TAIL if i else body)

    def pair_whole(level):
        return pair_copy(enc_all.at[:, enc_rows(level, 1 - core)], level)

    def relay(j, h):
        def act(r, level):
            enc_copy(r, level, h, enc_rows, 2 * level + h).wait_recv()

            @pl.when(can_go[r])
            def _():
                if j == last - 1 and h == 1:
                    enc_copy(r, level, h, enc_a, 2 * level + h).start()
                    enc_copy(r, level, h, enc_b, 2 * levels).start()
                else:
                    enc_copy(r, level, h, enc_rows, 2 * level + h).start()
            if h == 1:
                pair_copy(enc_all.at[:, enc_rows(level, core)], level).start()
        each(j, act)

    relay(1, 0)
    each(2, relay_grad)
    relay(1, 1)
    loaded(dec_all.at[left], dec_recv.at[0])
    loaded(del_all.at[pl.ds(0, 2)], del_recv.at[0])
    for r in range(2):
        del_relay(r, ring_from[r]).start()
        for i in range(2):
            dec_relay(r, i, ring_from[r]).start()
    pair_whole(z).wait_recv()
    each(1, lambda r, level: pair_whole(level).wait_recv())
    products(0, 2)
    each(3, relay_grad)
    relay(2, 0)

    relay(2, 1)
    loaded(dec_all.at[left], dec_recv.at[1])
    each(2, lambda r, level: pair_whole(level).wait_recv())
    products(3, 4)

    loaded(del_all.at[diag], del_recv.at[1])
    loaded(grad_all.at[pl.ds(0, levels * toks)], pg_recv.at[0])
    for d in range(n_down):
        for w in range(wins):
            for b in range(rows // BLOCK):
                hits = hits_of(b, [upb[s, d * wins + w] for s in range(uact)])
                slot = within(sum(s * hit for s, hit in enumerate(hits)), uact)
                t = (d * wins + w) * win
                masked[t:t + win, b * BLOCK:(b + 1) * BLOCK] = del_all[d, w, slot] * flag(sum(hits), 1, masked.dtype)
    whole = lax.dot_general(
        masked[...], grad_all[...], (((0,), (0,)), ((), ())), preferred_element_type=F32)
    for s in range(dact):
        prod[s] = whole[:, s * BLOCK:(s + 1) * BLOCK]
    prod[dact] = jnp.zeros((rows, BLOCK), F32)

    far = last - z

    def end_wait(h, where, sem):
        for r in range(2):
            @pl.when(z == (0 if r else last))
            def _():
                enc_copy(r, far, h, where, sem).wait_recv()

    @pl.when(at_end)
    def _():
        end_wait(0, enc_rows, 2 * far)
        pair_copy(enc_all.at[0, enc_rows(far, core)], far).start()
        pair_copy(enc_all.at[0, enc_rows(far, 1 - core)], far).wait_recv()

        @pl.when(far != diag)
        def _():
            mult(far, everything, 0)

    def first_relay():
        loaded(dec_all.at[diag, :, :body], dec_recv.at[2])
        diag_products(0)

    def inner():
        pair_copy(enc_all.at[1, enc_a(far, 1 - core)], levels).wait_recv()
        mult(far, everything, 1, core * TAIL, depth - TAIL)

    @pl.when(at_end)
    def _():
        pl.when(core == 1)(first_relay)
        end_wait(1, enc_a, 2 * far + 1)
        pair_copy(enc_all.at[1, enc_a(far, core)], levels).start()
        pl.when(core == 0)(first_relay)
        end_wait(1, enc_b, 2 * levels)
        pair_copy(enc_all.at[1, enc_b(far, core)], levels + 1).start()
        pl.when(core == 0)(inner)
    pl.when(jnp.logical_not(at_end))(first_relay)
    loaded(dec_all.at[diag, :, body:], dec_recv.at[3])
    diag_products(1)

    @pl.when(at_end)
    def _():
        pl.when(core == 1)(inner)
        pair_copy(enc_all.at[1, enc_b(far, 1 - core)], levels + 1).wait_recv()
        mult(far, everything, 1, (1 - core) * (depth - TAIL), TAIL)

    tile = 64
    places = []
    for c in range(blocks):
        hits = hits_of(c, [downb[s] for s in range(dact)])
        slot = sum(s * hit for s, hit in enumerate(hits))
        places.append((within(slot, dact), within(slot + dact * (1 - sum(hits)), dact + 1)))

    @pl.loop(0, rows // tile)
    def _(t):
        rs = pl.ds(pl.multiple_of(t * tile, tile), tile)
        for c, (slot, factor) in enumerate(places):
            out[rs, c * BLOCK:(c + 1) * BLOCK] = acc[slot, rs] * prod[factor, rs]

    def sent(ref, kind):
        pltpu.make_async_copy(ref, ref, send_sem.at[kind]).wait()

    sent(dec_all.at[pl.ds(0, 3)], 0)

    @pl.when(at_end)
    def _():
        sent(enc_all.at[:, pl.ds(0, height)], 1)
        sent(grad_all.at[pl.ds(0, toks)], 4)

    @pl.when(jnp.logical_not(at_end))
    def _():
        sent(enc_all.at[:, pl.ds(0, (levels + 1) * height)], 1)
        sent(grad_all.at[pl.ds(0, (levels + 1) * toks)], 4)
    sent(enc_all.at[:, pl.ds(0, levels * height)], 2)
    sent(del_all.at[pl.ds(0, n_down - 1)], 3)
    sent(grad_all.at[pl.ds(0, levels * toks)], 5)


def ring_local(n_up, n_down, win, deltas, gradients, up_blocks, down_blocks, decoder, encoder):
    rows, depth = decoder.shape
    height, cols = encoder.shape
    toks = gradients.shape[0]
    uact, dact = up_blocks.shape[1], down_blocks.shape[0]
    tokens = deltas.shape[0] * n_down
    wins = deltas.shape[0] // win
    used = dact * BLOCK
    levels = n_up // 2
    kind = decoder.dtype
    dma = pltpu.SemaphoreType.DMA
    hbm = pl.BlockSpec(memory_space=pltpu.HBM)
    return pl.pallas_call(
        functools.partial(gather_scores, n_up, n_down),
        out_shape=jax.ShapeDtypeStruct((rows, cols), F32),
        in_specs=[hbm] * 6,
        out_specs=pl.BlockSpec(memory_space=pltpu.VMEM),
        scratch_shapes=[
            pltpu.SMEM((uact, up_blocks.shape[0]), jnp.int32),
            pltpu.SMEM((dact,), jnp.int32),
            pltpu.VMEM((n_down, rows, depth), kind),
            pltpu.VMEM((cols // BLOCK, height, BLOCK), kind),
            pltpu.VMEM((2, n_up * height, used // 2), kind),
            pltpu.VMEM((rows // BLOCK, deltas.shape[0], BLOCK), kind),
            pltpu.VMEM((n_down, wins, uact, win, BLOCK), kind),
            pltpu.VMEM((cols // BLOCK, toks, BLOCK), kind),
            pltpu.VMEM((n_up * toks, used), kind),
            pltpu.VMEM((tokens, rows), kind),
            pltpu.VMEM((dact, rows, BLOCK), F32),
            pltpu.VMEM((dact + 1, rows, BLOCK), F32),
            dma((6,)),
            dma((6,)),
            dma((4,)),
            dma((2,)),
            dma((2 * levels + 1,)),
            dma((levels + 2,)),
            dma((levels,)),
            dma((1,)),
            pltpu.SemaphoreType.REGULAR,
            pltpu.SemaphoreType.REGULAR,
        ],
        compiler_params=pltpu.CompilerParams(collective_id=0, has_side_effects=True, vmem_limit_bytes=LARGE),
        name="gather_scores",
    )(*[pltpu.with_memory_space_constraint(x, pltpu.HBM) for x in (up_blocks.T, down_blocks, deltas, gradients, decoder, encoder)])


def plain_local(deltas, gradients, up_blocks, down_blocks, decoder, encoder):
    token_deltas = lax.all_gather(deltas, "down", axis=0, tiled=True)
    token_grads = lax.all_gather(gradients, "up", axis=0, tiled=True)
    tokens, rows = token_deltas.shape
    windows, dact = up_blocks.shape[0], down_blocks.shape[0]
    row_blocks, col_blocks = rows // BLOCK, encoder.shape[1] // BLOCK
    local_ids = jnp.arange(row_blocks, dtype=jnp.int32)
    block_on = jnp.any(up_blocks[:, :, None] == local_ids[None, None, :], axis=1)
    masked = token_deltas.reshape(windows, tokens // windows, row_blocks, BLOCK) * block_on[
        :, None, :, None].astype(token_deltas.dtype)
    masked = masked.reshape(tokens, rows)
    dec_whole = lax.all_gather(decoder, "down", axis=1, tiled=True)
    height = encoder.shape[0]
    enc_used = jnp.take(encoder.reshape(height, col_blocks, BLOCK), down_blocks, axis=1).reshape(height, dact * BLOCK)
    virtual = jnp.dot(dec_whole, lax.all_gather(enc_used, "up", axis=0, tiled=True), preferred_element_type=F32)
    grad_used = jnp.take(token_grads.reshape(tokens, col_blocks, BLOCK), down_blocks, axis=1).reshape(tokens, dact * BLOCK)
    product = lax.dot_general(masked, grad_used, (((0,), (0,)), ((), ())), preferred_element_type=F32)
    scored = (product * virtual).reshape(rows, dact, BLOCK)
    filled = jnp.zeros((rows, col_blocks, BLOCK), F32).at[:, down_blocks, :].set(scored)
    return filled.reshape(rows, encoder.shape[1])


def solution(mesh):
    n_up, n_down = mesh.shape["up"], mesh.shape["down"]
    ringed = n_down == 4 and n_up == 2 * n_down

    def local(deltas, gradients, up_blocks, down_blocks, decoder, encoder):
        args = (deltas, gradients, up_blocks, down_blocks, decoder, encoder)
        tokens = deltas.shape[0] * n_down
        win = tokens // up_blocks.shape[0]
        if ringed and deltas.shape[0] == 2 * win:
            return ring_local(n_up, n_down, win, *args)
        return plain_local(*args)

    placed = (P("down", "up"), P("up", "down"), P(None, "up"), P("down"), P("up", "down"), P("up", "down"))
    return jax.shard_map(local, mesh=mesh, in_specs=placed, out_specs=P("up", "down"), check_vma=False)
```

```python
import functools

import jax
import jax.numpy as jnp
from jax import lax
from jax.experimental import pallas as pl
from jax.experimental.pallas import tpu as pltpu
from jax.sharding import PartitionSpec as P

BLOCK = 128
TAIL = 128
LARGE, SMALL = 24 << 20, 8 << 20
MESH = pl.DeviceIdType.MESH
F32 = jnp.float32


def flag(number, block, kind):
    return jnp.where(jnp.full((1, BLOCK), number, jnp.int32) == block, 1.0, 0.0).astype(kind)


def within(number, count):
    return jnp.maximum(jnp.minimum(number, count - 1), 0)


def hits_of(number, slots):
    return [1 - jnp.minimum(jnp.abs(slot - number), 1) for slot in slots]


def gather_scores(
    n_up, n_down, upb_in, downb_in, deltas, grads, dec, enc, acc, prod, table,
    upb, downb, dec_all, enc_raw, enc_all, del_raw, del_all, grad_raw, grad_all, masked,
    load_sem, send_sem, dec_recv, del_recv, enc_recv, pair_recv, grad_recv, pg_recv, ready_z, ready_xy,
):
    levels = n_up // 2
    rows, depth = dec.shape
    height = enc.shape[0]
    half = enc_all.shape[2]
    part = rows // 2
    body = depth - TAIL
    toks = grads.shape[0]
    wins, uact, win = del_all.shape[1:4]
    dact = downb.shape[0]
    blocks = enc.shape[1] // BLOCK
    up, down = lax.axis_index("up"), lax.axis_index("down")
    z, core = up // 2, up % 2
    place = lambda d: 2 * (d // 2) + (d + d // 2) % 2
    pos = place(down)
    right, left = place((pos + 1) % 4), place((pos + 3) % 4)
    diag = place((pos + 2) % 4)
    ring_to = ((up, right), (up, left))
    ring_from = (left, right)
    step_of = (1, -1)
    pair = (2 * z + 1 - core, down)
    can_go = (z < levels - 1, z > 0)
    last = levels - 1
    at_end = jnp.logical_or(z == 0, z == last)
    inside = lambda level: jnp.logical_and(level >= 0, level < levels)

    high = levels // 2
    later = jnp.where(right > down, 1, 0) + jnp.where(left > down, 1, 0)
    barrier = pltpu.get_barrier_semaphore()

    def signal(sem, dev, when=None):
        if when is None:
            pl.semaphore_signal(sem, inc=1, device_id=dev, device_id_type=MESH)
        else:
            pl.when(when)(lambda: pl.semaphore_signal(sem, inc=1, device_id=dev, device_id_type=MESH))

    signal(barrier, pair)
    signal(barrier, (up + 2, down), z < last)
    signal(barrier, (up - 2, down), z > high)
    for d in (right, left):
        signal(barrier, (up, d), d > down)

    def by_block(src, dst, sem):
        return [pltpu.make_async_copy(src.at[:, b * BLOCK:(b + 1) * BLOCK], dst.at[b], sem) for b in range(dst.shape[0])]

    def loaded(ref, sem):
        pltpu.make_async_copy(ref, ref, sem).wait()

    load_downb = pltpu.make_async_copy(downb_in, downb, load_sem.at[0])
    load_upb = pltpu.make_async_copy(upb_in, upb, load_sem.at[4])
    load_dec = pltpu.make_async_copy(dec, dec_all.at[down], load_sem.at[3])
    for copy in (
        load_downb, *by_block(grads, grad_raw, load_sem.at[1]), *by_block(enc, enc_raw, load_sem.at[2]), load_dec,
        load_upb, *by_block(deltas, del_raw, load_sem.at[5]),
    ):
        copy.start()

    def remote(src, dst, kind, recv, dev):
        return pltpu.make_async_remote_copy(
            src, dst, send_sem.at[kind], recv, device_id=dev, device_id_type=MESH)

    def dec_half(r, i, owner):
        m = (i + r) % 2
        ref = dec_all.at[owner, m * part:(m + 1) * part]
        return remote(ref, ref, 0, dec_recv.at[i], ring_to[r])

    def dec_relay(r, i, owner):
        ref = dec_all.at[owner, r * part:(r + 1) * part, (body if i else 0):(depth if i else body)]
        return remote(ref, ref, 0, dec_recv.at[2 + i], ring_to[r])

    def enc_rows(level, c):
        return pl.ds(pl.multiple_of((level * 2 + c) * height, 16), height)

    def enc_a(level, c):
        return pl.ds(pl.multiple_of((level * 2 + c) * height + (1 - c) * TAIL, 16), height - TAIL)

    def enc_b(level, c):
        return pl.ds(pl.multiple_of((level * 2 + c) * height + c * (height - TAIL), 16), TAIL)

    def enc_copy(r, level, h, where, sem):
        ref = enc_all.at[h, where(level, core)]
        return remote(ref, ref, 1, enc_recv.at[sem], (up + 2 * step_of[r], down))

    def pair_copy(ref, sem):
        return remote(ref, ref, 2, pair_recv.at[sem], pair)

    def del_copy(r, owner):
        ref = del_all.at[owner]
        return remote(ref, ref, 3, del_recv.at[0], ring_to[r])

    def del_relay(r, owner):
        ref = del_all.at[owner, r]
        return remote(ref, ref, 3, del_recv.at[1], ring_to[r])

    def grad_rows(level, c):
        return grad_all.at[pl.ds(pl.multiple_of((level * 2 + c) * toks, toks), toks)]

    def grad_copy(r, level):
        ref = grad_rows(level, core)
        return remote(ref, ref, 4, grad_recv.at[level], (up + 2 * step_of[r], down))

    def pair_grad(level):
        ref = grad_rows(level, core)
        return remote(ref, ref, 5, pg_recv.at[0], pair)

    def pick_enc(h):
        for s in range(h * dact // 2, (h + 1) * dact // 2):
            at = s * BLOCK - h * half
            enc_all[h, pl.ds(pl.multiple_of(up * height, 16), height), at:at + BLOCK] = enc_raw[chosen[s]]

    load_downb.wait()
    chosen = [within(downb[s], blocks) for s in range(dact)]
    loaded(grad_raw, load_sem.at[1])
    for s in range(dact):
        grad_all[pl.ds(pl.multiple_of(up * toks, toks), toks), s * BLOCK:(s + 1) * BLOCK] = grad_raw[chosen[s]]
    pl.semaphore_wait(barrier, 3 - later + jnp.where(z > 0, 1, 0) + jnp.where(z >= high, 1, 0) - jnp.where(z == last, 1, 0))
    signal(ready_z, (up - 2, down), jnp.logical_and(z > 0, z <= high))
    for d in (right, left):
        signal(ready_xy, (up, d), d < down)

    early = (jnp.logical_and(z >= high, z < last), z > 0)

    def send_own(which, act):
        for r in (1, 0):
            @pl.when(which[r])
            def _():
                act(r)

    send_own(early, lambda r: grad_copy(r, z).start())
    loaded(enc_raw, load_sem.at[2])
    pick_enc(0)
    send_own(early, lambda r: enc_copy(r, z, 0, enc_rows, 2 * z).start())
    load_dec.wait()

    for r, d in enumerate((right, left)):
        @pl.when(d < down)
        def _():
            dec_half(r, 0, down).start()
    pick_enc(1)

    @pl.when(later > 0)
    def _():
        pl.semaphore_wait(ready_xy, later)
        for r, d in enumerate((right, left)):
            @pl.when(d > down)
            def _():
                dec_half(r, 0, down).start()
    pair_copy(enc_all.at[:, enc_rows(z, core)], z).start()
    load_upb.wait()
    loaded(del_raw, load_sem.at[5])
    for w in range(wins):
        for s in range(uact):
            del_all[down, w, s] = del_raw[within(upb[s, down * wins + w], rows // BLOCK), w * win:(w + 1) * win]
    for r in range(2):
        del_copy(r, down).start()
    for r in range(2):
        dec_half(r, 1, down).start()

    def each(j, act):
        for r in range(2):
            level = z - step_of[r] * j

            @pl.when(inside(level))
            def _():
                act(r, level)

    def relay_grad(r, level):
        grad_copy(r, level).wait_recv()

        @pl.when(can_go[r])
        def _():
            grad_copy(r, level).start()
        pair_grad(level).start()

    @pl.when(z < high)
    def _():
        pl.semaphore_wait(ready_z, 1)
        grad_copy(0, z).start()
        enc_copy(0, z, 0, enc_rows, 2 * z).start()
    pair_grad(z).start()
    each(1, relay_grad)
    send_own(can_go, lambda r: enc_copy(r, z, 1, enc_rows, 2 * z + 1).start())

    acc[...] = jnp.zeros_like(acc)

    def mult(q, rs, n, start=0, size=depth):
        ks = pl.ds(pl.multiple_of(start, BLOCK), size)
        result = jnp.dot(
            dec_all[q, rs, ks], enc_all[n, pl.ds(pl.multiple_of(q * depth + start, BLOCK), size), :],
            preferred_element_type=F32)
        for i in range(half // BLOCK):
            acc[n * (half // BLOCK) + i, rs] += result[:, i * BLOCK:(i + 1) * BLOCK]

    def enc_stage(q, n):
        gap = jnp.maximum(q - z, z - q)
        return jnp.where(gap == last, 5 + n, 2 * gap)

    def products(low, high):
        @pl.loop(0, 4 * levels)
        def _(u):
            q, m, n = u // 4, u // 2 % 2, u % 2
            first = jnp.where(jnp.where(q == left, 1, 0) + m == 1, 2, 4)
            stage = jnp.maximum(enc_stage(q, n), jnp.where(q == down, 0, first))
            ready = jnp.logical_and(stage >= low, stage <= high)

            @pl.when(jnp.logical_and(ready, q != diag))
            def _():
                mult(q, pl.ds(pl.multiple_of(m * part, part), part), n)

    everything = slice(0, rows)

    def diag_products(i):
        for n in range(2):
            @pl.when(enc_stage(diag, n) <= 5)
            def _():
                mult(diag, everything, n, body if i else 0, TAIL if i else body)

    def pair_whole(level):
        return pair_copy(enc_all.at[:, enc_rows(level, 1 - core)], level)

    def relay(j, h):
        def act(r, level):
            enc_copy(r, level, h, enc_rows, 2 * level + h).wait_recv()

            @pl.when(can_go[r])
            def _():
                if j == last - 1 and h == 1:
                    enc_copy(r, level, h, enc_a, 2 * level + h).start()
                    enc_copy(r, level, h, enc_b, 2 * levels).start()
                else:
                    enc_copy(r, level, h, enc_rows, 2 * level + h).start()
            if h == 1:
                pair_copy(enc_all.at[:, enc_rows(level, core)], level).start()
        each(j, act)

    relay(1, 0)
    each(2, relay_grad)
    relay(1, 1)
    loaded(dec_all.at[left], dec_recv.at[0])
    loaded(del_all.at[pl.ds(0, 2)], del_recv.at[0])
    for r in range(2):
        del_relay(r, ring_from[r]).start()
        for i in range(2):
            dec_relay(r, i, ring_from[r]).start()
    pair_whole(z).wait_recv()
    each(1, lambda r, level: pair_whole(level).wait_recv())
    products(0, 2)
    each(3, relay_grad)
    relay(2, 0)

    relay(2, 1)
    loaded(dec_all.at[left], dec_recv.at[1])
    each(2, lambda r, level: pair_whole(level).wait_recv())
    products(3, 4)

    loaded(del_all.at[diag], del_recv.at[1])
    loaded(grad_all.at[pl.ds(0, levels * toks)], pg_recv.at[0])
    for d in range(n_down):
        for w in range(wins):
            for b in range(rows // BLOCK):
                hits = hits_of(b, [upb[s, d * wins + w] for s in range(uact)])
                slot = within(sum(s * hit for s, hit in enumerate(hits)), uact)
                t = (d * wins + w) * win
                masked[t:t + win, b * BLOCK:(b + 1) * BLOCK] = del_all[d, w, slot] * flag(sum(hits), 1, masked.dtype)
    whole = lax.dot_general(
        masked[...], grad_all[...], (((0,), (0,)), ((), ())), preferred_element_type=F32)
    for s in range(dact):
        prod[s] = whole[:, s * BLOCK:(s + 1) * BLOCK]
        table[s] = jnp.full(table.shape[1:], downb[s], jnp.int32)

    far = last - z

    def end_wait(h, where, sem):
        for r in range(2):
            @pl.when(z == (0 if r else last))
            def _():
                enc_copy(r, far, h, where, sem).wait_recv()

    @pl.when(at_end)
    def _():
        end_wait(0, enc_rows, 2 * far)
        pair_copy(enc_all.at[0, enc_rows(far, core)], far).start()
        pair_copy(enc_all.at[0, enc_rows(far, 1 - core)], far).wait_recv()

        @pl.when(far != diag)
        def _():
            mult(far, everything, 0)

    def first_relay():
        loaded(dec_all.at[diag, :, :body], dec_recv.at[2])
        diag_products(0)

    def inner():
        pair_copy(enc_all.at[1, enc_a(far, 1 - core)], levels).wait_recv()
        mult(far, everything, 1, core * TAIL, depth - TAIL)

    @pl.when(at_end)
    def _():
        pl.when(core == 1)(first_relay)
        end_wait(1, enc_a, 2 * far + 1)
        pair_copy(enc_all.at[1, enc_a(far, core)], levels).start()
        pl.when(core == 0)(first_relay)
        end_wait(1, enc_b, 2 * levels)
        pair_copy(enc_all.at[1, enc_b(far, core)], levels + 1).start()
        pl.when(core == 0)(inner)
    pl.when(jnp.logical_not(at_end))(first_relay)
    loaded(dec_all.at[diag, :, body:], dec_recv.at[3])
    diag_products(1)

    @pl.when(at_end)
    def _():
        pl.when(core == 1)(inner)
        pair_copy(enc_all.at[1, enc_b(far, 1 - core)], levels + 1).wait_recv()
        mult(far, everything, 1, (1 - core) * (depth - TAIL), TAIL)

    def sent(ref, kind):
        pltpu.make_async_copy(ref, ref, send_sem.at[kind]).wait()

    sent(dec_all.at[pl.ds(0, 3)], 0)

    @pl.when(at_end)
    def _():
        sent(enc_all.at[:, pl.ds(0, height)], 1)
        sent(grad_all.at[pl.ds(0, toks)], 4)

    @pl.when(jnp.logical_not(at_end))
    def _():
        sent(enc_all.at[:, pl.ds(0, (levels + 1) * height)], 1)
        sent(grad_all.at[pl.ds(0, (levels + 1) * toks)], 4)
    sent(enc_all.at[:, pl.ds(0, levels * height)], 2)
    sent(del_all.at[pl.ds(0, n_down - 1)], 3)
    sent(grad_all.at[pl.ds(0, levels * toks)], 5)


def place(acc, prod, table, out, held, sem):
    dact, rows, _ = acc.shape
    blocks = out.shape[1] // BLOCK
    tile = 64

    @pl.loop(0, rows // tile)
    def _(t):
        rs = pl.ds(pl.multiple_of(t * tile, tile), tile)
        values = [acc[s, rs] * prod[s, rs] for s in range(dact)]
        numbers = [jnp.broadcast_to(table[s, 0:1], (tile, BLOCK)) for s in range(dact)]
        for c in range(blocks):
            total = jnp.zeros((tile, BLOCK), F32)
            for value, number in zip(values, numbers):
                total = jnp.where(number == c, value, total)
            held[rs, c * BLOCK:(c + 1) * BLOCK] = total
        pltpu.make_async_copy(held.at[rs], out.at[rs], sem.at[0]).start()

    pltpu.make_async_copy(held, out, sem.at[0]).wait()


def ring_local(n_up, n_down, win, deltas, gradients, up_blocks, down_blocks, decoder, encoder):
    rows, depth = decoder.shape
    height, cols = encoder.shape
    toks = gradients.shape[0]
    uact, dact = up_blocks.shape[1], down_blocks.shape[0]
    tokens = deltas.shape[0] * n_down
    wins = deltas.shape[0] // win
    used = dact * BLOCK
    levels = n_up // 2
    kind = decoder.dtype
    dma = pltpu.SemaphoreType.DMA
    hbm = pl.BlockSpec(memory_space=pltpu.HBM)
    vmem = pl.BlockSpec(memory_space=pltpu.VMEM)
    acc, prod, table = pl.pallas_call(
        functools.partial(gather_scores, n_up, n_down),
        out_shape=[
            jax.ShapeDtypeStruct((dact, rows, BLOCK), F32), jax.ShapeDtypeStruct((dact, rows, BLOCK), F32),
            jax.ShapeDtypeStruct((dact, 8, BLOCK), jnp.int32),
        ],
        in_specs=[hbm] * 6,
        out_specs=[vmem] * 3,
        scratch_shapes=[
            pltpu.SMEM((uact, up_blocks.shape[0]), jnp.int32),
            pltpu.SMEM((dact,), jnp.int32),
            pltpu.VMEM((n_down, rows, depth), kind),
            pltpu.VMEM((cols // BLOCK, height, BLOCK), kind),
            pltpu.VMEM((2, n_up * height, used // 2), kind),
            pltpu.VMEM((rows // BLOCK, deltas.shape[0], BLOCK), kind),
            pltpu.VMEM((n_down, wins, uact, win, BLOCK), kind),
            pltpu.VMEM((cols // BLOCK, toks, BLOCK), kind),
            pltpu.VMEM((n_up * toks, used), kind),
            pltpu.VMEM((tokens, rows), kind),
            dma((6,)),
            dma((6,)),
            dma((4,)),
            dma((2,)),
            dma((2 * levels + 1,)),
            dma((levels + 2,)),
            dma((levels,)),
            dma((1,)),
            pltpu.SemaphoreType.REGULAR,
            pltpu.SemaphoreType.REGULAR,
        ],
        compiler_params=pltpu.CompilerParams(collective_id=0, has_side_effects=True, vmem_limit_bytes=LARGE),
        name="gather_scores",
    )(*[pltpu.with_memory_space_constraint(x, pltpu.HBM) for x in (up_blocks.T, down_blocks, deltas, gradients, decoder, encoder)])
    return pl.pallas_call(
        place,
        out_shape=jax.ShapeDtypeStruct((rows, cols), F32),
        in_specs=[vmem] * 3,
        out_specs=hbm,
        scratch_shapes=[pltpu.VMEM((rows, cols), F32), dma((1,))],
        compiler_params=pltpu.CompilerParams(vmem_limit_bytes=SMALL),
        name="place",
    )(acc, prod, table)


def plain_local(deltas, gradients, up_blocks, down_blocks, decoder, encoder):
    token_deltas = lax.all_gather(deltas, "down", axis=0, tiled=True)
    token_grads = lax.all_gather(gradients, "up", axis=0, tiled=True)
    tokens, rows = token_deltas.shape
    windows, dact = up_blocks.shape[0], down_blocks.shape[0]
    row_blocks, col_blocks = rows // BLOCK, encoder.shape[1] // BLOCK
    local_ids = jnp.arange(row_blocks, dtype=jnp.int32)
    block_on = jnp.any(up_blocks[:, :, None] == local_ids[None, None, :], axis=1)
    masked = token_deltas.reshape(windows, tokens // windows, row_blocks, BLOCK) * block_on[
        :, None, :, None].astype(token_deltas.dtype)
    masked = masked.reshape(tokens, rows)
    dec_whole = lax.all_gather(decoder, "down", axis=1, tiled=True)
    height = encoder.shape[0]
    enc_used = jnp.take(encoder.reshape(height, col_blocks, BLOCK), down_blocks, axis=1).reshape(height, dact * BLOCK)
    virtual = jnp.dot(dec_whole, lax.all_gather(enc_used, "up", axis=0, tiled=True), preferred_element_type=F32)
    grad_used = jnp.take(token_grads.reshape(tokens, col_blocks, BLOCK), down_blocks, axis=1).reshape(tokens, dact * BLOCK)
    product = lax.dot_general(masked, grad_used, (((0,), (0,)), ((), ())), preferred_element_type=F32)
    scored = (product * virtual).reshape(rows, dact, BLOCK)
    filled = jnp.zeros((rows, col_blocks, BLOCK), F32).at[:, down_blocks, :].set(scored)
    return filled.reshape(rows, encoder.shape[1])


def solution(mesh):
    n_up, n_down = mesh.shape["up"], mesh.shape["down"]
    ringed = n_down == 4 and n_up == 2 * n_down

    def local(deltas, gradients, up_blocks, down_blocks, decoder, encoder):
        args = (deltas, gradients, up_blocks, down_blocks, decoder, encoder)
        tokens = deltas.shape[0] * n_down
        win = tokens // up_blocks.shape[0]
        if ringed and deltas.shape[0] == 2 * win:
            return ring_local(n_up, n_down, win, *args)
        return plain_local(*args)

    placed = (P("down", "up"), P("up", "down"), P(None, "up"), P("down"), P("up", "down"), P("up", "down"))
    return jax.shard_map(local, mesh=mesh, in_specs=placed, out_specs=P("up", "down"), check_vma=False)
```

```python
import functools

import jax
import jax.numpy as jnp
from jax import lax
from jax.experimental import pallas as pl
from jax.experimental.pallas import tpu as pltpu
from jax.sharding import PartitionSpec as P

BLOCK = 128
TAIL = 128
LARGE, SMALL = 24 << 20, 8 << 20
MESH = pl.DeviceIdType.MESH
F32 = jnp.float32


def flag(number, block, kind):
    return jnp.where(jnp.full((1, BLOCK), number, jnp.int32) == block, 1.0, 0.0).astype(kind)


def within(number, count):
    return jnp.maximum(jnp.minimum(number, count - 1), 0)


def hits_of(number, slots):
    return [1 - jnp.minimum(jnp.abs(slot - number), 1) for slot in slots]


def gather_scores(
    n_up, n_down, upb_in, downb_in, deltas, grads, dec, enc, acc, prod, table,
    upb, downb, dec_all, enc_raw, enc_all, del_raw, del_all, grad_raw, grad_all, masked,
    load_sem, send_sem, dec_recv, del_recv, enc_recv, pair_recv, grad_recv, pg_recv, ready_z, ready_xy,
):
    levels = n_up // 2
    rows, depth = dec.shape
    height = enc.shape[0]
    half = enc_all.shape[2]
    part = rows // 2
    body = depth - TAIL
    toks = grads.shape[0]
    wins, uact, win = del_all.shape[1:4]
    dact = downb.shape[0]
    blocks = enc.shape[1] // BLOCK
    up, down = lax.axis_index("up"), lax.axis_index("down")
    z, core = up // 2, up % 2
    place = lambda d: 2 * (d // 2) + (d + d // 2) % 2
    pos = place(down)
    right, left = place((pos + 1) % 4), place((pos + 3) % 4)
    diag = place((pos + 2) % 4)
    ring_to = ((up, right), (up, left))
    ring_from = (left, right)
    step_of = (1, -1)
    pair = (2 * z + 1 - core, down)
    can_go = (z < levels - 1, z > 0)
    last = levels - 1
    at_end = jnp.logical_or(z == 0, z == last)
    inside = lambda level: jnp.logical_and(level >= 0, level < levels)

    high = levels // 2
    later = jnp.where(right > down, 1, 0) + jnp.where(left > down, 1, 0)
    barrier = pltpu.get_barrier_semaphore()

    def signal(sem, dev, when=None):
        if when is None:
            pl.semaphore_signal(sem, inc=1, device_id=dev, device_id_type=MESH)
        else:
            pl.when(when)(lambda: pl.semaphore_signal(sem, inc=1, device_id=dev, device_id_type=MESH))

    signal(barrier, pair)
    signal(barrier, (up + 2, down), z < last)
    signal(barrier, (up - 2, down), z > high)
    for d in (right, left):
        signal(barrier, (up, d), d > down)

    def by_block(src, dst, sem):
        return [pltpu.make_async_copy(src.at[:, b * BLOCK:(b + 1) * BLOCK], dst.at[b], sem) for b in range(dst.shape[0])]

    def loaded(ref, sem):
        pltpu.make_async_copy(ref, ref, sem).wait()

    load_downb = pltpu.make_async_copy(downb_in, downb, load_sem.at[0])
    load_upb = pltpu.make_async_copy(upb_in, upb, load_sem.at[4])
    load_dec = pltpu.make_async_copy(dec, dec_all.at[down], load_sem.at[3])
    for copy in (
        load_downb, *by_block(grads, grad_raw, load_sem.at[1]), *by_block(enc, enc_raw, load_sem.at[2]), load_dec,
        load_upb, *by_block(deltas, del_raw, load_sem.at[5]),
    ):
        copy.start()

    def remote(src, dst, kind, recv, dev):
        return pltpu.make_async_remote_copy(
            src, dst, send_sem.at[kind], recv, device_id=dev, device_id_type=MESH)

    def dec_half(r, i, owner):
        m = (i + r) % 2
        ref = dec_all.at[owner, m * part:(m + 1) * part]
        return remote(ref, ref, 0, dec_recv.at[i], ring_to[r])

    def dec_relay(r, i, owner):
        ref = dec_all.at[owner, r * part:(r + 1) * part, (body if i else 0):(depth if i else body)]
        return remote(ref, ref, 0, dec_recv.at[2 + i], ring_to[r])

    def enc_rows(level, c):
        return pl.ds(pl.multiple_of((level * 2 + c) * height, 16), height)

    def enc_a(level, c):
        return pl.ds(pl.multiple_of((level * 2 + c) * height + (1 - c) * TAIL, 16), height - TAIL)

    def enc_b(level, c):
        return pl.ds(pl.multiple_of((level * 2 + c) * height + c * (height - TAIL), 16), TAIL)

    def enc_copy(r, level, h, where, sem):
        ref = enc_all.at[h, where(level, core)]
        return remote(ref, ref, 1, enc_recv.at[sem], (up + 2 * step_of[r], down))

    def pair_copy(ref, sem):
        return remote(ref, ref, 2, pair_recv.at[sem], pair)

    def del_copy(r, owner):
        ref = del_all.at[owner]
        return remote(ref, ref, 0, del_recv.at[0], ring_to[r])

    def del_relay(r, owner):
        ref = del_all.at[owner, r]
        return remote(ref, ref, 0, del_recv.at[1], ring_to[r])

    def grad_rows(level, c):
        return grad_all.at[pl.ds(pl.multiple_of((level * 2 + c) * toks, toks), toks)]

    def grad_copy(r, level):
        ref = grad_rows(level, core)
        return remote(ref, ref, 1, grad_recv.at[level], (up + 2 * step_of[r], down))

    def pair_grad(level):
        ref = grad_rows(level, core)
        return remote(ref, ref, 2, pg_recv.at[0], pair)

    def pick_enc(h):
        for s in range(h * dact // 2, (h + 1) * dact // 2):
            at = s * BLOCK - h * half
            enc_all[h, pl.ds(pl.multiple_of(up * height, 16), height), at:at + BLOCK] = enc_raw[chosen[s]]

    load_downb.wait()
    chosen = [within(downb[s], blocks) for s in range(dact)]
    loaded(grad_raw, load_sem.at[1])
    for s in range(dact):
        grad_all[pl.ds(pl.multiple_of(up * toks, toks), toks), s * BLOCK:(s + 1) * BLOCK] = grad_raw[chosen[s]]
    pl.semaphore_wait(barrier, 3 - later + jnp.where(z > 0, 1, 0) + jnp.where(z >= high, 1, 0) - jnp.where(z == last, 1, 0))
    signal(ready_z, (up - 2, down), jnp.logical_and(z > 0, z <= high))
    for d in (right, left):
        signal(ready_xy, (up, d), d < down)

    early = (jnp.logical_and(z >= high, z < last), z > 0)

    def send_own(which, act):
        for r in (1, 0):
            @pl.when(which[r])
            def _():
                act(r)

    send_own(early, lambda r: grad_copy(r, z).start())
    loaded(enc_raw, load_sem.at[2])
    pick_enc(0)
    send_own(early, lambda r: enc_copy(r, z, 0, enc_rows, 2 * z).start())
    load_dec.wait()

    for r, d in enumerate((right, left)):
        @pl.when(d < down)
        def _():
            dec_half(r, 0, down).start()
    pick_enc(1)

    @pl.when(later > 0)
    def _():
        pl.semaphore_wait(ready_xy, later)
        for r, d in enumerate((right, left)):
            @pl.when(d > down)
            def _():
                dec_half(r, 0, down).start()
    pair_copy(enc_all.at[:, enc_rows(z, core)], z).start()
    load_upb.wait()
    loaded(del_raw, load_sem.at[5])
    for w in range(wins):
        for s in range(uact):
            del_all[down, w, s] = del_raw[within(upb[s, down * wins + w], rows // BLOCK), w * win:(w + 1) * win]
    for r in range(2):
        del_copy(r, down).start()
    for r in range(2):
        dec_half(r, 1, down).start()

    def each(j, act):
        for r in range(2):
            level = z - step_of[r] * j

            @pl.when(inside(level))
            def _():
                act(r, level)

    def relay_grad(r, level):
        grad_copy(r, level).wait_recv()

        @pl.when(can_go[r])
        def _():
            grad_copy(r, level).start()
        pair_grad(level).start()

    @pl.when(z < high)
    def _():
        pl.semaphore_wait(ready_z, 1)
        grad_copy(0, z).start()
        enc_copy(0, z, 0, enc_rows, 2 * z).start()
    pair_grad(z).start()
    each(1, relay_grad)
    send_own(can_go, lambda r: enc_copy(r, z, 1, enc_rows, 2 * z + 1).start())

    acc[...] = jnp.zeros_like(acc)

    def mult(q, rs, n, start=0, size=depth):
        ks = pl.ds(pl.multiple_of(start, BLOCK), size)
        result = jnp.dot(
            dec_all[q, rs, ks], enc_all[n, pl.ds(pl.multiple_of(q * depth + start, BLOCK), size), :],
            preferred_element_type=F32)
        for i in range(half // BLOCK):
            acc[n * (half // BLOCK) + i, rs] += result[:, i * BLOCK:(i + 1) * BLOCK]

    def enc_stage(q, n):
        gap = jnp.maximum(q - z, z - q)
        return jnp.where(gap == last, 5 + n, 2 * gap)

    def products(low, high):
        @pl.loop(0, 4 * levels)
        def _(u):
            q, m, n = u // 4, u // 2 % 2, u % 2
            first = jnp.where(jnp.where(q == left, 1, 0) + m == 1, 2, 4)
            stage = jnp.maximum(enc_stage(q, n), jnp.where(q == down, 0, first))
            ready = jnp.logical_and(stage >= low, stage <= high)

            @pl.when(jnp.logical_and(ready, q != diag))
            def _():
                mult(q, pl.ds(pl.multiple_of(m * part, part), part), n)

    everything = slice(0, rows)

    def diag_products(i):
        for n in range(2):
            @pl.when(enc_stage(diag, n) <= 5)
            def _():
                mult(diag, everything, n, body if i else 0, TAIL if i else body)

    def pair_whole(level):
        return pair_copy(enc_all.at[:, enc_rows(level, 1 - core)], level)

    def relay(j, h):
        def act(r, level):
            enc_copy(r, level, h, enc_rows, 2 * level + h).wait_recv()

            @pl.when(can_go[r])
            def _():
                if j == last - 1 and h == 1:
                    enc_copy(r, level, h, enc_a, 2 * level + h).start()
                    enc_copy(r, level, h, enc_b, 2 * levels).start()
                else:
                    enc_copy(r, level, h, enc_rows, 2 * level + h).start()
            if h == 1:
                pair_copy(enc_all.at[:, enc_rows(level, core)], level).start()
        each(j, act)

    relay(1, 0)
    each(2, relay_grad)
    relay(1, 1)
    loaded(dec_all.at[left], dec_recv.at[0])
    loaded(del_all.at[pl.ds(0, 2)], del_recv.at[0])
    for r in range(2):
        del_relay(r, ring_from[r]).start()
        for i in range(2):
            dec_relay(r, i, ring_from[r]).start()
    pair_whole(z).wait_recv()
    each(1, lambda r, level: pair_whole(level).wait_recv())
    products(0, 2)
    each(3, relay_grad)
    relay(2, 0)

    relay(2, 1)
    loaded(dec_all.at[left], dec_recv.at[1])
    each(2, lambda r, level: pair_whole(level).wait_recv())
    products(3, 4)

    loaded(del_all.at[diag], del_recv.at[1])
    loaded(grad_all.at[pl.ds(0, levels * toks)], pg_recv.at[0])
    for d in range(n_down):
        for w in range(wins):
            for b in range(rows // BLOCK):
                hits = hits_of(b, [upb[s, d * wins + w] for s in range(uact)])
                slot = within(sum(s * hit for s, hit in enumerate(hits)), uact)
                t = (d * wins + w) * win
                masked[t:t + win, b * BLOCK:(b + 1) * BLOCK] = del_all[d, w, slot] * flag(sum(hits), 1, masked.dtype)
    whole = lax.dot_general(
        masked[...], grad_all[...], (((0,), (0,)), ((), ())), preferred_element_type=F32)
    for s in range(dact):
        prod[s] = whole[:, s * BLOCK:(s + 1) * BLOCK]
        table[s] = jnp.full(table.shape[1:], downb[s], jnp.int32)

    far = last - z

    def end_wait(h, where, sem):
        for r in range(2):
            @pl.when(z == (0 if r else last))
            def _():
                enc_copy(r, far, h, where, sem).wait_recv()

    @pl.when(at_end)
    def _():
        end_wait(0, enc_rows, 2 * far)
        pair_copy(enc_all.at[0, enc_rows(far, core)], far).start()
        pair_copy(enc_all.at[0, enc_rows(far, 1 - core)], far).wait_recv()

        @pl.when(far != diag)
        def _():
            mult(far, everything, 0)

    def first_relay():
        loaded(dec_all.at[diag, :, :body], dec_recv.at[2])
        diag_products(0)

    def inner():
        pair_copy(enc_all.at[1, enc_a(far, 1 - core)], levels).wait_recv()
        mult(far, everything, 1, core * TAIL, depth - TAIL)

    @pl.when(at_end)
    def _():
        pl.when(core == 1)(first_relay)
        end_wait(1, enc_a, 2 * far + 1)
        pair_copy(enc_all.at[1, enc_a(far, core)], levels).start()
        pl.when(core == 0)(first_relay)
        end_wait(1, enc_b, 2 * levels)
        pair_copy(enc_all.at[1, enc_b(far, core)], levels + 1).start()
        pl.when(core == 0)(inner)
    pl.when(jnp.logical_not(at_end))(first_relay)
    loaded(dec_all.at[diag, :, body:], dec_recv.at[3])
    diag_products(1)

    @pl.when(at_end)
    def _():
        pl.when(core == 1)(inner)
        pair_copy(enc_all.at[1, enc_b(far, 1 - core)], levels + 1).wait_recv()
        mult(far, everything, 1, (1 - core) * (depth - TAIL), TAIL)

    def sent(ref, kind):
        pltpu.make_async_copy(ref, ref, send_sem.at[kind]).wait()

    both = height + toks
    sent(enc_all.at[:, pl.ds(0, (n_down - 1) * (rows * depth + wins * uact * win * BLOCK) // (2 * half))], 0)

    @pl.when(at_end)
    def _():
        sent(enc_all.at[:, pl.ds(0, both)], 1)

    @pl.when(jnp.logical_not(at_end))
    def _():
        sent(enc_all.at[:, pl.ds(0, (levels + 1) * both)], 1)
    sent(enc_all.at[:, pl.ds(0, levels * both)], 2)


def place(acc, prod, table, out, held, sem):
    dact, rows, _ = acc.shape
    blocks = out.shape[1] // BLOCK
    tile = 32

    @pl.loop(0, rows // tile)
    def _(t):
        rs = pl.ds(pl.multiple_of(t * tile, tile), tile)
        values = [acc[s, rs] * prod[s, rs] for s in range(dact)]
        numbers = [jnp.broadcast_to(table[s, 0:1], (tile, BLOCK)) for s in range(dact)]
        for c in range(blocks):
            total = jnp.zeros((tile, BLOCK), F32)
            for value, number in zip(values, numbers):
                total = jnp.where(number == c, value, total)
            held[rs, c * BLOCK:(c + 1) * BLOCK] = total
        pltpu.make_async_copy(held.at[rs], out.at[rs], sem.at[0]).start()

    pltpu.make_async_copy(held, out, sem.at[0]).wait()


def ring_local(n_up, n_down, win, deltas, gradients, up_blocks, down_blocks, decoder, encoder):
    rows, depth = decoder.shape
    height, cols = encoder.shape
    toks = gradients.shape[0]
    uact, dact = up_blocks.shape[1], down_blocks.shape[0]
    tokens = deltas.shape[0] * n_down
    wins = deltas.shape[0] // win
    used = dact * BLOCK
    levels = n_up // 2
    kind = decoder.dtype
    dma = pltpu.SemaphoreType.DMA
    hbm = pl.BlockSpec(memory_space=pltpu.HBM)
    vmem = pl.BlockSpec(memory_space=pltpu.VMEM)
    acc, prod, table = pl.pallas_call(
        functools.partial(gather_scores, n_up, n_down),
        out_shape=[
            jax.ShapeDtypeStruct((dact, rows, BLOCK), F32), jax.ShapeDtypeStruct((dact, rows, BLOCK), F32),
            jax.ShapeDtypeStruct((dact, 8, BLOCK), jnp.int32),
        ],
        in_specs=[hbm] * 6,
        out_specs=[vmem] * 3,
        scratch_shapes=[
            pltpu.SMEM((uact, up_blocks.shape[0]), jnp.int32),
            pltpu.SMEM((dact,), jnp.int32),
            pltpu.VMEM((n_down, rows, depth), kind),
            pltpu.VMEM((cols // BLOCK, height, BLOCK), kind),
            pltpu.VMEM((2, n_up * height, used // 2), kind),
            pltpu.VMEM((rows // BLOCK, deltas.shape[0], BLOCK), kind),
            pltpu.VMEM((n_down, wins, uact, win, BLOCK), kind),
            pltpu.VMEM((cols // BLOCK, toks, BLOCK), kind),
            pltpu.VMEM((n_up * toks, used), kind),
            pltpu.VMEM((tokens, rows), kind),
            dma((6,)),
            dma((3,)),
            dma((4,)),
            dma((2,)),
            dma((2 * levels + 1,)),
            dma((levels + 2,)),
            dma((levels,)),
            dma((1,)),
            pltpu.SemaphoreType.REGULAR,
            pltpu.SemaphoreType.REGULAR,
        ],
        compiler_params=pltpu.CompilerParams(collective_id=0, has_side_effects=True, vmem_limit_bytes=LARGE),
        name="gather_scores",
    )(*[pltpu.with_memory_space_constraint(x, pltpu.HBM) for x in (up_blocks.T, down_blocks, deltas, gradients, decoder, encoder)])
    return pl.pallas_call(
        place,
        out_shape=jax.ShapeDtypeStruct((rows, cols), F32),
        in_specs=[vmem] * 3,
        out_specs=hbm,
        scratch_shapes=[pltpu.VMEM((rows, cols), F32), dma((1,))],
        compiler_params=pltpu.CompilerParams(vmem_limit_bytes=SMALL),
        name="place",
    )(acc, prod, table)


def plain_local(deltas, gradients, up_blocks, down_blocks, decoder, encoder):
    token_deltas = lax.all_gather(deltas, "down", axis=0, tiled=True)
    token_grads = lax.all_gather(gradients, "up", axis=0, tiled=True)
    tokens, rows = token_deltas.shape
    windows, dact = up_blocks.shape[0], down_blocks.shape[0]
    row_blocks, col_blocks = rows // BLOCK, encoder.shape[1] // BLOCK
    local_ids = jnp.arange(row_blocks, dtype=jnp.int32)
    block_on = jnp.any(up_blocks[:, :, None] == local_ids[None, None, :], axis=1)
    masked = token_deltas.reshape(windows, tokens // windows, row_blocks, BLOCK) * block_on[
        :, None, :, None].astype(token_deltas.dtype)
    masked = masked.reshape(tokens, rows)
    dec_whole = lax.all_gather(decoder, "down", axis=1, tiled=True)
    height = encoder.shape[0]
    enc_used = jnp.take(encoder.reshape(height, col_blocks, BLOCK), down_blocks, axis=1).reshape(height, dact * BLOCK)
    virtual = jnp.dot(dec_whole, lax.all_gather(enc_used, "up", axis=0, tiled=True), preferred_element_type=F32)
    grad_used = jnp.take(token_grads.reshape(tokens, col_blocks, BLOCK), down_blocks, axis=1).reshape(tokens, dact * BLOCK)
    product = lax.dot_general(masked, grad_used, (((0,), (0,)), ((), ())), preferred_element_type=F32)
    scored = (product * virtual).reshape(rows, dact, BLOCK)
    filled = jnp.zeros((rows, col_blocks, BLOCK), F32).at[:, down_blocks, :].set(scored)
    return filled.reshape(rows, encoder.shape[1])


def solution(mesh):
    n_up, n_down = mesh.shape["up"], mesh.shape["down"]
    ringed = n_down == 4 and n_up == 2 * n_down

    def local(deltas, gradients, up_blocks, down_blocks, decoder, encoder):
        args = (deltas, gradients, up_blocks, down_blocks, decoder, encoder)
        tokens = deltas.shape[0] * n_down
        win = tokens // up_blocks.shape[0]
        if ringed and deltas.shape[0] == 2 * win:
            return ring_local(n_up, n_down, win, *args)
        return plain_local(*args)

    placed = (P("down", "up"), P("up", "down"), P(None, "up"), P("down"), P("up", "down"), P("up", "down"))
    return jax.shard_map(local, mesh=mesh, in_specs=placed, out_specs=P("up", "down"), check_vma=False)
```

```python
import functools

import jax
import jax.numpy as jnp
from jax import lax
from jax.experimental import pallas as pl
from jax.experimental.pallas import tpu as pltpu
from jax.sharding import PartitionSpec as P

BLOCK = 128
TAIL = 128
LARGE, SMALL = 24 << 20, 8 << 20
MESH = pl.DeviceIdType.MESH
F32 = jnp.float32


def flag(number, block, kind):
    return jnp.where(jnp.full((1, BLOCK), number, jnp.int32) == block, 1.0, 0.0).astype(kind)


def within(number, count):
    return jnp.maximum(jnp.minimum(number, count - 1), 0)


def hits_of(number, slots):
    return [1 - jnp.minimum(jnp.abs(slot - number), 1) for slot in slots]


def gather_scores(
    n_up, n_down, upb_in, downb_in, deltas, grads, dec, enc, acc, prod, table,
    upb, downb, dec_all, enc_raw, enc_all, del_raw, del_all, grad_raw, grad_all, masked,
    load_sem, send_sem, dec_recv, del_recv, enc_recv, pair_recv, grad_recv, pg_recv, ready_z, ready_xy,
):
    levels = n_up // 2
    rows, depth = dec.shape
    height = enc.shape[0]
    half = enc_all.shape[2]
    part = rows // 2
    body = depth - TAIL
    toks = grads.shape[0]
    wins, uact, win = del_all.shape[1:4]
    dact = downb.shape[0]
    blocks = enc.shape[1] // BLOCK
    up, down = lax.axis_index("up"), lax.axis_index("down")
    z, core = up // 2, up % 2
    place = lambda d: 2 * (d // 2) + (d + d // 2) % 2
    pos = place(down)
    right, left = place((pos + 1) % 4), place((pos + 3) % 4)
    diag = place((pos + 2) % 4)
    ring_to = ((up, right), (up, left))
    ring_from = (left, right)
    step_of = (1, -1)
    pair = (2 * z + 1 - core, down)
    can_go = (z < levels - 1, z > 0)
    last = levels - 1
    at_end = jnp.logical_or(z == 0, z == last)
    inside = lambda level: jnp.logical_and(level >= 0, level < levels)

    high = levels // 2
    later = jnp.where(right > down, 1, 0) + jnp.where(left > down, 1, 0)
    barrier = pltpu.get_barrier_semaphore()

    def signal(sem, dev, when=None):
        if when is None:
            pl.semaphore_signal(sem, inc=1, device_id=dev, device_id_type=MESH)
        else:
            pl.when(when)(lambda: pl.semaphore_signal(sem, inc=1, device_id=dev, device_id_type=MESH))

    signal(barrier, pair)
    signal(barrier, (up + 2, down), z < last)
    signal(barrier, (up - 2, down), z > high)
    for d in (right, left):
        signal(barrier, (up, d), d > down)

    def by_block(src, dst, sem):
        return [pltpu.make_async_copy(src.at[:, b * BLOCK:(b + 1) * BLOCK], dst.at[b], sem) for b in range(dst.shape[0])]

    def loaded(ref, sem):
        pltpu.make_async_copy(ref, ref, sem).wait()

    load_downb = pltpu.make_async_copy(downb_in, downb, load_sem.at[0])
    load_upb = pltpu.make_async_copy(upb_in, upb, load_sem.at[4])
    load_dec = pltpu.make_async_copy(dec, dec_all.at[down], load_sem.at[3])
    for copy in (
        load_downb, *by_block(grads, grad_raw, load_sem.at[1]), *by_block(enc, enc_raw, load_sem.at[2]), load_dec,
        load_upb, *by_block(deltas, del_raw, load_sem.at[5]),
    ):
        copy.start()

    def remote(src, dst, kind, recv, dev):
        return pltpu.make_async_remote_copy(
            src, dst, send_sem.at[kind], recv, device_id=dev, device_id_type=MESH)

    def dec_half(r, i, owner):
        m = (i + r) % 2
        ref = dec_all.at[owner, m * part:(m + 1) * part]
        return remote(ref, ref, 0, dec_recv.at[i], ring_to[r])

    def dec_relay(r, i, owner):
        ref = dec_all.at[owner, r * part:(r + 1) * part, (body if i else 0):(depth if i else body)]
        return remote(ref, ref, 0, dec_recv.at[2 + i], ring_to[r])

    def enc_rows(level, c):
        return pl.ds(pl.multiple_of((level * 2 + c) * height, 16), height)

    def enc_a(level, c):
        return pl.ds(pl.multiple_of((level * 2 + c) * height + (1 - c) * TAIL, 16), height - TAIL)

    def enc_b(level, c):
        return pl.ds(pl.multiple_of((level * 2 + c) * height + c * (height - TAIL), 16), TAIL)

    def enc_copy(r, level, h, where, sem):
        ref = enc_all.at[h, where(level, core)]
        return remote(ref, ref, 1, enc_recv.at[sem], (up + 2 * step_of[r], down))

    def pair_copy(ref, sem):
        return remote(ref, ref, 2, pair_recv.at[sem], pair)

    def del_copy(r, owner):
        ref = del_all.at[owner]
        return remote(ref, ref, 0, del_recv.at[0], ring_to[r])

    def del_relay(r, owner):
        ref = del_all.at[owner, r]
        return remote(ref, ref, 0, del_recv.at[1], ring_to[r])

    def grad_rows(level, c):
        return grad_all.at[pl.ds(pl.multiple_of((level * 2 + c) * toks, toks), toks)]

    def grad_copy(r, level):
        ref = grad_rows(level, core)
        return remote(ref, ref, 1, grad_recv.at[level], (up + 2 * step_of[r], down))

    def pair_grad(level):
        ref = grad_rows(level, core)
        return remote(ref, ref, 2, pg_recv.at[0], pair)

    def pick_enc(h):
        for s in range(h * dact // 2, (h + 1) * dact // 2):
            at = s * BLOCK - h * half
            enc_all[h, pl.ds(pl.multiple_of(up * height, 16), height), at:at + BLOCK] = enc_raw[chosen[s]]

    load_downb.wait()
    chosen = [within(downb[s], blocks) for s in range(dact)]
    loaded(grad_raw, load_sem.at[1])
    for s in range(dact):
        grad_all[pl.ds(pl.multiple_of(up * toks, toks), toks), s * BLOCK:(s + 1) * BLOCK] = grad_raw[chosen[s]]
    pl.semaphore_wait(barrier, 3 - later + jnp.where(z > 0, 1, 0) + jnp.where(z >= high, 1, 0) - jnp.where(z == last, 1, 0))
    signal(ready_z, (up - 2, down), jnp.logical_and(z > 0, z <= high))
    for d in (right, left):
        signal(ready_xy, (up, d), d < down)

    early = (jnp.logical_and(z >= high, z < last), z > 0)

    def send_own(which, act):
        for r in (1, 0):
            @pl.when(which[r])
            def _():
                act(r)

    send_own(early, lambda r: grad_copy(r, z).start())
    loaded(enc_raw, load_sem.at[2])
    pick_enc(0)
    send_own(early, lambda r: enc_copy(r, z, 0, enc_rows, 2 * z).start())
    load_dec.wait()

    for r, d in enumerate((right, left)):
        @pl.when(d < down)
        def _():
            dec_half(r, 0, down).start()
    pick_enc(1)

    @pl.when(later > 0)
    def _():
        pl.semaphore_wait(ready_xy, later)
        for r, d in enumerate((right, left)):
            @pl.when(d > down)
            def _():
                dec_half(r, 0, down).start()
    pair_copy(enc_all.at[:, enc_rows(z, core)], z).start()
    load_upb.wait()
    loaded(del_raw, load_sem.at[5])
    for w in range(wins):
        for s in range(uact):
            del_all[down, w, s] = del_raw[within(upb[s, down * wins + w], rows // BLOCK), w * win:(w + 1) * win]
    for r in range(2):
        del_copy(r, down).start()
    for r in range(2):
        dec_half(r, 1, down).start()

    def each(j, act):
        for r in range(2):
            level = z - step_of[r] * j

            @pl.when(inside(level))
            def _():
                act(r, level)

    def relay_grad(r, level):
        grad_copy(r, level).wait_recv()

        @pl.when(can_go[r])
        def _():
            grad_copy(r, level).start()
        pair_grad(level).start()

    @pl.when(z < high)
    def _():
        pl.semaphore_wait(ready_z, 1)
        grad_copy(0, z).start()
        enc_copy(0, z, 0, enc_rows, 2 * z).start()
    pair_grad(z).start()
    each(1, relay_grad)
    send_own(can_go, lambda r: enc_copy(r, z, 1, enc_rows, 2 * z + 1).start())

    acc[...] = jnp.zeros_like(acc)

    def mult(q, rs, n, start=0, size=depth):
        ks = pl.ds(pl.multiple_of(start, BLOCK), size)
        result = jnp.dot(
            dec_all[q, rs, ks], enc_all[n, pl.ds(pl.multiple_of(q * depth + start, BLOCK), size), :],
            preferred_element_type=F32)
        for i in range(half // BLOCK):
            acc[n * (half // BLOCK) + i, rs] += result[:, i * BLOCK:(i + 1) * BLOCK]

    def enc_stage(q, n):
        gap = jnp.maximum(q - z, z - q)
        return jnp.where(gap == last, 5 + n, 2 * gap)

    def products(low, high):
        @pl.loop(0, 4 * levels)
        def _(u):
            q, m, n = u // 4, u // 2 % 2, u % 2
            first = jnp.where(jnp.where(q == left, 1, 0) + m == 1, 2, 4)
            stage = jnp.maximum(enc_stage(q, n), jnp.where(q == down, 0, first))
            ready = jnp.logical_and(stage >= low, stage <= high)

            @pl.when(jnp.logical_and(ready, q != diag))
            def _():
                mult(q, pl.ds(pl.multiple_of(m * part, part), part), n)

    everything = slice(0, rows)

    def diag_products(i):
        for n in range(2):
            @pl.when(enc_stage(diag, n) <= 5)
            def _():
                mult(diag, everything, n, body if i else 0, TAIL if i else body)

    def pair_whole(level):
        return pair_copy(enc_all.at[:, enc_rows(level, 1 - core)], level)

    def relay(j, h):
        def act(r, level):
            enc_copy(r, level, h, enc_rows, 2 * level + h).wait_recv()

            @pl.when(can_go[r])
            def _():
                if j == last - 1 and h == 1:
                    enc_copy(r, level, h, enc_a, 2 * level + h).start()
                    enc_copy(r, level, h, enc_b, 2 * levels).start()
                else:
                    enc_copy(r, level, h, enc_rows, 2 * level + h).start()
            if h == 1:
                pair_copy(enc_all.at[:, enc_rows(level, core)], level).start()
        each(j, act)

    relay(1, 0)
    each(2, relay_grad)
    relay(1, 1)
    loaded(dec_all.at[left], dec_recv.at[0])
    loaded(del_all.at[pl.ds(0, 2)], del_recv.at[0])
    for r in range(2):
        del_relay(r, ring_from[r]).start()
        for i in range(2):
            dec_relay(r, i, ring_from[r]).start()
    pair_whole(z).wait_recv()
    each(1, lambda r, level: pair_whole(level).wait_recv())
    products(0, 2)
    each(3, relay_grad)
    relay(2, 0)

    relay(2, 1)
    loaded(dec_all.at[left], dec_recv.at[1])
    each(2, lambda r, level: pair_whole(level).wait_recv())
    products(3, 4)

    loaded(del_all.at[diag], del_recv.at[1])
    loaded(grad_all.at[pl.ds(0, levels * toks)], pg_recv.at[0])
    for d in range(n_down):
        for w in range(wins):
            for b in range(rows // BLOCK):
                hits = hits_of(b, [upb[s, d * wins + w] for s in range(uact)])
                slot = within(sum(s * hit for s, hit in enumerate(hits)), uact)
                t = (d * wins + w) * win
                masked[t:t + win, b * BLOCK:(b + 1) * BLOCK] = del_all[d, w, slot] * flag(sum(hits), 1, masked.dtype)
    whole = lax.dot_general(
        masked[...], grad_all[...], (((0,), (0,)), ((), ())), preferred_element_type=F32)
    for s in range(dact):
        prod[s] = whole[:, s * BLOCK:(s + 1) * BLOCK]
        table[s] = jnp.full(table.shape[1:], downb[s], jnp.int32)

    far = last - z

    def end_wait(h, where, sem):
        for r in range(2):
            @pl.when(z == (0 if r else last))
            def _():
                enc_copy(r, far, h, where, sem).wait_recv()

    @pl.when(at_end)
    def _():
        end_wait(0, enc_rows, 2 * far)
        pair_copy(enc_all.at[0, enc_rows(far, core)], far).start()
        pair_copy(enc_all.at[0, enc_rows(far, 1 - core)], far).wait_recv()

        @pl.when(far != diag)
        def _():
            mult(far, everything, 0)

    def first_relay():
        loaded(dec_all.at[diag, :, :body], dec_recv.at[2])
        diag_products(0)

    def inner():
        pair_copy(enc_all.at[1, enc_a(far, 1 - core)], levels).wait_recv()
        mult(far, everything, 1, core * TAIL, depth - TAIL)

    @pl.when(at_end)
    def _():
        pl.when(core == 1)(first_relay)
        end_wait(1, enc_a, 2 * far + 1)
        pair_copy(enc_all.at[1, enc_a(far, core)], levels).start()
        pl.when(core == 0)(first_relay)
        end_wait(1, enc_b, 2 * levels)
        pair_copy(enc_all.at[1, enc_b(far, core)], levels + 1).start()
        pl.when(core == 0)(inner)
    pl.when(jnp.logical_not(at_end))(first_relay)
    loaded(dec_all.at[diag, :, body:], dec_recv.at[3])
    diag_products(1)

    @pl.when(at_end)
    def _():
        pl.when(core == 1)(inner)
        pair_copy(enc_all.at[1, enc_b(far, 1 - core)], levels + 1).wait_recv()
        mult(far, everything, 1, (1 - core) * (depth - TAIL), TAIL)

    def sent(ref, kind):
        pltpu.make_async_copy(ref, ref, send_sem.at[kind]).wait()

    both = height + toks
    sent(enc_all.at[:, pl.ds(0, (n_down - 1) * (rows * depth + wins * uact * win * BLOCK) // (2 * half))], 0)

    @pl.when(at_end)
    def _():
        sent(enc_all.at[:, pl.ds(0, both)], 1)

    @pl.when(jnp.logical_not(at_end))
    def _():
        sent(enc_all.at[:, pl.ds(0, (levels + 1) * both)], 1)
    sent(enc_all.at[:, pl.ds(0, levels * both)], 2)


def place(acc, prod, table, out, held, sem):
    dact, rows, _ = acc.shape
    blocks = out.shape[1] // BLOCK
    tile = 32

    for t in range(rows // tile):
        rs = slice(t * tile, (t + 1) * tile)
        values = [acc[s, rs] * prod[s, rs] for s in range(dact)]
        numbers = [jnp.broadcast_to(table[s, 0:1], (tile, BLOCK)) for s in range(dact)]
        for c in range(blocks):
            total = jnp.zeros((tile, BLOCK), F32)
            for value, number in zip(values, numbers):
                total = jnp.where(number == c, value, total)
            held[rs, c * BLOCK:(c + 1) * BLOCK] = total
        pltpu.make_async_copy(held.at[rs], out.at[rs], sem.at[0]).start()

    pltpu.make_async_copy(held, out, sem.at[0]).wait()


def ring_local(n_up, n_down, win, deltas, gradients, up_blocks, down_blocks, decoder, encoder):
    rows, depth = decoder.shape
    height, cols = encoder.shape
    toks = gradients.shape[0]
    uact, dact = up_blocks.shape[1], down_blocks.shape[0]
    tokens = deltas.shape[0] * n_down
    wins = deltas.shape[0] // win
    used = dact * BLOCK
    levels = n_up // 2
    kind = decoder.dtype
    dma = pltpu.SemaphoreType.DMA
    hbm = pl.BlockSpec(memory_space=pltpu.HBM)
    vmem = pl.BlockSpec(memory_space=pltpu.VMEM)
    acc, prod, table = pl.pallas_call(
        functools.partial(gather_scores, n_up, n_down),
        out_shape=[
            jax.ShapeDtypeStruct((dact, rows, BLOCK), F32), jax.ShapeDtypeStruct((dact, rows, BLOCK), F32),
            jax.ShapeDtypeStruct((dact, 8, BLOCK), jnp.int32),
        ],
        in_specs=[hbm] * 6,
        out_specs=[vmem] * 3,
        scratch_shapes=[
            pltpu.SMEM((uact, up_blocks.shape[0]), jnp.int32),
            pltpu.SMEM((dact,), jnp.int32),
            pltpu.VMEM((n_down, rows, depth), kind),
            pltpu.VMEM((cols // BLOCK, height, BLOCK), kind),
            pltpu.VMEM((2, n_up * height, used // 2), kind),
            pltpu.VMEM((rows // BLOCK, deltas.shape[0], BLOCK), kind),
            pltpu.VMEM((n_down, wins, uact, win, BLOCK), kind),
            pltpu.VMEM((cols // BLOCK, toks, BLOCK), kind),
            pltpu.VMEM((n_up * toks, used), kind),
            pltpu.VMEM((tokens, rows), kind),
            dma((6,)),
            dma((3,)),
            dma((4,)),
            dma((2,)),
            dma((2 * levels + 1,)),
            dma((levels + 2,)),
            dma((levels,)),
            dma((1,)),
            pltpu.SemaphoreType.REGULAR,
            pltpu.SemaphoreType.REGULAR,
        ],
        compiler_params=pltpu.CompilerParams(collective_id=0, has_side_effects=True, vmem_limit_bytes=LARGE),
        name="gather_scores",
    )(*[pltpu.with_memory_space_constraint(x, pltpu.HBM) for x in (up_blocks.T, down_blocks, deltas, gradients, decoder, encoder)])
    return pl.pallas_call(
        place,
        out_shape=jax.ShapeDtypeStruct((rows, cols), F32),
        in_specs=[vmem] * 3,
        out_specs=hbm,
        scratch_shapes=[pltpu.VMEM((rows, cols), F32), dma((1,))],
        compiler_params=pltpu.CompilerParams(vmem_limit_bytes=SMALL),
        name="place",
    )(acc, prod, table)


def plain_local(deltas, gradients, up_blocks, down_blocks, decoder, encoder):
    token_deltas = lax.all_gather(deltas, "down", axis=0, tiled=True)
    token_grads = lax.all_gather(gradients, "up", axis=0, tiled=True)
    tokens, rows = token_deltas.shape
    windows, dact = up_blocks.shape[0], down_blocks.shape[0]
    row_blocks, col_blocks = rows // BLOCK, encoder.shape[1] // BLOCK
    local_ids = jnp.arange(row_blocks, dtype=jnp.int32)
    block_on = jnp.any(up_blocks[:, :, None] == local_ids[None, None, :], axis=1)
    masked = token_deltas.reshape(windows, tokens // windows, row_blocks, BLOCK) * block_on[
        :, None, :, None].astype(token_deltas.dtype)
    masked = masked.reshape(tokens, rows)
    dec_whole = lax.all_gather(decoder, "down", axis=1, tiled=True)
    height = encoder.shape[0]
    enc_used = jnp.take(encoder.reshape(height, col_blocks, BLOCK), down_blocks, axis=1).reshape(height, dact * BLOCK)
    virtual = jnp.dot(dec_whole, lax.all_gather(enc_used, "up", axis=0, tiled=True), preferred_element_type=F32)
    grad_used = jnp.take(token_grads.reshape(tokens, col_blocks, BLOCK), down_blocks, axis=1).reshape(tokens, dact * BLOCK)
    product = lax.dot_general(masked, grad_used, (((0,), (0,)), ((), ())), preferred_element_type=F32)
    scored = (product * virtual).reshape(rows, dact, BLOCK)
    filled = jnp.zeros((rows, col_blocks, BLOCK), F32).at[:, down_blocks, :].set(scored)
    return filled.reshape(rows, encoder.shape[1])


def solution(mesh):
    n_up, n_down = mesh.shape["up"], mesh.shape["down"]
    ringed = n_down == 4 and n_up == 2 * n_down

    def local(deltas, gradients, up_blocks, down_blocks, decoder, encoder):
        args = (deltas, gradients, up_blocks, down_blocks, decoder, encoder)
        tokens = deltas.shape[0] * n_down
        win = tokens // up_blocks.shape[0]
        if ringed and deltas.shape[0] == 2 * win:
            return ring_local(n_up, n_down, win, *args)
        return plain_local(*args)

    placed = (P("down", "up"), P("up", "down"), P(None, "up"), P("down"), P("up", "down"), P("up", "down"))
    return jax.shard_map(local, mesh=mesh, in_specs=placed, out_specs=P("up", "down"), check_vma=False)
```
